128 devices in a mesh: seq: 16 (over z, x_lo, core), chan: 8 (over x_hi, y).
Axes of the slice: x: 4 (x_hi: 2, x_lo: 2; x = x_hi * 2 + x_lo), y: 4, z: 4, core: 2. Of those that a mesh axis runs over, the one named last changes fastest.
Arguments:
- hidden: bfloat16 [8192, 2560], P('seq'), may hold values from -16 to 16
- embedding: bfloat16 [8192, 2560], P('seq'), may hold values from -16 to 16
- segments: int32 [8192], replicated, may hold values from 0 to 2, never falling along the last dimension, each value on 1 to 6144 neighbouring positions
- input_norm_gain: float32 [2560], replicated, may hold values from 0.5 to 1.5
- gate_proj: bfloat16 [2560, 5120], P(None, 'chan'), may hold values from -0.125 to 0.125
- input_proj: bfloat16 [2560, 5120], P(None, 'chan'), may hold values from -0.125 to 0.125
- state_proj: bfloat16 [2560, 128], replicated, may hold values from -0.125 to 0.125
- step_proj: bfloat16 [2560, 80], P(None, 'chan'), may hold values from -1 to 1
- step_bias: float32 [80], P('chan'), may hold values from -5 to -3
- decay_log: float32 [80], P('chan'), may hold values from -8 to 1
- skip_gain: float32 [80], P('chan'), may hold values from 0.5 to 1.5
- out_gain: float32 [5120], P('chan'), may hold values from 0.5 to 1.5
- out_proj: bfloat16 [5120, 2560], P('chan'), may hold values from -0.078125 to 0.078125
- attn_gain: float32 [5120], replicated, may hold values from 0.5 to 1.5
- query_proj: bfloat16 [5120, 5120], P('seq', 'chan'), may hold values from -1 to 1
- key_proj: bfloat16 [5120, 5120], P('seq', 'chan'), may hold values from -1 to 1
- value_proj: bfloat16 [5120, 5120], P('seq', 'chan'), may hold values from -0.078125 to 0.078125
- attn_out: bfloat16 [5120, 2560], P('chan', 'seq'), may hold values from -0.078125 to 0.078125
Outputs:
- mixed: bfloat16 [8192, 2560], P('seq', 'chan')
The draws below stay inside these ranges and needn't reach their ends.
Inputs may be any that keep to these rules, and one draw needn't show every extreme that they name: `segments`: document ids never fall along the sequence, and every document has 1 to 6144 positions.
All inputs are finite; a program needn't handle non-finite values.
Results may differ from the reference program's by a relative error of at most 0.0095.
Values may be sent and summed in bfloat16 or wider, within the bound.
A program may use at most 256 MiB of HBM per device.

```python
import math
import jax
import jax.numpy as jnp
import numpy as np
from jax import lax

D = 2560
N = 64
HEAD_CHANNELS = 64
AH = 32
DI = 5120
H = 80
AP = 160
TOK_DEV = 512
SEQUENCE_TOKENS = 8192


def spike_weights(key):
    source = jax.random.normal(jax.random.fold_in(key, 7), (D, H), jnp.float32)
    return jnp.clip(source, -6.0, 6.0) / math.sqrt(D)


def drawn_weight(key, salt):
    source = jnp.clip(jax.random.normal(jax.random.fold_in(key, salt), (2 * D, 2 * D), jnp.float32), -6.0, 6.0)
    values = source / math.sqrt(2 * D)
    return values


def draw_query_proj(key, part):
    return drawn_weight(key, 32).astype(jnp.bfloat16)


def draw_key_proj(key, part):
    return drawn_weight(key, 33).astype(jnp.bfloat16)


def draw_embedding(key, part):
    values = jnp.clip(jax.random.normal(jax.random.fold_in(key, 31), (SEQUENCE_TOKENS, D), jnp.float32), -6.0, 6.0)
    return jnp.clip(values, -16.0, 16.0).astype(jnp.bfloat16)


def draw_step_proj(key, part):
    return spike_weights(key).astype(jnp.bfloat16)


def draw_hidden(key, part):
    source = jnp.clip(jax.random.normal(jax.random.fold_in(key, 3), (SEQUENCE_TOKENS, D), jnp.float32), -6.0, 6.0)
    heading_vector = jnp.sum(spike_weights(key), axis=1)
    heading_vector = heading_vector / jnp.sqrt(jnp.mean(heading_vector * heading_vector))
    spots = jax.random.randint(jax.random.fold_in(key, 5), (6,), 0, SEQUENCE_TOKENS)
    marks = jnp.zeros((SEQUENCE_TOKENS,), jnp.float32).at[spots].set(1.0)
    values = source * (1.0 - 0.7 * marks[:, None]) + 3.0 * marks[:, None] * heading_vector[None, :]
    return jnp.clip(values, -16.0, 16.0).astype(jnp.bfloat16)


def draw_decay_log(key, part):
    order = jax.random.permutation(jax.random.fold_in(key, 1), H)
    slow_count = H // 2
    slower = (order < slow_count).astype(jnp.float32)
    unit = jax.random.uniform(jax.random.fold_in(key, 2), (H,), jnp.float32)
    slow_rate = jnp.log(0.2 / (0.02 * SEQUENCE_TOKENS)) + unit * jnp.log(5.0)
    fast_rate = -0.7 + unit * 1.7
    values = slower * slow_rate + (1.0 - slower) * fast_rate
    return values


def block_levels(key, dims, cuts, least, largest):
    level = 1.0
    for dim, parts in cuts:
        draws = jax.random.uniform(jax.random.fold_in(jax.random.fold_in(key, 6), dim), (parts,), jnp.float32, least / len(cuts), largest / len(cuts))
        level = level * jnp.repeat(jnp.exp(draws), dims[dim] // parts).reshape((-1,) + (1,) * (len(dims) - 1 - dim))
    return level


def profile(amount, total, most, lean):
    portions = [(1 << 20) // math.isqrt(rank ** lean) + 1 for rank in range(2, amount + 1)]
    surplus, counts = total - most - (amount - 1), [1] * (amount - 1)
    while surplus > 0:
        candidates = [i for i in range(amount - 1) if counts[i] < most]
        whole, left = sum([portions[i] for i in candidates]), surplus
        for i in candidates:
            addition = min(most - counts[i], max(1, left * portions[i] // whole), surplus)
            counts[i] = counts[i] + addition
            surplus = surplus - addition
    return np.array([most] + counts)


def ragged_sizes(stream_key, number_of, total, most, slope):
    if number_of == 2:
        one = jax.random.randint(stream_key, (), max(1, total - most), min(most, total - 1) + 1)
        return jnp.stack([one, total - one])
    lengths = jnp.asarray(profile(number_of, total, most, slope), jnp.int32)
    pairs = (number_of - 1) // 2
    giver, sink = lengths[1:1 + 2 * pairs:2], lengths[2:2 + 2 * pairs:2]
    margin = jnp.minimum(giver - 1, most - sink)
    moved = jax.random.randint(jax.random.fold_in(stream_key, 1), (pairs,), 0, 1 << 20) % (margin + 1)
    lengths = lengths.at[1:1 + 2 * pairs:2].set(giver - moved).at[2:2 + 2 * pairs:2].set(sink + moved)
    return lengths[jax.random.permutation(jax.random.fold_in(stream_key, 2), number_of)]


def scatter_about(stream_key, shape, width, most, split=(), kind=jnp.bfloat16):
    entries = width * jax.random.normal(stream_key, shape, jnp.float32)
    if split:
        entries = entries * block_levels(stream_key, shape, split, -0.22, 0.18)
    return jnp.clip(entries, -most, most).astype(kind)


def setup_inputs(seed: int = 0) -> dict:
    keys = jax.random.split(jax.random.key(seed), 19)
    hidden = draw_hidden(jax.random.fold_in(keys[18], 71), 0)
    embedding = draw_embedding(jax.random.fold_in(keys[18], 71), 0)
    segments = jnp.searchsorted(jnp.cumsum(ragged_sizes(keys[2], 3, SEQUENCE_TOKENS, 3 * SEQUENCE_TOKENS // 4, 0)), jnp.arange(SEQUENCE_TOKENS), side="right").astype(jnp.int32)
    input_norm_gain = jnp.clip(1.0 + 0.1 * jax.random.normal(keys[3], (D,), jnp.float32), 0.5, 1.5)
    gate_proj = scatter_about(keys[4], (D, DI), D ** -0.5, 0.125, ((1, 8),))
    input_proj = scatter_about(keys[5], (D, DI), D ** -0.5, 0.125, ((1, 8),))
    state_proj = scatter_about(keys[6], (D, 2 * N), D ** -0.5, 0.125)
    step_proj = draw_step_proj(jax.random.fold_in(keys[18], 71), 0)
    step_bias = jnp.clip(-5.0 + 2.0 * jax.random.uniform(keys[8], (H,), jnp.float32) ** block_levels(keys[8], (H,), ((0, 8),), -0.2, 0.2), -5.0, -3.0)
    decay_log = draw_decay_log(jax.random.fold_in(keys[18], 71), 0)
    skip_gain = jnp.clip(0.5 + 1.0 * jax.random.uniform(keys[10], (H,), jnp.float32) ** block_levels(keys[10], (H,), ((0, 8),), -0.2, 0.2), 0.5, 1.5)
    out_gain = jnp.clip(1.0 + 0.1 * jax.random.normal(keys[11], (DI,), jnp.float32), 0.5, 1.5)
    out_proj = scatter_about(keys[12], (DI, D), DI ** -0.5, 0.078125, ((0, 8),))
    attn_gain = jnp.clip(1.0 + 0.1 * jax.random.normal(keys[13], (2 * D,), jnp.float32), 0.5, 1.5)
    query_proj = draw_query_proj(jax.random.fold_in(keys[18], 71), 0)
    key_proj = draw_key_proj(jax.random.fold_in(keys[18], 71), 0)
    value_proj = scatter_about(keys[16], (2 * D, 2 * D), (2 * D) ** -0.5, 0.078125, ((0, 16), (1, 8)))
    attn_out = scatter_about(keys[17], (2 * D, D), (2 * D) ** -0.5, 0.078125, ((0, 8), (1, 16)))
    return dict(hidden=hidden, embedding=embedding, segments=segments, input_norm_gain=input_norm_gain, gate_proj=gate_proj, input_proj=input_proj, state_proj=state_proj, step_proj=step_proj, step_bias=step_bias, decay_log=decay_log, skip_gain=skip_gain, out_gain=out_gain, out_proj=out_proj, attn_gain=attn_gain, query_proj=query_proj, key_proj=key_proj, value_proj=value_proj, attn_out=attn_out)


EPSILON = 1e-05
HIGHEST = lax.Precision.HIGHEST

def normalize(values_in, gain_in):
    widened = values_in.astype(jnp.float32)
    factor = lax.rsqrt(lax.optimization_barrier(jnp.mean(widened * widened, axis=-1, keepdims=True)) + EPSILON)
    return (widened * factor * gain_in).astype(jnp.bfloat16)

def block_terms(inputs_x, steps_dt, rate_vec, b_rows, c_rows, doc_ids, prev_doc):
    block_len = inputs_x.shape[0]
    head_count = steps_dt.shape[1]
    per_head = inputs_x.shape[1] // head_count
    logdecay = steps_dt * rate_vec[None, :]
    running = jnp.cumsum(logdecay, axis=0)
    places = jnp.arange(block_len)
    allowed = (places[:, None] >= places[None, :]) & (doc_ids[:, None] == doc_ids[None, :])
    spread = running.T[:, :, None] - running.T[:, None, :]
    decays = jnp.exp(jnp.where(allowed[None], spread, -1e+30))
    intersection = jnp.dot(c_rows, b_rows.T, precision=HIGHEST)
    scaled_x = inputs_x.reshape(block_len, head_count, per_head) * steps_dt[:, :, None]
    intra_out = jnp.einsum('hts,shp->thp', decays * intersection[None], scaled_x, precision=HIGHEST)
    final_doc = doc_ids[block_len - 1]
    keeping = jnp.exp(running[block_len - 1][None, :] - running) * (doc_ids == final_doc).astype(jnp.float32)[:, None]
    own_state = jnp.einsum('sn,shp->hnp', b_rows, scaled_x * keeping[:, :, None], precision=HIGHEST)
    through = jnp.exp(running[block_len - 1]) * (final_doc == prev_doc).astype(jnp.float32)
    entering = jnp.exp(running) * (doc_ids == prev_doc).astype(jnp.float32)[:, None]
    return (intra_out, own_state, through, entering)

def carried(c_rows, entering, state_in):
    return jnp.einsum('tn,hnp->thp', c_rows, state_in, precision=HIGHEST) * entering[:, :, None]

def reference(hidden, embedding, segments, input_norm_gain, gate_proj, input_proj, state_proj, step_proj, step_bias, decay_log, skip_gain, out_gain, out_proj, attn_gain, query_proj, key_proj, value_proj, attn_out):
    tokens_n = normalize(hidden, input_norm_gain)
    gate_z = jnp.dot(tokens_n, gate_proj, preferred_element_type=jnp.float32)
    inputs_x = jax.nn.silu(jnp.dot(tokens_n, input_proj, preferred_element_type=jnp.float32))
    b_and_c = jax.nn.silu(jnp.dot(tokens_n, state_proj, preferred_element_type=jnp.float32))
    b_rows = b_and_c[:, :N]
    c_rows = b_and_c[:, N:]
    steps_dt = jax.nn.softplus(jnp.dot(tokens_n, step_proj, preferred_element_type=jnp.float32) + step_bias[None, :])
    rate_vec = -jnp.exp(decay_log)
    blocks = SEQUENCE_TOKENS // TOK_DEV

    def advance(carry, pieces):
        state, prev_doc = carry
        piece_x, piece_dt, piece_b, piece_c, document_index = pieces
        intra_out, own_state, through, entering = block_terms(piece_x, piece_dt, rate_vec, piece_b, piece_c, document_index, prev_doc)
        outputs = intra_out + carried(piece_c, entering, state)
        return ((through[:, None, None] * state + own_state, document_index[TOK_DEV - 1]), outputs)
    start_state = jnp.zeros((H, N, HEAD_CHANNELS), jnp.float32)
    final_carry, mixed_y = lax.scan(advance, (start_state, jnp.int32(-1)), (inputs_x.reshape(blocks, TOK_DEV, DI), steps_dt.reshape(blocks, TOK_DEV, H), b_rows.reshape(blocks, TOK_DEV, N), c_rows.reshape(blocks, TOK_DEV, N), segments.reshape(blocks, TOK_DEV)))
    y_full = mixed_y.reshape(SEQUENCE_TOKENS, DI) + inputs_x * jnp.repeat(skip_gain, HEAD_CHANNELS)[None, :]
    gated = y_full * jax.nn.silu(gate_z)
    squares = lax.optimization_barrier(jnp.sum(gated * gated, axis=-1, keepdims=True))
    weighted = (gated * out_gain[None, :]).astype(jnp.bfloat16)
    partial_value = jnp.dot(weighted, out_proj, preferred_element_type=jnp.float32)
    mamba_out = partial_value * lax.rsqrt(squares / DI + EPSILON)
    mixed_h = (hidden.astype(jnp.float32) + mamba_out).astype(jnp.bfloat16)
    joined = jnp.concatenate((mixed_h, embedding), axis=1)
    attention_input = normalize(joined, attn_gain)
    queries = jnp.dot(attention_input, query_proj, preferred_element_type=jnp.float32).astype(jnp.bfloat16)
    keys_all = jnp.dot(attention_input, key_proj, preferred_element_type=jnp.float32).astype(jnp.bfloat16)
    values_all = jnp.dot(attention_input, value_proj, preferred_element_type=jnp.float32).astype(jnp.bfloat16)
    places = jnp.arange(SEQUENCE_TOKENS)
    visible = (places[None, :] <= places[:, None]) & (segments[None, :] == segments[:, None])

    def one_head(trio):
        query_head, key_head, value_head = trio
        scores = jnp.dot(query_head, key_head.T, preferred_element_type=jnp.float32) * AP ** (-0.5)
        scores = jnp.where(visible, scores, -1e+30)
        row_max = lax.optimization_barrier(jnp.max(scores, axis=-1, keepdims=True))
        weights = jnp.where(visible, jnp.exp(scores - row_max), 0.0)
        row_sum = lax.optimization_barrier(jnp.sum(weights, axis=-1, keepdims=True))
        return jnp.dot(weights.astype(jnp.bfloat16), value_head, preferred_element_type=jnp.float32) / row_sum
    contexts = lax.map(one_head, (queries.reshape(SEQUENCE_TOKENS, AH, AP).transpose(1, 0, 2), keys_all.reshape(SEQUENCE_TOKENS, AH, AP).transpose(1, 0, 2), values_all.reshape(SEQUENCE_TOKENS, AH, AP).transpose(1, 0, 2)))
    context = contexts.transpose(1, 0, 2).reshape(SEQUENCE_TOKENS, 2 * D).astype(jnp.bfloat16)
    result = jnp.dot(context, attn_out, preferred_element_type=jnp.float32) + mixed_h.astype(jnp.float32)
    return result.astype(jnp.bfloat16)
```

```python
import functools
import jax
import jax.numpy as jnp
from jax import lax
from jax.experimental import pallas as pl
from jax.experimental.pallas import tpu as pltpu
from jax.sharding import PartitionSpec as P

N = 64
HEAD_CHANNELS = 64
AP = 160
EPSILON = 1e-05
MESH = pl.DeviceIdType.MESH
VMEM = pltpu.VMEM
LIMIT = 62 * 1024 * 1024
F32 = jnp.float32
BF16 = jnp.bfloat16


def normalize(values_in, gain_in):
    widened = values_in.astype(jnp.float32)
    factor = lax.rsqrt(jnp.mean(widened * widened, axis=-1, keepdims=True) + EPSILON)
    return (widened * factor * gain_in).astype(jnp.bfloat16)


def block_terms(inputs_x, steps_dt, rate_vec, b_rows, c_rows, doc_ids, prev_doc):
    block_len = inputs_x.shape[0]
    head_count = steps_dt.shape[1]
    per_head = inputs_x.shape[1] // head_count
    logdecay = steps_dt * rate_vec[None, :]
    running = jnp.cumsum(logdecay, axis=0)
    places = jnp.arange(block_len)
    allowed = (places[:, None] >= places[None, :]) & (doc_ids[:, None] == doc_ids[None, :])
    spread = running.T[:, :, None] - running.T[:, None, :]
    decays = jnp.exp(jnp.where(allowed[None], spread, -1e30))
    intersection = jnp.dot(c_rows, b_rows.T)
    scaled_x = inputs_x.reshape(block_len, head_count, per_head) * steps_dt[:, :, None]
    intra_out = jnp.einsum("hts,shp->thp", decays * intersection[None], scaled_x)
    final_doc = doc_ids[block_len - 1]
    keeping = (
        jnp.exp(running[block_len - 1][None, :] - running)
        * (doc_ids == final_doc).astype(jnp.float32)[:, None]
    )
    own_state = jnp.einsum("sn,shp->hnp", b_rows, scaled_x * keeping[:, :, None])
    through = jnp.exp(running[block_len - 1]) * (final_doc == prev_doc).astype(jnp.float32)
    entering = jnp.exp(running) * (doc_ids == prev_doc).astype(jnp.float32)[:, None]
    return (intra_out, own_state, through, entering)


def carried(c_rows, entering, state_in):
    return jnp.einsum("tn,hnp->thp", c_rows, state_in) * entering[:, :, None]


def greet(peers):
    barrier = pltpu.get_barrier_semaphore()
    for peer in peers:
        pl.semaphore_signal(barrier, inc=1, device_id=peer, device_id_type=MESH)
    pl.semaphore_wait(barrier, len(peers))


def copy_to(src, dst, send, recv, where):
    return pltpu.make_async_remote_copy(
        src_ref=src, dst_ref=dst, send_sem=send, recv_sem=recv,
        device_id=where, device_id_type=MESH,
    )


OFFSETS = ((1, 2), (1, 1), (1, 3), (0, 2), (1, 0), (0, 1), (0, 3))


def chan_peers(s, c):
    half, place = c // 4, lax.rem(c, 4)
    return [lax.rem(half + a, 2) * 4 + lax.rem(place + b, 4) for a, b in OFFSETS]


def chan_sources(s, c):
    half, place = c // 4, lax.rem(c, 4)
    return [lax.rem(half + a, 2) * 4 + lax.rem(place + 4 - b, 4) for a, b in OFFSETS]


def sum_kernel(weighted, squares, proj, hidden, mixed, part, sqbuf, recv, send_sem, recv_sem,
               sq_send, sq_recv, out_send, out_recv):
    s, c = lax.axis_index("seq"), lax.axis_index("chan")
    peers, sources = chan_peers(s, c), chan_sources(s, c)
    greet([(s, p) for p in peers])

    def columns(n, _):
        at = pl.ds(pl.multiple_of(n * 256, 256), 256)
        tile = jnp.dot(weighted[...], proj[:, at], preferred_element_type=F32)
        part[:, :, at] = tile.astype(BF16).reshape(8, 64, 256)
        return 0

    lax.fori_loop(0, 10, columns, 0)
    copies = []
    for i, p in enumerate(peers):
        small = copy_to(squares.at[p], sqbuf.at[i], sq_send.at[i], sq_recv.at[i], (s, p))
        small.start()
        big = copy_to(part.at[p], recv.at[i], send_sem.at[i], recv_sem.at[i], (s, p))
        big.start()
        copies += [small, big]
    for one in copies:
        one.wait_recv()
    rows = pl.ds(pl.multiple_of(c * 64, 64), 64)
    total = squares[c]
    for i in range(7):
        total = total + sqbuf[i]
    column = jnp.broadcast_to(total, (128, 128)).T[:64, :1]
    factor = lax.rsqrt(column / 5120.0 + EPSILON)

    def gather_sum(n, _):
        at = pl.ds(pl.multiple_of(n * 256, 256), 256)
        value = part[c, :, at].astype(F32)
        for i in range(7):
            value = value + recv[i, :, at].astype(F32)
        mixed[c, :, at] = (hidden[rows, at].astype(F32) + value * factor).astype(BF16)
        return 0

    lax.fori_loop(0, 10, gather_sum, 0)
    outs = []
    for i, p in enumerate(peers):
        one = copy_to(mixed.at[c], mixed.at[c], out_send.at[i], out_recv.at[c], (s, p))
        one.start()
        outs.append(one)
    for p in sources:
        copy_to(mixed.at[p], mixed.at[p], out_send.at[0], out_recv.at[p], (s, p)).wait_recv()
    for one in copies + outs:
        one.wait_send()


def sum_and_share(weighted, squares, proj, hidden):
    return pl.pallas_call(
        sum_kernel,
        out_shape=jax.ShapeDtypeStruct((8, 64, 2560), BF16),
        in_specs=[pl.BlockSpec(memory_space=VMEM)] * 4,
        out_specs=pl.BlockSpec(memory_space=VMEM),
        scratch_shapes=[
            VMEM((8, 64, 2560), BF16),
            VMEM((7, 1, 128), F32),
            VMEM((7, 64, 2560), BF16),
            pltpu.SemaphoreType.DMA((7,)),
            pltpu.SemaphoreType.DMA((7,)),
            pltpu.SemaphoreType.DMA((7,)),
            pltpu.SemaphoreType.DMA((7,)),
            pltpu.SemaphoreType.DMA((7,)),
            pltpu.SemaphoreType.DMA((8,)),
        ],
        compiler_params=pltpu.CompilerParams(
            collective_id=0, has_side_effects=True, vmem_limit_bytes=40 * 1024 * 1024
        ),
        cost_estimate=pl.CostEstimate(flops=60_000_000_000, bytes_accessed=9_000_000, transcendentals=0),
        name="sum_and_share",
    )(weighted, squares, proj, hidden)


def seq_parts(s):
    return s // 4, lax.rem(s // 2, 2), lax.rem(s, 2)


def seq_at(z, xl, core):
    return z * 4 + xl * 2 + core


def qkv_kernel(mixed, embedding, gain, wk, wv, wq, k_out, v_out, q_out, weights, rows_in, flat,
               w_sem, z_send, x_send, d_send, f_send, k_recv, v_recv, q_send, q_recv, local_sem):
    s, c = lax.axis_index("seq"), lax.axis_index("chan")
    z, xl, core = seq_parts(s)
    greet([(lax.rem(s + d, 16), c) for d in range(1, 16)])
    loads = []
    for i, w in enumerate((wk, wv, wq)):
        one = pltpu.make_async_copy(w, weights.at[:, pl.ds(i * 640, 640)], w_sem.at[i])
        one.start()
        loads.append(one)

    def norm(p, _):
        at = pl.ds(pl.multiple_of(p * 64, 64), 64)
        top = mixed[p].astype(F32)
        low = embedding[at, :].astype(F32)
        mean = (jnp.sum(top * top, axis=-1, keepdims=True)
                + jnp.sum(low * low, axis=-1, keepdims=True)) / 5120.0
        factor = lax.rsqrt(mean + EPSILON)
        rows_in[at, pl.ds(0, 2560)] = (top * factor * gain[:, pl.ds(0, 2560)]).astype(BF16)
        rows_in[at, pl.ds(2560, 2560)] = (low * factor * gain[:, pl.ds(2560, 2560)]).astype(BF16)
        return 0

    lax.fori_loop(0, 8, norm, 0)

    def tile(n, _):
        at = pl.ds(pl.multiple_of(n * 256, 256), 256)
        value = jnp.dot(rows_in[...], weights[:, at], preferred_element_type=F32)
        flat[at, :] = value.T.astype(BF16)
        return 0

    waits = []

    def first_stage(base, out, recv, lane):
        mine = pltpu.make_async_copy(
            flat.at[pl.ds(pl.multiple_of(base + z * 160, 32), 160), :], out.at[s], local_sem.at[lane])
        mine.start()
        for d in (2, 1, 3):
            to = lax.rem(z + d, 4)
            one = copy_to(
                flat.at[pl.ds(pl.multiple_of(base + to * 160, 32), 160), :], out.at[s],
                z_send.at[lane, d - 1], recv.at[s], (seq_at(to, xl, core), c))
            one.start()
            waits.append(one)
        return mine

    def pass_on(out, recv, lane, d, own):
        block = seq_at(lax.rem(z + 4 - d, 4), xl, core)
        if own is None:
            copy_to(out.at[block], out.at[block], z_send.at[lane, 0], recv.at[block], (block, c)).wait_recv()
        else:
            own.wait()
        across = copy_to(out.at[block], out.at[block], x_send.at[lane, d], recv.at[block],
                         (seq_at(z, 1 - xl, core), c))
        across.start()
        beside = copy_to(out.at[block], out.at[block], d_send.at[lane, d], recv.at[block],
                         (seq_at(z, xl, 1 - core), c))
        beside.start()
        waits.append(across)
        waits.append(beside)

    def relay(out, recv, lane, d):
        block = seq_at(lax.rem(z + 4 - d, 4), 1 - xl, core)
        copy_to(out.at[block], out.at[block], z_send.at[lane, 0], recv.at[block],
                (seq_at(z, 1 - xl, core), c)).wait_recv()
        beside = copy_to(out.at[block], out.at[block], f_send.at[lane, d], recv.at[block],
                         (seq_at(z, xl, 1 - core), c))
        beside.start()
        waits.append(beside)

    def settle(out, recv, d, side):
        block = seq_at(lax.rem(z + 4 - d, 4), side, 1 - core)
        copy_to(out.at[block], out.at[block], z_send.at[0, 0], recv.at[block],
                (seq_at(z, xl, 1 - core), c)).wait_recv()

    loads[0].wait()
    loads[1].wait()
    lax.fori_loop(0, 3, tile, 0)
    own_k = first_stage(0, k_out, k_recv, 0)
    pass_on(k_out, k_recv, 0, 0, own_k)
    lax.fori_loop(3, 5, tile, 0)
    own_v = first_stage(640, v_out, v_recv, 1)
    pass_on(v_out, v_recv, 1, 0, own_v)
    loads[2].wait()
    lax.fori_loop(5, 7, tile, 0)
    last = pl.ds(1792, 128)
    flat[last, :] = jnp.dot(rows_in[...], weights[:, last], preferred_element_type=F32).T.astype(BF16)
    quarter = xl * 2 + core
    for d in range(16):
        to = lax.rem(s + d, 16)
        piece = flat.at[pl.ds(pl.multiple_of(1280 + (to // 4) * 160, 32), 160),
                        pl.ds(pl.multiple_of(lax.rem(to, 4) * 128, 128), 128)]
        if d == 0:
            own_q = pltpu.make_async_copy(piece, q_out.at[s], local_sem.at[2])
            own_q.start()
        else:
            one = copy_to(piece, q_out.at[s], q_send.at[d - 1], q_recv.at[s], (to, c))
            one.start()
            waits.append(one)
    for d in (1, 3, 2):
        pass_on(k_out, k_recv, 0, d, None)
    relay(k_out, k_recv, 0, 0)
    for d in (1, 3, 2):
        pass_on(v_out, v_recv, 1, d, None)
    relay(v_out, v_recv, 1, 0)
    for d in (1, 3, 2):
        relay(k_out, k_recv, 0, d)
    for d in (1, 3, 2):
        relay(v_out, v_recv, 1, d)
    for d in (0, 1, 3, 2):
        for side in (0, 1):
            settle(k_out, k_recv, d, side)
            settle(v_out, v_recv, d, side)
    own_q.wait()
    for d in range(1, 16):
        block = lax.rem(s + d, 16)
        copy_to(q_out.at[block], q_out.at[block], q_send.at[0], q_recv.at[block], (block, c)).wait_recv()
    for one in waits:
        one.wait_send()


def project(mixed, embedding, gain, wk, wv, wq):
    dma = pltpu.SemaphoreType.DMA
    vm, anyw = pl.BlockSpec(memory_space=VMEM), pl.BlockSpec(memory_space=pl.ANY)
    return pl.pallas_call(
        qkv_kernel,
        out_shape=(
            jax.ShapeDtypeStruct((16, 160, 512), BF16),
            jax.ShapeDtypeStruct((16, 160, 512), BF16),
            jax.ShapeDtypeStruct((16, 160, 128), BF16),
        ),
        in_specs=[vm, vm, vm, anyw, anyw, anyw],
        out_specs=(vm, vm, vm),
        scratch_shapes=[
            VMEM((5120, 1920), BF16),
            VMEM((512, 5120), BF16),
            VMEM((1920, 512), BF16),
            dma((3,)),
            dma((2, 3)),
            dma((2, 4)),
            dma((2, 4)),
            dma((2, 4)),
            dma((16,)),
            dma((16,)),
            dma((15,)),
            dma((16,)),
            dma((3,)),
        ],
        compiler_params=pltpu.CompilerParams(
            collective_id=1, has_side_effects=True, vmem_limit_bytes=LIMIT
        ),
        cost_estimate=pl.CostEstimate(flops=60_000_000_000, bytes_accessed=30_000_000, transcendentals=0),
        name="project",
    )(mixed, embedding, gain, wk, wv, wq)


def attend_kernel(ends, q_in, k_in, v_in, out):
    quarter = lax.rem(lax.axis_index("seq"), 4)
    i = pl.program_id(0)
    first, second = ends[0], ends[1]
    queries = jnp.concatenate(
        [q_in[2 * i].astype(F32).T, q_in[2 * i + 1].astype(F32).T], axis=0
    ).astype(BF16)
    row = lax.broadcasted_iota(jnp.int32, (256, 1), 0)
    place = i * 1024 + quarter * 128 + row + jnp.where(row >= 128, 384, 0)

    def start_of(p):
        return jnp.where(p >= second, second, jnp.where(p >= first, first, 0))

    begin = start_of(place)
    low_place = i * 1024 + quarter * 128
    top_begin = start_of(low_place + 512 + 127)
    low_begin = start_of(low_place)
    lowest = low_begin // 512
    scale = (AP ** -0.5) * 1.4426950408889634

    def step(b, carry, masked):
        top, total, acc = carry
        scores = jnp.dot(queries, k_in[b], preferred_element_type=F32)
        if masked:
            key = b * 512 + lax.broadcasted_iota(jnp.int32, (256, 512), 1)
            visible = (key >= begin) & (key <= place)
            scores = jnp.where(visible, scores, -1e30)
        new_top = jnp.maximum(top, jnp.max(scores, axis=-1, keepdims=True))
        weights = jnp.exp2((scores - new_top) * scale)
        if masked:
            weights = jnp.where(visible, weights, 0.0)
        keep = jnp.exp2((top - new_top) * scale)
        total = total * keep + jnp.sum(weights, axis=-1, keepdims=True)
        acc = acc * keep + lax.dot_general(
            weights.astype(BF16), v_in[b], (((1,), (1,)), ((), ())), preferred_element_type=F32
        )
        return new_top, total, acc

    carry = (jnp.full((256, 1), -1e30, F32), jnp.zeros((256, 1), F32), jnp.zeros((256, AP), F32))
    plain_from = jnp.minimum((top_begin + 511) // 512, 2 * i)
    carry = lax.fori_loop(lowest, plain_from, lambda b, t: step(b, t, True), carry)
    carry = lax.fori_loop(jnp.maximum(lowest, plain_from), 2 * i, lambda b, t: step(b, t, False), carry)
    carry = lax.fori_loop(jnp.maximum(lowest, 2 * i), 2 * i + 2, lambda b, t: step(b, t, True), carry)
    top, total, acc = carry
    context = (acc / total).T.astype(BF16)
    out[0] = context[:, :128]
    out[1] = context[:, 128:]


def attend(ends, q_in, k_in, v_in):
    vm = pl.BlockSpec(memory_space=VMEM)
    return pl.pallas_call(
        attend_kernel,
        out_shape=jax.ShapeDtypeStruct((16, 160, 128), BF16),
        grid=(8,),
        in_specs=[pl.BlockSpec(memory_space=pltpu.SMEM), vm, vm, vm],
        out_specs=pl.BlockSpec((2, 160, 128), lambda i: (i, 0, 0)),
        compiler_params=pltpu.CompilerParams(vmem_limit_bytes=40 * 1024 * 1024),
        cost_estimate=pl.CostEstimate(flops=10_000_000_000, bytes_accessed=6_000_000, transcendentals=0),
        name="attend",
    )(ends, q_in, k_in, v_in)


def finish_kernel(ctx, proj_t, out, gathered, part, recv, in_send, in_recv, send_sem, recv_sem, local_sem):
    s, c = lax.axis_index("seq"), lax.axis_index("chan")
    peers, sources = chan_peers(s, c), chan_sources(s, c)
    greet([(s, p) for p in peers] + [(lax.rem(s + d, 16), c) for d in range(1, 16)])
    z = s // 4
    lanes = pl.ds(pl.multiple_of(lax.rem(s, 4) * 128, 128), 128)
    waits = []
    for d in range(16):
        to = lax.rem(s + d, 16)
        where = gathered.at[pl.ds(pl.multiple_of(z * 160, 32), 160), lanes]
        if d == 0:
            own = pltpu.make_async_copy(ctx.at[s], where, local_sem.at[0])
            own.start()
        else:
            one = copy_to(ctx.at[to], where, in_send.at[d - 1], in_recv.at[s], (to, c))
            one.start()
            waits.append(one)
    own.wait()
    for d in range(1, 16):
        block = lax.rem(s + d, 16)
        where = gathered.at[pl.ds(pl.multiple_of((block // 4) * 160, 32), 160),
                            pl.ds(pl.multiple_of(lax.rem(block, 4) * 128, 128), 128)]
        copy_to(ctx.at[0], where, in_send.at[0], in_recv.at[block], (block, c)).wait_recv()
    copies = []
    for i, p in enumerate(peers):
        at = pl.ds(pl.multiple_of(p * 320, 32), 320)
        part[p] = jnp.dot(proj_t[at, :], gathered[...], preferred_element_type=F32).astype(BF16)
        one = copy_to(part.at[p], recv.at[i], send_sem.at[i], recv_sem.at[i], (s, p))
        one.start()
        copies.append(one)
    at = pl.ds(pl.multiple_of(c * 320, 32), 320)
    value = jnp.dot(proj_t[at, :], gathered[...], preferred_element_type=F32)
    for i in (6, 5, 4, 3, 2, 1, 0):
        copies[i].wait_recv()
        value = value + recv[i].astype(F32)
    out[...] = value.T
    for one in waits + copies:
        one.wait_send()


def finish(ctx, proj_t):
    dma = pltpu.SemaphoreType.DMA
    vm = pl.BlockSpec(memory_space=VMEM)
    return pl.pallas_call(
        finish_kernel,
        out_shape=jax.ShapeDtypeStruct((512, 320), F32),
        in_specs=[vm, vm],
        out_specs=vm,
        scratch_shapes=[
            VMEM((640, 512), BF16),
            VMEM((8, 320, 512), BF16),
            VMEM((7, 320, 512), BF16),
            dma((15,)),
            dma((16,)),
            dma((7,)),
            dma((7,)),
            dma((1,)),
        ],
        compiler_params=pltpu.CompilerParams(
            collective_id=2, has_side_effects=True, vmem_limit_bytes=40 * 1024 * 1024
        ),
        cost_estimate=pl.CostEstimate(flops=50_000_000_000, bytes_accessed=6_000_000, transcendentals=0),
        name="finish",
    )(ctx, proj_t)


def local(
    hidden,
    embedding,
    segments,
    input_norm_gain,
    gate_proj,
    input_proj,
    state_proj,
    step_proj,
    step_bias,
    decay_log,
    skip_gain,
    out_gain,
    out_proj,
    attn_gain,
    query_proj,
    key_proj,
    value_proj,
    attn_out,
):
    tok_rows = hidden.shape[0]
    seq_index = lax.axis_index("seq")
    chan_index = lax.axis_index("chan")
    row_start = seq_index * tok_rows
    wk, wv, wq = (lax.all_gather(w, "seq", axis=0, tiled=True) for w in (key_proj, value_proj, query_proj))
    proj_t = lax.all_gather(attn_out.T, "seq", axis=0, tiled=True)
    ends = jnp.stack([jnp.sum((segments < 1).astype(jnp.int32)), jnp.sum((segments < 2).astype(jnp.int32))])
    tokens_n = normalize(hidden, input_norm_gain)
    gate_z = jnp.dot(tokens_n, gate_proj, preferred_element_type=jnp.float32)
    inputs_x = jax.nn.silu(jnp.dot(tokens_n, input_proj, preferred_element_type=jnp.float32))
    b_and_c = jax.nn.silu(jnp.dot(tokens_n, state_proj, preferred_element_type=jnp.float32))
    b_rows = b_and_c[:, :N]
    c_rows = b_and_c[:, N:]
    steps_dt = jax.nn.softplus(
        jnp.dot(tokens_n, step_proj, preferred_element_type=jnp.float32) + step_bias[None, :]
    )
    rate_vec = -jnp.exp(decay_log)
    doc_ids = lax.dynamic_slice_in_dim(segments, row_start, tok_rows)
    before = lax.dynamic_slice_in_dim(segments, jnp.maximum(row_start - 1, 0), 1)[0]
    prev_doc = jnp.where(seq_index > 0, before, -1)
    intra_out, own_state, through, entering = block_terms(
        inputs_x, steps_dt, rate_vec, b_rows, c_rows, doc_ids, prev_doc
    )
    packed = jnp.concatenate(
        [own_state, jnp.broadcast_to(through[:, None, None], (10, 1, HEAD_CHANNELS))], axis=1
    )
    everything = lax.all_gather(packed, "seq", axis=0)
    all_states, all_through = everything[:, :, :N], everything[:, :, N, 0]
    spots = jnp.arange(16)
    between = (spots[None, :] > spots[:, None]) & (spots[None, :] < seq_index)
    factors = jnp.prod(jnp.where(between[:, :, None], all_through[None], 1.0), axis=1)
    factors = jnp.where((spots < seq_index)[:, None], factors, 0.0)
    state_in = jnp.sum(all_states * factors[:, :, None, None], axis=0)
    mixed_y = intra_out + carried(c_rows, entering, state_in)
    y_full = (
        mixed_y.reshape(tok_rows, -1) + inputs_x * jnp.repeat(skip_gain, HEAD_CHANNELS)[None, :]
    )
    gated = y_full * jax.nn.silu(gate_z)
    squares = jnp.sum(gated * gated, axis=-1)
    weighted = (gated * out_gain[None, :]).astype(jnp.bfloat16)
    squares = jnp.pad(squares.reshape(8, 1, 64), ((0, 0), (0, 0), (0, 64)))
    mixed = sum_and_share(weighted, squares, out_proj, hidden)
    k_all, v_all, q_all = project(mixed, embedding, attn_gain[None, :], wk, wv, wq)
    ctx = attend(ends, q_all, k_all, v_all)
    out_share = finish(ctx, proj_t)
    own_mixed = lax.dynamic_slice_in_dim(mixed.reshape(512, 2560), chan_index * 320, 320, 1)
    return (out_share + own_mixed.astype(jnp.float32)).astype(jnp.bfloat16)


def solution(mesh):
    in_specs = (
        P("seq", None),
        P("seq", None),
        P(),
        P(),
        P(None, "chan"),
        P(None, "chan"),
        P(),
        P(None, "chan"),
        P("chan"),
        P("chan"),
        P("chan"),
        P("chan"),
        P("chan", None),
        P(),
        P("seq", "chan"),
        P("seq", "chan"),
        P("seq", "chan"),
        P("chan", "seq"),
    )
    out_specs = P("seq", "chan")
    return jax.shard_map(local, mesh=mesh, in_specs=in_specs, out_specs=out_specs, check_vma=False)
```

```python
import jax
import jax.numpy as jnp
from jax import lax
from jax.experimental import pallas as pl
from jax.experimental.pallas import tpu as pltpu
from jax.sharding import PartitionSpec as P

N = 64
HEAD_CHANNELS = 64
AP = 160
EPSILON = 1e-05
MESH = pl.DeviceIdType.MESH
VMEM = pltpu.VMEM
LIMIT = 62 * 1024 * 1024
F32 = jnp.float32
BF16 = jnp.bfloat16


def greet(peers):
    barrier = pltpu.get_barrier_semaphore()
    for peer in peers:
        pl.semaphore_signal(barrier, inc=1, device_id=peer, device_id_type=MESH)
    pl.semaphore_wait(barrier, len(peers))


def copy_to(src, dst, send, recv, where):
    return pltpu.make_async_remote_copy(
        src_ref=src, dst_ref=dst, send_sem=send, recv_sem=recv,
        device_id=where, device_id_type=MESH,
    )


OFFSETS = ((1, 2), (1, 1), (1, 3), (0, 2), (1, 0), (0, 1), (0, 3))


def chan_peers(s, c):
    half, place = c // 4, lax.rem(c, 4)
    return [lax.rem(half + a, 2) * 4 + lax.rem(place + b, 4) for a, b in OFFSETS]


def chan_sources(s, c):
    half, place = c // 4, lax.rem(c, 4)
    return [lax.rem(half + a, 2) * 4 + lax.rem(place + 4 - b, 4) for a, b in OFFSETS]


def seq_parts(s):
    return s // 4, lax.rem(s // 2, 2), lax.rem(s, 2)


def seq_at(z, xl, core):
    return z * 4 + xl * 2 + core


def start_of(place, first, second):
    return jnp.where(place >= second, second, jnp.where(place >= first, first, 0))


def silu(v):
    return v / (1.0 + jnp.exp(-v))


def front_kernel(ends, hidden, norm_gain, input_w, gate_w, state_w, small, out_w, embedding, attn_gain,
                 wk, wv, wq, p_in,
                 mixed, k_out, v_out, q_out, p_out,
                 hid, iw, gw, sw, ow, w, rows_in, part, recv, flat_t, run_e, xs, ys, states, tx, rx, planes,
                 run_rows, run_cols, step_e, bc_rows, bc_cols, pb, sq_all, sq_cols, weighted,
                 load_sem, w_send, w_recv, p_send, p_recv, st_send, st_recv,
                 sq_send, sq_recv, rs_send, rs_recv, ag_send, ag_recv,
                 z_send, x_send, d_send, f_send, k_recv, v_recv, q_send, q_recv, local_sem):
    s, c = lax.axis_index("seq"), lax.axis_index("chan")
    z, xl, core = seq_parts(s)
    peers, sources = chan_peers(s, c), chan_sources(s, c)
    up, down, far = lax.rem(z + 1, 4), lax.rem(z + 3, 4), lax.rem(z + 2, 4)
    waits = []

    def load(i, src, dst):
        one = pltpu.make_async_copy(src, dst, load_sem.at[i])
        one.start()
        return one

    own_rows = pl.ds(pl.multiple_of(s * 320, 64), 320)
    w_loads = [load(i, src, w.at[own_rows, pl.ds(i * 640, 640)]) for i, src in enumerate((wk, wv, wq))]
    l_hid = load(3, hidden, hid)
    l_sw = load(4, state_w, sw)
    l_iw = load(5, input_w, iw)
    l_pb = load(6, p_in, pb)
    l_gw = load(7, gate_w, gw)
    l_ow = load(8, out_w, ow)
    greet([(s, p) for p in peers] + [(lax.rem(s + d, 16), c) for d in range(1, 16)])

    used = [0, 0]

    def w_rows(block, half):
        return w.at[pl.ds(pl.multiple_of(block * 320 + half * 160, 32), 160), :]

    def w_to(block, half, to):
        rows = w_rows(block, half)
        one = copy_to(rows, rows, w_send.at[used[0]], w_recv.at[block, half], (to, c))
        used[0] += 1
        one.start()
        waits.append(one)

    def w_wait(block, half):
        rows = w_rows(block, half)
        copy_to(rows, rows, w_send.at[0], w_recv.at[block, half], (seq_at(z, xl, 1 - core), c)).wait_recv()

    def p_rows(block):
        return p_out.at[pl.ds(pl.multiple_of(block * 160, 32), 160), :]

    def p_to(block, to, src=None):
        rows = p_rows(block)
        one = copy_to(rows if src is None else src, rows, p_send.at[used[1]], p_recv.at[block], (to, c))
        used[1] += 1
        one.start()
        waits.append(one)

    def p_wait(block):
        rows = p_rows(block)
        copy_to(rows, rows, p_send.at[0], p_recv.at[block], (seq_at(z, xl, 1 - core), c)).wait_recv()

    sibling = seq_at(z, xl, 1 - core)

    def w_first(half):
        w_to(s, half, seq_at(z, 1 - xl, core))
        w_to(s, half, seq_at(up, xl, core))
        w_to(s, half, seq_at(down, xl, core))
        w_to(s, half, sibling)

    def w_second():
        block = seq_at(z, 1 - xl, core)
        for half in (0, 1):
            w_wait(block, half)
            w_to(block, half, seq_at(up, xl, core))
            w_to(block, half, seq_at(down, xl, core))
            w_to(block, half, sibling)
        for half in (0, 1):
            w_wait(seq_at(down, xl, core), half)
            w_wait(seq_at(up, xl, core), half)
        w_to(seq_at(down, xl, core), 0, seq_at(up, xl, core))
        w_to(seq_at(up, xl, core), 1, seq_at(down, xl, core))
        for half in (0, 1):
            w_to(seq_at(down, xl, core), half, sibling)
            w_to(seq_at(up, xl, core), half, sibling)

    def w_third():
        for half in (0, 1):
            w_wait(seq_at(down, 1 - xl, core), half)
            w_wait(seq_at(up, 1 - xl, core), half)
        w_to(seq_at(down, 1 - xl, core), 0, seq_at(up, xl, core))
        w_to(seq_at(up, 1 - xl, core), 1, seq_at(down, xl, core))
        for half in (0, 1):
            w_to(seq_at(down, 1 - xl, core), half, sibling)
            w_to(seq_at(up, 1 - xl, core), half, sibling)
        for half in (0, 1):
            w_wait(seq_at(far, xl, core), half)
            w_to(seq_at(far, xl, core), half, sibling)

    def w_last():
        for half in (0, 1):
            w_wait(seq_at(far, 1 - xl, core), half)
            w_to(seq_at(far, 1 - xl, core), half, sibling)
        for zz in range(4):
            for xx in range(2):
                for half in (0, 1):
                    w_wait(seq_at(zz, xx, 1 - core), half)

    def p_first():
        for to in (seq_at(z, 1 - xl, core), seq_at(up, xl, core), seq_at(down, xl, core), sibling):
            p_to(s, to, pb)

    def p_second():
        block = seq_at(z, 1 - xl, core)
        p_wait(block)
        for to in (seq_at(up, xl, core), seq_at(down, xl, core), sibling):
            p_to(block, to)
        p_wait(seq_at(down, xl, core))
        p_wait(seq_at(up, xl, core))
        p_to(seq_at(down, xl, core), seq_at(up, xl, core))
        p_to(seq_at(down, xl, core), sibling)
        p_to(seq_at(up, xl, core), sibling)

    def p_third():
        p_wait(seq_at(down, 1 - xl, core))
        p_wait(seq_at(up, 1 - xl, core))
        p_to(seq_at(down, 1 - xl, core), seq_at(up, xl, core))
        p_to(seq_at(down, 1 - xl, core), sibling)
        p_to(seq_at(up, 1 - xl, core), sibling)
        p_wait(seq_at(far, xl, core))
        p_to(seq_at(far, xl, core), sibling)

    def p_last():
        p_wait(seq_at(far, 1 - xl, core))
        p_to(seq_at(far, 1 - xl, core), sibling)
        for zz in range(4):
            for xx in range(2):
                p_wait(seq_at(zz, xx, 1 - core))

    for one in w_loads:
        one.wait()
    w_first(0)

    first, second = ends[0], ends[1]
    base = s * 512
    l_hid.wait()

    def norm_first(p, _):
        at = pl.ds(pl.multiple_of(p * 64, 64), 64)
        value = hid[p].astype(F32)
        factor = lax.rsqrt(jnp.sum(value * value, axis=-1, keepdims=True) / 2560.0 + EPSILON)
        rows_in[at, pl.ds(0, 2560)] = (value * factor * norm_gain[...]).astype(BF16)
        return 0

    lax.fori_loop(0, 8, norm_first, 0)
    tokens = rows_in.at[:, pl.ds(0, 2560)]
    l_sw.wait()
    both = jnp.dot(tokens[...], sw[...], preferred_element_type=F32)
    bc = silu(both[:, :128])
    bc_rows[...] = bc.astype(BF16)
    bc_cols[...] = bc.T.astype(BF16)
    logits = both[:, 128:] + small[0:1, :128]
    steps = jnp.maximum(logits, 0.0) + jnp.log1p(jnp.exp(-jnp.abs(logits)))
    rate = -jnp.exp(small[1:2, :128])
    lower = (lax.broadcasted_iota(jnp.int32, (512, 512), 0)
             >= lax.broadcasted_iota(jnp.int32, (512, 512), 1)).astype(F32)
    running = jnp.dot(lower, steps * rate, preferred_element_type=F32, precision=lax.Precision.HIGHEST)
    spread = (lax.broadcasted_iota(jnp.int32, (128, 640), 1) // 64
              == lax.broadcasted_iota(jnp.int32, (128, 640), 0)).astype(F32)
    run_rows[...] = running
    run_cols[...] = running.T
    wide_steps = jnp.dot(steps, spread, preferred_element_type=F32, precision=lax.Precision.HIGHEST)
    run_e[...] = jnp.dot(running, spread, preferred_element_type=F32, precision=lax.Precision.HIGHEST)
    step_e[...] = wide_steps
    l_iw.wait()

    def input_tile(n, width):
        at = pl.ds(n, width)
        xs[:, at] = silu(jnp.dot(tokens[...], iw[:, at], preferred_element_type=F32))
        step_e[:, at] = xs[:, at] * step_e[:, at]

    input_tile(0, 256)
    input_tile(256, 256)
    input_tile(512, 128)

    states[0] = jnp.zeros((64, 640), F32)
    total = None
    for k in range(4):
        rows = slice(k * 128, k * 128 + 128)
        end = run_e[k * 128 + 127:k * 128 + 128, :]
        begin_end = start_of(base + k * 128 + 127, first, second)
        place = base + k * 128 + lax.broadcasted_iota(jnp.int32, (128, 1), 0)
        keep = jnp.where(place >= begin_end, jnp.exp(end - run_e[rows, :]), 0.0)
        own = jnp.dot(bc_cols[:64, rows], (step_e[rows, :] * keep).astype(BF16), preferred_element_type=F32)
        gap = end if k == 0 else end - run_e[k * 128 - 1:k * 128, :]
        through = jnp.where(base + k * 128 - 1 >= begin_end, jnp.exp(gap), 0.0)
        if k == 0:
            total = through
            states[1] = own
        else:
            total = total * through
            if k < 3:
                states[k + 1] = through * states[k] + own
            else:
                tx[0, 0:64, :] = through * states[k] + own
    tx[0, 64:72, :] = jnp.broadcast_to(total, (8, 640))

    def state_to(src, dst, i, to):
        one = copy_to(src, dst, st_send.at[i], st_recv.at[i], (to, c))
        one.start()
        waits.append(one)
        return one

    one = state_to(tx.at[0], rx.at[0], 0, sibling)
    one.wait_recv()
    mine_s, mine_t = tx[0, 0:64, :], tx[0, 64:65, :]
    its_s, its_t = rx[0, 0:64, :], rx[0, 64:65, :]
    s0, t0 = jnp.where(core == 0, mine_s, its_s), jnp.where(core == 0, mine_t, its_t)
    s1, t1 = jnp.where(core == 0, its_s, mine_s), jnp.where(core == 0, its_t, mine_t)
    tx[1, 0:64, :] = t1 * s0 + s1
    tx[1, 64:72, :] = jnp.broadcast_to(t0 * t1, (8, 640))
    one = state_to(tx.at[1], rx.at[1], 1, seq_at(z, 1 - xl, core))

    def chunk(k, _):
        at = pl.ds(pl.multiple_of(k * 128, 128), 128)
        place = base + k * 128 + lax.broadcasted_iota(jnp.int32, (128, 1), 0)
        key = base + k * 128 + lax.broadcasted_iota(jnp.int32, (1, 128), 1)
        begin = start_of(place, first, second)
        allowed = (key >= begin) & (key <= place)
        cross = jnp.dot(bc_rows[at, 64:128], bc_cols[0:64, at], preferred_element_type=F32)
        cross = jnp.where(allowed, cross, 0.0)
        lane = lax.broadcasted_iota(jnp.int32, (128, 128), 1)
        for pair in range(5):
            lanes = pl.ds(pair * 128, 128)
            scaled = step_e[at, lanes].astype(BF16)
            halves = []
            for h in (2 * pair, 2 * pair + 1):
                gap = run_rows[at, h:h + 1] - run_cols[h:h + 1, at]
                decay = jnp.exp(jnp.where(allowed, gap, -1e30))
                halves.append(jnp.dot((decay * cross).astype(BF16), scaled, preferred_element_type=F32))
            ys[at, lanes] = jnp.where(lane < 64, halves[0], halves[1])
        return 0

    lax.fori_loop(0, 2, chunk, 0)
    one.wait_recv()
    mine_s, mine_t = tx[1, 0:64, :], tx[1, 64:65, :]
    its_s, its_t = rx[1, 0:64, :], rx[1, 64:65, :]
    q0, u0 = jnp.where(xl == 0, mine_s, its_s), jnp.where(xl == 0, mine_t, its_t)
    q1, u1 = jnp.where(xl == 0, its_s, mine_s), jnp.where(xl == 0, its_t, mine_t)
    planes[z, 0:64, :] = u1 * q0 + q1
    planes[z, 64:72, :] = jnp.broadcast_to(u0 * u1, (8, 640))
    for d in (2, 1, 3):
        to = lax.rem(z + d, 4)
        one = copy_to(planes.at[z], planes.at[z], st_send.at[1 + d], st_recv.at[2 + z], (seq_at(to, xl, core), c))
        one.start()
        waits.append(one)
    w_first(1)
    l_pb.wait()
    own_p = pltpu.make_async_copy(pb, p_rows(s), local_sem.at[3])
    own_p.start()
    lax.fori_loop(2, 4, chunk, 0)

    for k in range(1, 4):
        rows = slice(k * 128, k * 128 + 128)
        place = base + k * 128 + lax.broadcasted_iota(jnp.int32, (128, 1), 0)
        begin = start_of(place, first, second)
        enter = jnp.where(base + k * 128 - 1 >= begin,
                          jnp.exp(run_e[rows, :] - run_e[k * 128 - 1:k * 128, :]), 0.0)
        ys[rows, :] += enter * jnp.dot(bc_rows[rows, 64:128], states[k].astype(BF16), preferred_element_type=F32)

    l_gw.wait()
    for n, width in ((0, 256), (256, 256), (512, 128)):
        at = pl.ds(n, width)
        step_e[:, at] = silu(jnp.dot(tokens[...], gw[:, at], preferred_element_type=F32))

    enter_s = jnp.zeros((64, 640), F32)
    for d in (1, 2, 3):
        zz = lax.rem(z + d, 4)
        copy_to(planes.at[zz], planes.at[zz], st_send.at[0], st_recv.at[2 + zz], (seq_at(zz, xl, core), c)).wait_recv()
    for zz in range(3):
        enter_s = jnp.where(zz < z, planes[zz, 64:65, :] * enter_s + planes[zz, 0:64, :], enter_s)
    first_s = jnp.where(xl == 0, tx[1, 0:64, :], rx[1, 0:64, :])
    first_t = jnp.where(xl == 0, tx[1, 64:65, :], rx[1, 64:65, :])
    enter_s = jnp.where(xl == 1, first_t * enter_s + first_s, enter_s)
    first_s = jnp.where(core == 0, tx[0, 0:64, :], rx[0, 0:64, :])
    first_t = jnp.where(core == 0, tx[0, 64:65, :], rx[0, 64:65, :])
    enter_s = jnp.where(core == 1, first_t * enter_s + first_s, enter_s)
    states[0] = enter_s

    def gating(k, _):
        at = pl.ds(pl.multiple_of(k * 128, 128), 128)
        place = base + k * 128 + lax.broadcasted_iota(jnp.int32, (128, 1), 0)
        begin = start_of(place, first, second)
        enter = jnp.where(base - 1 >= begin, jnp.exp(run_e[at, :]), 0.0)
        y = ys[at, :] + enter * jnp.dot(bc_rows[at, 64:128], states[0].astype(BF16), preferred_element_type=F32)
        y = y + xs[at, :] * small[2:3, :]
        gated = y * step_e[at, :]
        sq_cols[at, :] = jnp.broadcast_to(jnp.sum(gated * gated, axis=-1, keepdims=True), (128, 128))
        weighted[at, :] = (gated * small[3:4, :]).astype(BF16)
        return 0

    lax.fori_loop(0, 4, gating, 0)
    sq_all[c] = sq_cols[...].T[0:1, :]
    l_ow.wait()

    def columns(n, _):
        at = pl.ds(pl.multiple_of(n * 256, 256), 256)
        tile = jnp.dot(weighted[...], ow[:, at], preferred_element_type=F32)
        part[:, :, at] = tile.astype(BF16).reshape(8, 64, 256)
        return 0

    lax.fori_loop(0, 10, columns, 0)
    copies = []
    for i, p in enumerate(peers):
        few = copy_to(sq_all.at[c], sq_all.at[c], sq_send.at[i], sq_recv.at[c], (s, p))
        few.start()
        waits.append(few)
        big = copy_to(part.at[p], recv.at[i], rs_send.at[i], rs_recv.at[i], (s, p))
        big.start()
        copies.append(big)
    w_second()
    p_first()
    for i, p in enumerate(sources):
        copy_to(sq_all.at[p], sq_all.at[p], sq_send.at[0], sq_recv.at[p], (s, p)).wait_recv()
    for one in copies:
        one.wait_recv()
    own64 = pl.ds(pl.multiple_of(c * 64, 64), 64)
    squares = sq_all[0]
    for i in range(1, 8):
        squares = squares + sq_all[i]
    sq_cols[...] = jnp.broadcast_to(squares, (128, 512)).T
    factor = lax.rsqrt(sq_cols[own64, 0:1] / 5120.0 + EPSILON)

    def gather_sum(n, _):
        at = pl.ds(pl.multiple_of(n * 256, 256), 256)
        value = part[c, :, at].astype(F32)
        for i in range(7):
            value = value + recv[i, :, at].astype(F32)
        mixed[c, :, at] = (hid[c, :, at].astype(F32) + value * factor).astype(BF16)
        return 0

    lax.fori_loop(0, 10, gather_sum, 0)
    for i, p in enumerate(peers):
        one = copy_to(mixed.at[c], mixed.at[c], ag_send.at[i], ag_recv.at[c], (s, p))
        one.start()
        waits.append(one)
    for one in copies:
        one.wait_send()
    l_emb = load(9, embedding, part)
    w_third()
    p_second()
    l_emb.wait()
    for p in sources:
        copy_to(mixed.at[p], mixed.at[p], ag_send.at[0], ag_recv.at[p], (s, p)).wait_recv()

    def norm_second(p, _):
        at = pl.ds(pl.multiple_of(p * 64, 64), 64)
        top = mixed[p].astype(F32)
        low = part[p].astype(F32)
        mean = (jnp.sum(top * top, axis=-1, keepdims=True)
                + jnp.sum(low * low, axis=-1, keepdims=True)) / 5120.0
        scale = lax.rsqrt(mean + EPSILON)
        rows_in[at, pl.ds(0, 2560)] = (top * scale * attn_gain[:, pl.ds(0, 2560)]).astype(BF16)
        rows_in[at, pl.ds(2560, 2560)] = (low * scale * attn_gain[:, pl.ds(2560, 2560)]).astype(BF16)
        return 0

    lax.fori_loop(0, 8, norm_second, 0)
    w_last()

    def project_tile(n, _):
        at = pl.ds(pl.multiple_of(n * 256, 256), 256)
        value = jnp.dot(rows_in[...], w[:, at], preferred_element_type=F32)
        flat_t[at, :] = value.T.astype(BF16)
        return 0

    def first_stage(base, out, recv, lane):
        mine = pltpu.make_async_copy(
            flat_t.at[pl.ds(pl.multiple_of(base + z * 160, 32), 160), :], out.at[s], local_sem.at[lane])
        mine.start()
        for d in (2, 1, 3):
            to = lax.rem(z + d, 4)
            one = copy_to(
                flat_t.at[pl.ds(pl.multiple_of(base + to * 160, 32), 160), :], out.at[s],
                z_send.at[lane, d - 1], recv.at[s], (seq_at(to, xl, core), c))
            one.start()
            waits.append(one)
        return mine

    def pass_on(out, recv, lane, d, own):
        block = seq_at(lax.rem(z + 4 - d, 4), xl, core)
        if own is None:
            copy_to(out.at[block], out.at[block], z_send.at[lane, 0], recv.at[block], (block, c)).wait_recv()
        else:
            own.wait()
        across = copy_to(out.at[block], out.at[block], x_send.at[lane, d], recv.at[block],
                         (seq_at(z, 1 - xl, core), c))
        across.start()
        beside = copy_to(out.at[block], out.at[block], d_send.at[lane, d], recv.at[block],
                         (seq_at(z, xl, 1 - core), c))
        beside.start()
        waits.append(across)
        waits.append(beside)

    def relay(out, recv, lane, d):
        block = seq_at(lax.rem(z + 4 - d, 4), 1 - xl, core)
        copy_to(out.at[block], out.at[block], z_send.at[lane, 0], recv.at[block],
                (seq_at(z, 1 - xl, core), c)).wait_recv()
        beside = copy_to(out.at[block], out.at[block], f_send.at[lane, d], recv.at[block],
                         (seq_at(z, xl, 1 - core), c))
        beside.start()
        waits.append(beside)

    def settle(out, recv, d, side):
        block = seq_at(lax.rem(z + 4 - d, 4), side, 1 - core)
        copy_to(out.at[block], out.at[block], z_send.at[0, 0], recv.at[block],
                (seq_at(z, xl, 1 - core), c)).wait_recv()

    lax.fori_loop(0, 3, project_tile, 0)
    own_k = first_stage(0, k_out, k_recv, 0)
    pass_on(k_out, k_recv, 0, 0, own_k)
    lax.fori_loop(3, 5, project_tile, 0)
    own_v = first_stage(640, v_out, v_recv, 1)
    pass_on(v_out, v_recv, 1, 0, own_v)
    lax.fori_loop(5, 7, project_tile, 0)
    last = pl.ds(1792, 128)
    flat_t[last, :] = jnp.dot(rows_in[...], w[:, last], preferred_element_type=F32).T.astype(BF16)
    quarter = xl * 2 + core
    for d in range(16):
        to = lax.rem(s + d, 16)
        piece = flat_t.at[pl.ds(pl.multiple_of(1280 + (to // 4) * 160, 32), 160),
                        pl.ds(pl.multiple_of(lax.rem(to, 4) * 128, 128), 128)]
        if d == 0:
            own_q = pltpu.make_async_copy(piece, q_out.at[s], local_sem.at[2])
            own_q.start()
        else:
            one = copy_to(piece, q_out.at[s], q_send.at[d - 1], q_recv.at[s], (to, c))
            one.start()
            waits.append(one)
    for d in (1, 3, 2):
        pass_on(k_out, k_recv, 0, d, None)
    relay(k_out, k_recv, 0, 0)
    for d in (1, 3, 2):
        pass_on(v_out, v_recv, 1, d, None)
    relay(v_out, v_recv, 1, 0)
    for d in (1, 3, 2):
        relay(k_out, k_recv, 0, d)
    for d in (1, 3, 2):
        relay(v_out, v_recv, 1, d)
    for d in (0, 1, 3, 2):
        for side in (0, 1):
            settle(k_out, k_recv, d, side)
            settle(v_out, v_recv, d, side)
    own_q.wait()
    own_p.wait()
    p_third()
    p_last()
    for d in range(1, 16):
        block = lax.rem(s + d, 16)
        copy_to(q_out.at[block], q_out.at[block], q_send.at[0], q_recv.at[block], (block, c)).wait_recv()
    for one in waits:
        one.wait_send()


def front(ends, hidden, norm_gain, input_w, gate_w, state_w, small, out_w, embedding, attn_gain, wk, wv, wq, p_in):
    dma = pltpu.SemaphoreType.DMA
    vm, anyw = pl.BlockSpec(memory_space=VMEM), pl.BlockSpec(memory_space=pl.ANY)
    return pl.pallas_call(
        front_kernel,
        out_shape=(
            jax.ShapeDtypeStruct((8, 64, 2560), BF16),
            jax.ShapeDtypeStruct((16, 160, 512), BF16),
            jax.ShapeDtypeStruct((16, 160, 512), BF16),
            jax.ShapeDtypeStruct((16, 160, 128), BF16),
            jax.ShapeDtypeStruct((2560, 640), BF16),
        ),
        in_specs=[pl.BlockSpec(memory_space=pltpu.SMEM), anyw, vm, anyw, anyw, anyw, vm, anyw, anyw, vm,
                  anyw, anyw, anyw, anyw],
        out_specs=(vm, anyw, anyw, vm, anyw),
        scratch_shapes=[
            VMEM((8, 64, 2560), BF16),
            VMEM((2560, 640), BF16),
            VMEM((2560, 640), BF16),
            VMEM((2560, 256), BF16),
            VMEM((640, 2560), BF16),
            VMEM((5120, 1920), BF16),
            VMEM((512, 5120), BF16),
            VMEM((8, 64, 2560), BF16),
            VMEM((7, 64, 2560), BF16),
            VMEM((1920, 512), BF16),
            VMEM((512, 640), F32),
            VMEM((512, 640), F32),
            VMEM((512, 640), F32),
            VMEM((4, 64, 640), F32),
            VMEM((2, 72, 640), F32),
            VMEM((2, 72, 640), F32),
            VMEM((4, 72, 640), F32),
            VMEM((512, 128), F32),
            VMEM((128, 512), F32),
            VMEM((512, 640), F32),
            VMEM((512, 128), BF16),
            VMEM((128, 512), BF16),
            VMEM((160, 640), BF16),
            VMEM((8, 1, 512), F32),
            VMEM((512, 128), F32),
            VMEM((512, 640), BF16),
            dma((10,)),
            dma((30,)),
            dma((16, 2)),
            dma((15,)),
            dma((16,)),
            dma((5,)),
            dma((6,)),
            dma((7,)),
            dma((8,)),
            dma((7,)),
            dma((7,)),
            dma((7,)),
            dma((8,)),
            dma((2, 3)),
            dma((2, 4)),
            dma((2, 4)),
            dma((2, 4)),
            dma((16,)),
            dma((16,)),
            dma((15,)),
            dma((16,)),
            dma((4,)),
        ],
        compiler_params=pltpu.CompilerParams(
            collective_id=0, has_side_effects=True, vmem_limit_bytes=67043328
        ),
        name="front",
    )(ends, hidden, norm_gain, input_w, gate_w, state_w, small, out_w, embedding, attn_gain, wk, wv, wq, p_in)


def attend_kernel(ends, q_in, k_in, v_in, out):
    quarter = lax.rem(lax.axis_index("seq"), 4)
    i = pl.program_id(0)
    first, second = ends[0], ends[1]
    queries = jnp.concatenate(
        [q_in[2 * i].astype(F32).T, q_in[2 * i + 1].astype(F32).T], axis=0
    ).astype(BF16)
    row = lax.broadcasted_iota(jnp.int32, (256, 1), 0)
    place = i * 1024 + quarter * 128 + row + jnp.where(row >= 128, 384, 0)

    def start_of(p):
        return jnp.where(p >= second, second, jnp.where(p >= first, first, 0))

    begin = start_of(place)
    low_place = i * 1024 + quarter * 128
    top_begin = start_of(low_place + 512 + 127)
    low_begin = start_of(low_place)
    lowest = low_begin // 512
    scale = (AP ** -0.5) * 1.4426950408889634

    def step(b, carry, masked):
        top, total, acc = carry
        scores = jnp.dot(queries, k_in[b], preferred_element_type=F32)
        if masked:
            key = b * 512 + lax.broadcasted_iota(jnp.int32, (256, 512), 1)
            visible = (key >= begin) & (key <= place)
            scores = jnp.where(visible, scores, -1e30)
        new_top = jnp.maximum(top, jnp.max(scores, axis=-1, keepdims=True))
        weights = jnp.exp2((scores - new_top) * scale)
        if masked:
            weights = jnp.where(visible, weights, 0.0)
        keep = jnp.exp2((top - new_top) * scale)
        total = total * keep + jnp.sum(weights, axis=-1, keepdims=True)
        acc = acc * keep + lax.dot_general(
            weights.astype(BF16), v_in[b], (((1,), (1,)), ((), ())), preferred_element_type=F32
        )
        return new_top, total, acc

    carry = (jnp.full((256, 1), -1e30, F32), jnp.zeros((256, 1), F32), jnp.zeros((256, AP), F32))
    plain_from = jnp.minimum((top_begin + 511) // 512, 2 * i)
    carry = lax.fori_loop(lowest, plain_from, lambda b, t: step(b, t, True), carry)
    carry = lax.fori_loop(jnp.maximum(lowest, plain_from), 2 * i, lambda b, t: step(b, t, False), carry)
    carry = lax.fori_loop(jnp.maximum(lowest, 2 * i), 2 * i + 2, lambda b, t: step(b, t, True), carry)
    top, total, acc = carry
    context = (acc / total).T.astype(BF16)
    out[0] = context[:, :128]
    out[1] = context[:, 128:]


def attend(ends, q_in, k_in, v_in):
    vm = pl.BlockSpec(memory_space=VMEM)
    return pl.pallas_call(
        attend_kernel,
        out_shape=jax.ShapeDtypeStruct((16, 160, 128), BF16),
        grid=(8,),
        in_specs=[pl.BlockSpec(memory_space=pltpu.SMEM), vm, vm, vm],
        out_specs=pl.BlockSpec((2, 160, 128), lambda i: (i, 0, 0)),
        compiler_params=pltpu.CompilerParams(vmem_limit_bytes=40 * 1024 * 1024),
        cost_estimate=pl.CostEstimate(flops=10_000_000_000, bytes_accessed=6_000_000, transcendentals=0),
        name="attend",
    )(ends, q_in, k_in, v_in)


def finish_kernel(ctx, proj_t, out, gathered, part, recv, in_send, in_recv, send_sem, recv_sem, local_sem):
    s, c = lax.axis_index("seq"), lax.axis_index("chan")
    peers, sources = chan_peers(s, c), chan_sources(s, c)
    greet([(s, p) for p in peers] + [(lax.rem(s + d, 16), c) for d in range(1, 16)])
    z = s // 4
    lanes = pl.ds(pl.multiple_of(lax.rem(s, 4) * 128, 128), 128)
    waits = []
    for d in range(16):
        to = lax.rem(s + d, 16)
        where = gathered.at[pl.ds(pl.multiple_of(z * 160, 32), 160), lanes]
        if d == 0:
            own = pltpu.make_async_copy(ctx.at[s], where, local_sem.at[0])
            own.start()
        else:
            one = copy_to(ctx.at[to], where, in_send.at[d - 1], in_recv.at[s], (to, c))
            one.start()
            waits.append(one)
    own.wait()
    for d in range(1, 16):
        block = lax.rem(s + d, 16)
        where = gathered.at[pl.ds(pl.multiple_of((block // 4) * 160, 32), 160),
                            pl.ds(pl.multiple_of(lax.rem(block, 4) * 128, 128), 128)]
        copy_to(ctx.at[0], where, in_send.at[0], in_recv.at[block], (block, c)).wait_recv()
    copies = []
    for i, p in enumerate(peers):
        at = pl.ds(pl.multiple_of(p * 320, 32), 320)
        part[p] = jnp.dot(proj_t[at, :], gathered[...], preferred_element_type=F32).astype(BF16)
        one = copy_to(part.at[p], recv.at[i], send_sem.at[i], recv_sem.at[i], (s, p))
        one.start()
        copies.append(one)
    at = pl.ds(pl.multiple_of(c * 320, 32), 320)
    value = jnp.dot(proj_t[at, :], gathered[...], preferred_element_type=F32)
    for i in (6, 5, 4, 3, 2, 1, 0):
        copies[i].wait_recv()
        value = value + recv[i].astype(F32)
    out[...] = value.T
    for one in waits + copies:
        one.wait_send()


def finish(ctx, proj_t):
    dma = pltpu.SemaphoreType.DMA
    vm = pl.BlockSpec(memory_space=VMEM)
    return pl.pallas_call(
        finish_kernel,
        out_shape=jax.ShapeDtypeStruct((512, 320), F32),
        in_specs=[vm, vm],
        out_specs=vm,
        scratch_shapes=[
            VMEM((640, 512), BF16),
            VMEM((8, 320, 512), BF16),
            VMEM((7, 320, 512), BF16),
            dma((15,)),
            dma((16,)),
            dma((7,)),
            dma((7,)),
            dma((1,)),
        ],
        compiler_params=pltpu.CompilerParams(
            collective_id=2, has_side_effects=True, vmem_limit_bytes=40 * 1024 * 1024
        ),
        cost_estimate=pl.CostEstimate(flops=50_000_000_000, bytes_accessed=6_000_000, transcendentals=0),
        name="finish",
    )(ctx, proj_t)


def local(
    hidden,
    embedding,
    segments,
    input_norm_gain,
    gate_proj,
    input_proj,
    state_proj,
    step_proj,
    step_bias,
    decay_log,
    skip_gain,
    out_gain,
    out_proj,
    attn_gain,
    query_proj,
    key_proj,
    value_proj,
    attn_out,
):
    chan_index = lax.axis_index("chan")
    ends = jnp.stack([jnp.sum((segments < 1).astype(jnp.int32)), jnp.sum((segments < 2).astype(jnp.int32))])
    state_w = jnp.concatenate([state_proj, jnp.pad(step_proj, ((0, 0), (0, 118)))], axis=1)
    small = jnp.stack([
        jnp.pad(step_bias, (0, 630)), jnp.pad(decay_log, (0, 630)),
        jnp.repeat(skip_gain, HEAD_CHANNELS), out_gain,
    ])
    mixed, k_all, v_all, q_all, proj_t = front(
        ends, hidden.reshape(8, 64, 2560), input_norm_gain[None, :], input_proj, gate_proj, state_w, small,
        out_proj, embedding.reshape(8, 64, 2560), attn_gain[None, :], key_proj, value_proj, query_proj,
        attn_out.T,
    )
    ctx = attend(ends, q_all, k_all, v_all)
    out_share = finish(ctx, proj_t)
    own_mixed = lax.dynamic_slice_in_dim(mixed.reshape(512, 2560), chan_index * 320, 320, 1)
    return (out_share + own_mixed.astype(jnp.float32)).astype(jnp.bfloat16)


def solution(mesh):
    in_specs = (
        P("seq", None),
        P("seq", None),
        P(),
        P(),
        P(None, "chan"),
        P(None, "chan"),
        P(),
        P(None, "chan"),
        P("chan"),
        P("chan"),
        P("chan"),
        P("chan"),
        P("chan", None),
        P(),
        P("seq", "chan"),
        P("seq", "chan"),
        P("seq", "chan"),
        P("chan", "seq"),
    )
    out_specs = P("seq", "chan")
    return jax.shard_map(local, mesh=mesh, in_specs=in_specs, out_specs=out_specs, check_vma=False)
```

```python
import jax
import jax.numpy as jnp
from jax import lax
from jax.experimental import pallas as pl
from jax.experimental.pallas import tpu as pltpu
from jax.sharding import PartitionSpec as P

N = 64
HEAD_CHANNELS = 64
AP = 160
EPSILON = 1e-05
MESH = pl.DeviceIdType.MESH
VMEM = pltpu.VMEM
LIMIT = 62 * 1024 * 1024
F32 = jnp.float32
BF16 = jnp.bfloat16


def greet(peers):
    barrier = pltpu.get_barrier_semaphore()
    for peer in peers:
        pl.semaphore_signal(barrier, inc=1, device_id=peer, device_id_type=MESH)
    pl.semaphore_wait(barrier, len(peers))


def copy_to(src, dst, send, recv, where):
    return pltpu.make_async_remote_copy(
        src_ref=src, dst_ref=dst, send_sem=send, recv_sem=recv,
        device_id=where, device_id_type=MESH,
    )


OFFSETS = ((1, 2), (1, 1), (1, 3), (0, 2), (1, 0), (0, 1), (0, 3))


def chan_peers(s, c):
    half, place = c // 4, lax.rem(c, 4)
    return [lax.rem(half + a, 2) * 4 + lax.rem(place + b, 4) for a, b in OFFSETS]


def chan_sources(s, c):
    half, place = c // 4, lax.rem(c, 4)
    return [lax.rem(half + a, 2) * 4 + lax.rem(place + 4 - b, 4) for a, b in OFFSETS]


def seq_parts(s):
    return s // 4, lax.rem(s // 2, 2), lax.rem(s, 2)


def seq_at(z, xl, core):
    return z * 4 + xl * 2 + core


class ChanSum:
    def __init__(self, s, c, part, ring, fin, comb, across, send_sem, recv_sem):
        self.s, self.part, self.ring, self.fin = s, part, ring, fin
        self.comb, self.across, self.send_sem, self.recv_sem = comb, across, send_sem, recv_sem
        self.rows, self.width = part.shape[1] // 2, part.shape[2]
        self.xh, self.yy = c // 4, lax.rem(c, 4)
        self.up = lax.rem(self.yy + 1, 4)
        self.down = lax.rem(self.yy + 3, 4)
        self.far = lax.rem(self.yy + 2, 4)
        self.sent = []

    def column(self, turn):
        return 1 - self.xh if turn == 0 else self.xh

    def side(self, ref, half):
        return ref.at[pl.ds(half * self.rows, self.rows), :]

    def piece(self, turn, y, half):
        return self.side(self.part.at[self.column(turn) * 4 + y], half)

    def copy(self, i, src, dst, y, turn=1):
        to = self.column(turn) * 4 + y
        return copy_to(src, dst, self.send_sem.at[i], self.recv_sem.at[i], (self.s, to))

    def send(self, i, src, dst, y, turn=1):
        one = self.copy(i, src, dst, y, turn)
        one.start()
        self.sent.append(one)

    def wait(self, i, dst):
        self.copy(i, dst, dst, self.up).wait_recv()

    def first(self, turn):
        i = 6 * turn
        self.send(i, self.piece(turn, self.far, 0), self.ring.at[turn, 0], self.up)
        self.send(i + 2, self.piece(turn, self.far, 1), self.ring.at[turn, 1], self.down)
        self.send(i + 1, self.piece(turn, self.up, 1), self.side(self.fin.at[turn, 0], 1), self.up)
        self.send(i + 3, self.piece(turn, self.down, 0), self.side(self.fin.at[turn, 1], 0), self.down)

    def second(self, turn):
        for way, y in ((0, self.up), (1, self.down)):
            self.wait(6 * turn + 2 * way, self.ring.at[turn, way])
            mine, its, both = self.piece(turn, y, way), self.ring.at[turn, way], self.comb.at[turn, way]

            def add(n, _):
                at = pl.ds(pl.multiple_of(n * 256, 256), 256)
                both[:, at] = (mine[:, at].astype(F32) + its[:, at].astype(F32)).astype(BF16)
                return 0

            lax.fori_loop(0, self.width // 256, add, 0)
            self.send(6 * turn + 4 + way, both, self.side(self.fin.at[turn, way], way), y)

    def arrived(self, turn):
        i = 6 * turn
        for way in (0, 1):
            self.wait(i + 1 + 2 * way, self.side(self.fin.at[turn, way], 1 - way))
            self.wait(i + 4 + way, self.side(self.fin.at[turn, way], way))

    def total(self, turn, at):
        value = self.part[self.column(turn) * 4 + self.yy, :, at].astype(F32)
        return value + self.fin[turn, 0, :, at].astype(F32) + self.fin[turn, 1, :, at].astype(F32)

    def cross(self):
        self.arrived(0)
        own = self.column(0) * 4 + self.yy

        def add(n, _):
            at = pl.ds(pl.multiple_of(n * 256, 256), 256)
            self.part[own, :, at] = self.total(0, at).astype(BF16)
            return 0

        lax.fori_loop(0, self.width // 256, add, 0)
        self.send(12, self.part.at[own], self.across, self.yy, 0)

    def close(self):
        self.arrived(1)
        self.wait(12, self.across)

    def result(self, at):
        return self.total(1, at) + self.across[:, at].astype(F32)


def ring_scratch(rows, width):
    return [
        VMEM((2, 2, rows // 2, width), BF16),
        VMEM((2, 2, rows, width), BF16),
        VMEM((2, 2, rows // 2, width), BF16),
        VMEM((rows, width), BF16),
        pltpu.SemaphoreType.DMA((13,)),
        pltpu.SemaphoreType.DMA((13,)),
    ]


def start_of(place, first, second):
    return jnp.where(place >= second, second, jnp.where(place >= first, first, 0))


def silu(v):
    return v / (1.0 + jnp.exp(-v))


def front_kernel(segments, hidden, norm_gain, input_w, gate_w, state_w, step_w, bias, decay, skip, out_gain,
                 out_w, embedding, attn_gain, wk, wv, wq, p_in,
                 mixed, k_out, v_out, q_out, p_out,
                 hid, iw, gw, sw, dw, ow, ao, vec, w, rows_in, part, flat_t, run_e, xs, ys, states, tx, rx, planes, tx_t, rx_t, planes_t,
                 run_rows, run_cols, step_e, bc_rows, bc_cols, pb, sq_all, sq_cols, weighted,
                 load_sem, w_send, w_recv, p_send, p_recv, st_send, st_recv,
                 sq_send, sq_recv, ring, fin, comb, across, rs_send, rs_recv, ag_send, ag_recv,
                 z_send, x_send, d_send, f_send, k_recv, v_recv, q_send, q_recv, local_sem, own_sem):
    s, c = lax.axis_index("seq"), lax.axis_index("chan")
    z, xl, core = seq_parts(s)
    peers, sources = chan_peers(s, c), chan_sources(s, c)
    up, down, far = lax.rem(z + 1, 4), lax.rem(z + 3, 4), lax.rem(z + 2, 4)
    waits = []

    def load(i, src, dst):
        one = pltpu.make_async_copy(src, dst, load_sem.at[i])
        one.start()
        return one

    own_rows = pl.ds(pl.multiple_of(s * 320, 64), 320)
    w_loads = [load(i, src, w.at[own_rows, pl.ds(i * 640, 640)]) for i, src in enumerate((wk, wv, wq))]
    l_hid = load(3, hidden, hid)
    l_sw = load(4, state_w, sw.at[:, pl.ds(0, 128)])
    l_dw = load(10, step_w, dw)
    l_iw = load(5, input_w, iw)
    l_pb = load(6, p_in, ao)
    l_gw = load(7, gate_w, gw)
    l_ow = load(8, out_w, ow)
    greet([(s, p) for p in peers] + [(lax.rem(s + d, 16), c) for d in range(1, 16)])

    used = [0, 0]
    sibling = seq_at(z, xl, 1 - core)

    def w_rows(block, half, group):
        rows = pl.ds(pl.multiple_of(block * 320 + half * 160, 32), 160)
        return w.at[rows, pl.ds(1280 * group, 1280 - 640 * group)]

    def w_to(block, half, group, to):
        rows = w_rows(block, half, group)
        one = copy_to(rows, rows, w_send.at[used[0]], w_recv.at[block, half, group], (to, c))
        used[0] += 1
        one.start()
        waits.append(one)

    def w_wait(block, half, group):
        rows = w_rows(block, half, group)
        copy_to(rows, rows, w_send.at[0], w_recv.at[block, half, group], (sibling, c)).wait_recv()

    def p_rows(block):
        return p_out.at[pl.ds(pl.multiple_of(block * 160, 32), 160), :]

    def p_to(block, to, src=None):
        rows = p_rows(block)
        one = copy_to(rows if src is None else src, rows, p_send.at[used[1]], p_recv.at[block], (to, c))
        used[1] += 1
        one.start()
        waits.append(one)

    def p_wait(block):
        rows = p_rows(block)
        copy_to(rows, rows, p_send.at[0], p_recv.at[block], (seq_at(z, xl, 1 - core), c)).wait_recv()

    def w_across(half, group):
        w_to(s, half, group, seq_at(z, 1 - xl, core))

    def w_first(half, group):
        w_to(s, half, group, seq_at(up, xl, core))
        w_to(s, half, group, seq_at(down, xl, core))
        w_to(s, half, group, sibling)

    def w_second(half, group):
        block = seq_at(z, 1 - xl, core)
        w_wait(block, half, group)
        w_to(block, half, group, seq_at(up, xl, core))
        w_to(block, half, group, seq_at(down, xl, core))
        w_to(block, half, group, sibling)

    def w_ring(side, group):
        for half in (0, 1):
            w_wait(seq_at(down, side, core), half, group)
            w_wait(seq_at(up, side, core), half, group)
            if half == 0:
                w_to(seq_at(down, side, core), 0, group, seq_at(up, xl, core))
        w_to(seq_at(up, side, core), 1, group, seq_at(down, xl, core))
        for half in (0, 1):
            w_to(seq_at(down, side, core), half, group, sibling)
            w_to(seq_at(up, side, core), half, group, sibling)

    def w_far(side, group):
        for half in (0, 1):
            w_wait(seq_at(far, side, core), half, group)
            w_to(seq_at(far, side, core), half, group, sibling)

    def w_last(group):
        for zz in range(4):
            for xx in range(2):
                for half in (0, 1):
                    w_wait(seq_at(zz, xx, 1 - core), half, group)

    def p_first():
        for to in (seq_at(z, 1 - xl, core), seq_at(up, xl, core), seq_at(down, xl, core), sibling):
            p_to(s, to, pb)

    def p_second():
        block = seq_at(z, 1 - xl, core)
        p_wait(block)
        for to in (seq_at(up, xl, core), seq_at(down, xl, core), sibling):
            p_to(block, to)
        p_wait(seq_at(down, xl, core))
        p_wait(seq_at(up, xl, core))
        p_to(seq_at(down, xl, core), seq_at(up, xl, core))
        p_to(seq_at(down, xl, core), sibling)
        p_to(seq_at(up, xl, core), sibling)

    def p_third():
        p_wait(seq_at(down, 1 - xl, core))
        p_wait(seq_at(up, 1 - xl, core))
        p_to(seq_at(down, 1 - xl, core), seq_at(up, xl, core))
        p_to(seq_at(down, 1 - xl, core), sibling)
        p_to(seq_at(up, 1 - xl, core), sibling)
        p_wait(seq_at(far, xl, core))
        p_to(seq_at(far, xl, core), sibling)

    def p_last():
        p_wait(seq_at(far, 1 - xl, core))
        p_to(seq_at(far, 1 - xl, core), sibling)
        for zz in range(4):
            for xx in range(2):
                p_wait(seq_at(zz, xx, 1 - core))

    for one in w_loads:
        one.wait()
    w_first(0, 0)
    w_first(0, 1)

    first, second = boundary(segments, 1), boundary(segments, 2)
    base = s * 512
    l_hid.wait()

    def norm_first(p, _):
        at = pl.ds(pl.multiple_of(p * 64, 64), 64)
        value = hid[p].astype(F32)
        factor = lax.rsqrt(jnp.sum(value * value, axis=-1, keepdims=True) / 2560.0 + EPSILON)
        rows_in[at, pl.ds(0, 2560)] = (value * factor * norm_gain[...]).astype(BF16)
        return 0

    lax.fori_loop(0, 8, norm_first, 0)
    tokens = rows_in.at[:, pl.ds(0, 2560)]
    sw[:, 128:256] = jnp.zeros((2560, 128), BF16)
    vec[...] = jnp.zeros((8, 128), F32)
    vec[0:1, 0:10] = bias[...]
    vec[1:2, 0:10] = decay[...]
    vec[2:3, 0:10] = skip[...]
    l_sw.wait()
    l_dw.wait()
    sw[:, 128:138] = dw[...]
    both = jnp.dot(tokens[...], sw[...], preferred_element_type=F32)
    bc = silu(both[:, :128])
    bc_rows[...] = bc.astype(BF16)
    bc_cols[...] = bc.T.astype(BF16)
    logits = both[:, 128:] + vec[0:1, :]
    steps = jnp.maximum(logits, 0.0) + jnp.log1p(jnp.exp(-jnp.abs(logits)))
    rate = -jnp.exp(vec[1:2, :])
    lower = (lax.broadcasted_iota(jnp.int32, (512, 512), 0)
             >= lax.broadcasted_iota(jnp.int32, (512, 512), 1)).astype(F32)
    running = jnp.dot(lower, steps * rate, preferred_element_type=F32, precision=lax.Precision.HIGHEST)
    spread = (lax.broadcasted_iota(jnp.int32, (128, 640), 1) // 64
              == lax.broadcasted_iota(jnp.int32, (128, 640), 0)).astype(F32)
    run_rows[...] = running
    run_cols[...] = running.T
    wide_steps = jnp.dot(steps, spread, preferred_element_type=F32, precision=lax.Precision.HIGHEST)
    run_e[...] = jnp.dot(running, spread, preferred_element_type=F32, precision=lax.Precision.HIGHEST)
    step_e[...] = wide_steps
    skip_e = jnp.dot(vec[...], spread, preferred_element_type=F32, precision=lax.Precision.HIGHEST)[2:3, :]
    l_iw.wait()

    def input_tile(n, width):
        at = pl.ds(n, width)
        xs[:, at] = silu(jnp.dot(tokens[...], iw[:, at], preferred_element_type=F32))
        step_e[:, at] = xs[:, at] * step_e[:, at]

    input_tile(0, 256)
    input_tile(256, 256)
    input_tile(512, 128)

    states[0] = jnp.zeros((64, 640), F32)
    total = None
    for k in range(4):
        rows = slice(k * 128, k * 128 + 128)
        end = run_e[k * 128 + 127:k * 128 + 128, :]
        begin_end = start_of(base + k * 128 + 127, first, second)
        place = base + k * 128 + lax.broadcasted_iota(jnp.int32, (128, 1), 0)
        keep = jnp.where(place >= begin_end, jnp.exp(end - run_e[rows, :]), 0.0)
        own = jnp.dot(bc_cols[:64, rows], (step_e[rows, :] * keep).astype(BF16), preferred_element_type=F32)
        gap = end if k == 0 else end - run_e[k * 128 - 1:k * 128, :]
        through = jnp.where(base + k * 128 - 1 >= begin_end, jnp.exp(gap), 0.0)
        if k == 0:
            total = through
            states[1] = own
        else:
            total = total * through
            if k < 3:
                states[k + 1] = through * states[k] + own
            else:
                tx[0] = (through * states[k] + own).astype(BF16)
    tx_t[0] = jnp.broadcast_to(total, (8, 640))

    def state_to(i, to):
        pair = [
            copy_to(tx_t.at[i], rx_t.at[i], st_send.at[2 * i], st_recv.at[2 * i], (to, c)),
            copy_to(tx.at[i], rx.at[i], st_send.at[2 * i + 1], st_recv.at[2 * i + 1], (to, c)),
        ]
        for one in pair:
            one.start()
            waits.append(one)
        return pair

    def joined(i, low):
        mine_s, mine_t = tx[i].astype(F32), tx_t[i, 0:1, :]
        its_s, its_t = rx[i].astype(F32), rx_t[i, 0:1, :]
        first_s, first_t = jnp.where(low, mine_s, its_s), jnp.where(low, mine_t, its_t)
        last_s, last_t = jnp.where(low, its_s, mine_s), jnp.where(low, its_t, mine_t)
        return (last_t * first_s + last_s).astype(BF16), jnp.broadcast_to(first_t * last_t, (8, 640))

    for one in state_to(0, sibling):
        one.wait_recv()
    tx[1], tx_t[1] = joined(0, core == 0)
    pair = state_to(1, seq_at(z, 1 - xl, core))
    for group in (0, 1):
        w_across(0, group)
        w_across(1, group)

    def chunk(k, _):
        at = pl.ds(pl.multiple_of(k * 128, 128), 128)
        place = base + k * 128 + lax.broadcasted_iota(jnp.int32, (128, 1), 0)
        key = base + k * 128 + lax.broadcasted_iota(jnp.int32, (1, 128), 1)
        begin = start_of(place, first, second)
        allowed = (key >= begin) & (key <= place)
        cross = jnp.dot(bc_rows[at, 64:128], bc_cols[0:64, at], preferred_element_type=F32)
        cross = jnp.where(allowed, cross, 0.0)
        lane = lax.broadcasted_iota(jnp.int32, (128, 128), 1)
        for pair in range(5):
            lanes = pl.ds(pair * 128, 128)
            scaled = step_e[at, lanes].astype(BF16)
            halves = []
            for h in (2 * pair, 2 * pair + 1):
                gap = run_rows[at, h:h + 1] - run_cols[h:h + 1, at]
                decay = jnp.exp(jnp.where(allowed, gap, -1e30))
                halves.append(jnp.dot((decay * cross).astype(BF16), scaled, preferred_element_type=F32))
            ys[at, lanes] = jnp.where(lane < 64, halves[0], halves[1])
        return 0

    lax.fori_loop(0, 2, chunk, 0)
    for one in pair:
        one.wait_recv()
    planes[z], planes_t[z] = joined(1, xl == 0)
    for d in (2, 1, 3):
        to = (seq_at(lax.rem(z + d, 4), xl, core), c)
        for one in (
            copy_to(planes_t.at[z], planes_t.at[z], st_send.at[2 + 2 * d], st_recv.at[4 + 2 * z], to),
            copy_to(planes.at[z], planes.at[z], st_send.at[3 + 2 * d], st_recv.at[5 + 2 * z], to),
        ):
            one.start()
            waits.append(one)
    w_first(1, 0)
    l_pb.wait()
    pb[...] = ao[...].astype(F32).T.astype(BF16)
    own_p = pltpu.make_async_copy(pb, p_rows(s), own_sem.at[0])
    own_p.start()
    lax.fori_loop(2, 4, chunk, 0)

    for k in range(1, 4):
        rows = slice(k * 128, k * 128 + 128)
        place = base + k * 128 + lax.broadcasted_iota(jnp.int32, (128, 1), 0)
        begin = start_of(place, first, second)
        enter = jnp.where(base + k * 128 - 1 >= begin,
                          jnp.exp(run_e[rows, :] - run_e[k * 128 - 1:k * 128, :]), 0.0)
        ys[rows, :] += enter * jnp.dot(bc_rows[rows, 64:128], states[k].astype(BF16), preferred_element_type=F32)

    l_gw.wait()
    for n, width in ((0, 256), (256, 256), (512, 128)):
        at = pl.ds(n, width)
        step_e[:, at] = silu(jnp.dot(tokens[...], gw[:, at], preferred_element_type=F32))

    enter_s = jnp.zeros((64, 640), F32)
    for d in (1, 2, 3):
        zz = lax.rem(z + d, 4)
        of = (seq_at(zz, xl, core), c)
        copy_to(planes_t.at[zz], planes_t.at[zz], st_send.at[0], st_recv.at[4 + 2 * zz], of).wait_recv()
        copy_to(planes.at[zz], planes.at[zz], st_send.at[0], st_recv.at[5 + 2 * zz], of).wait_recv()
    for zz in range(3):
        enter_s = jnp.where(zz < z, planes_t[zz, 0:1, :] * enter_s + planes[zz].astype(F32), enter_s)
    for i, low in ((1, xl == 0), (0, core == 0)):
        first_s = jnp.where(low, tx[i].astype(F32), rx[i].astype(F32))
        first_t = jnp.where(low, tx_t[i, 0:1, :], rx_t[i, 0:1, :])
        enter_s = jnp.where(low, enter_s, first_t * enter_s + first_s)
    states[0] = enter_s

    def gating(k, _):
        at = pl.ds(pl.multiple_of(k * 128, 128), 128)
        place = base + k * 128 + lax.broadcasted_iota(jnp.int32, (128, 1), 0)
        begin = start_of(place, first, second)
        enter = jnp.where(base - 1 >= begin, jnp.exp(run_e[at, :]), 0.0)
        y = ys[at, :] + enter * jnp.dot(bc_rows[at, 64:128], states[0].astype(BF16), preferred_element_type=F32)
        y = y + xs[at, :] * skip_e
        gated = y * step_e[at, :]
        sq_cols[at, :] = jnp.broadcast_to(jnp.sum(gated * gated, axis=-1, keepdims=True), (128, 128))
        weighted[at, :] = (gated * out_gain[...]).astype(BF16)
        return 0

    w_second(0, 0)
    lax.fori_loop(0, 4, gating, 0)
    sq_all[c] = sq_cols[...].T[0:1, :]
    l_ow.wait()

    gather = ChanSum(s, c, part, ring, fin, comb, across, rs_send, rs_recv)

    def make(turn):
        rows = pl.ds(pl.multiple_of(gather.column(turn) * 256, 256), 256)
        first_piece = gather.column(turn) * 4

        def columns(n, _):
            at = pl.ds(pl.multiple_of(n * 256, 256), 256)
            tile = jnp.dot(weighted[rows, :], ow[:, at], preferred_element_type=F32)
            part[pl.ds(first_piece, 4), :, at] = tile.astype(BF16).reshape(4, 64, 256)
            return 0

        lax.fori_loop(0, 10, columns, 0)

    make(0)
    gather.first(0)
    for i, p in enumerate(peers):
        few = copy_to(sq_all.at[c], sq_all.at[c], sq_send.at[i], sq_recv.at[c], (s, p))
        few.start()
        waits.append(few)
    make(1)
    gather.second(0)
    gather.first(1)
    w_second(1, 0)
    w_ring(xl, 0)
    gather.second(1)
    gather.cross()
    for i, p in enumerate(sources):
        copy_to(sq_all.at[p], sq_all.at[p], sq_send.at[0], sq_recv.at[p], (s, p)).wait_recv()
    gather.close()
    own64 = pl.ds(pl.multiple_of(c * 64, 64), 64)
    squares = sq_all[0]
    for i in range(1, 8):
        squares = squares + sq_all[i]
    sq_cols[...] = jnp.broadcast_to(squares, (128, 512)).T
    factor = lax.rsqrt(sq_cols[own64, 0:1] / 5120.0 + EPSILON)

    def gather_sum(n, _):
        at = pl.ds(pl.multiple_of(n * 256, 256), 256)
        mixed[c, :, at] = (hid[c, :, at].astype(F32) + gather.result(at) * factor).astype(BF16)
        return 0

    lax.fori_loop(0, 10, gather_sum, 0)
    xh, yy = c // 4, lax.rem(c, 4)
    y_up, y_down, y_far = lax.rem(yy + 1, 4), lax.rem(yy + 3, 4), lax.rem(yy + 2, 4)
    shared = [0]

    def m_rows(piece, side):
        return mixed.at[piece, pl.ds(side * 32, 32), :]

    def m_to(piece, side, to):
        rows = m_rows(piece, side)
        one = copy_to(rows, rows, ag_send.at[shared[0]], ag_recv.at[piece, side], (s, to))
        shared[0] += 1
        one.start()
        waits.append(one)

    def m_wait(piece, side):
        rows = m_rows(piece, side)
        copy_to(rows, rows, ag_send.at[0], ag_recv.at[piece, side], (s, (1 - xh) * 4 + yy)).wait_recv()

    def m_spread(piece):
        for side in (0, 1):
            m_to(piece, side, xh * 4 + y_up)
            m_to(piece, side, xh * 4 + y_down)

    def m_ring(col):
        for side in (0, 1):
            m_wait(col * 4 + y_down, side)
            m_wait(col * 4 + y_up, side)
            if side == 0:
                m_to(col * 4 + y_down, 0, xh * 4 + y_up)
        m_to(col * 4 + y_up, 1, xh * 4 + y_down)

    def m_end(col):
        for side in (0, 1):
            m_wait(col * 4 + y_far, side)

    for side in (0, 1):
        m_to(c, side, (1 - xh) * 4 + yy)
    m_spread(c)
    for one in gather.sent:
        one.wait_send()
    l_emb = load(9, embedding, part)
    w_ring(1 - xl, 0)
    w_first(1, 1)
    w_second(0, 1)
    m_ring(xh)
    for side in (0, 1):
        m_wait((1 - xh) * 4 + yy, side)
    m_spread((1 - xh) * 4 + yy)
    l_emb.wait()
    w_far(xl, 0)
    m_end(xh)

    def norm_second(p, _):
        at = pl.ds(pl.multiple_of(p * 64, 64), 64)
        top = mixed[p].astype(F32)
        low = part[p].astype(F32)
        mean = (jnp.sum(top * top, axis=-1, keepdims=True)
                + jnp.sum(low * low, axis=-1, keepdims=True)) / 5120.0
        scale = lax.rsqrt(mean + EPSILON)
        rows_in[at, pl.ds(0, 2560)] = (top * scale * attn_gain[:, pl.ds(0, 2560)]).astype(BF16)
        rows_in[at, pl.ds(2560, 2560)] = (low * scale * attn_gain[:, pl.ds(2560, 2560)]).astype(BF16)
        return 0

    def project_tiles(low, high, half):
        tokens_at = pl.ds(pl.multiple_of(half * 256, 256), 256)

        def project_tile(n, _):
            at = pl.ds(pl.multiple_of(n * 256, 256), 256)
            value = jnp.dot(rows_in[tokens_at, :], w[:, at], preferred_element_type=F32)
            flat_t[at, tokens_at] = value.T.astype(BF16)
            return 0

        lax.fori_loop(low, high, project_tile, 0)
        if high == 7:
            last = pl.ds(1792, 128)
            value = jnp.dot(rows_in[tokens_at, :], w[:, last], preferred_element_type=F32)
            flat_t[last, tokens_at] = value.T.astype(BF16)

    outs, recvs = (k_out, v_out), (k_recv, v_recv)

    def landing(lane, block, half):
        return outs[lane].at[block, :, pl.ds(pl.multiple_of(half * 256, 256), 256)]

    def head_rows(lane, head, half):
        return flat_t.at[pl.ds(pl.multiple_of(lane * 640 + head * 160, 32), 160),
                         pl.ds(pl.multiple_of(half * 256, 256), 256)]

    def first_stage(lane, half, turn):
        mine = pltpu.make_async_copy(head_rows(lane, z, half), landing(lane, s, half), local_sem.at[lane, turn])
        mine.start()
        for d in (2, 1, 3):
            to = lax.rem(z + d, 4)
            one = copy_to(head_rows(lane, to, half), landing(lane, s, half), z_send.at[lane, turn, d - 1],
                          recvs[lane].at[s, half], (seq_at(to, xl, core), c))
            one.start()
            waits.append(one)
        for there, sem in ((seq_at(z, 1 - xl, core), x_send), (sibling, d_send)):
            one = copy_to(head_rows(lane, z, half), landing(lane, s, half), sem.at[lane, turn, 0],
                          recvs[lane].at[s, half], (there, c))
            one.start()
            waits.append(one)
        return mine

    def block_wait(lane, block, half):
        rows = landing(lane, block, half)
        copy_to(rows, rows, z_send.at[0, 0, 0], recvs[lane].at[block, half], (sibling, c)).wait_recv()

    def block_to(lane, block, half, sem, there):
        rows = landing(lane, block, half)
        one = copy_to(rows, rows, sem, recvs[lane].at[block, half], (there, c))
        one.start()
        waits.append(one)

    def pass_on(lane, half, turn, d):
        block = seq_at(lax.rem(z + 4 - d, 4), xl, core)
        block_wait(lane, block, half)
        block_to(lane, block, half, x_send.at[lane, turn, d], seq_at(z, 1 - xl, core))
        block_to(lane, block, half, d_send.at[lane, turn, d], sibling)

    def relay(lane, half, turn, d):
        block = seq_at(lax.rem(z + 4 - d, 4), 1 - xl, core)
        block_wait(lane, block, half)
        block_to(lane, block, half, f_send.at[lane, turn, d], sibling)

    def send_queries(half, turn):
        for d in range(4):
            for j in range(2):
                to_z = lax.rem(z + d, 4)
                to = seq_at(to_z, half, j)
                piece = flat_t.at[pl.ds(pl.multiple_of(1280 + to_z * 160, 32), 160),
                                  pl.ds(pl.multiple_of(half * 256 + j * 128, 128), 128)]
                send_query(piece, to, d, j, turn, half)

    def send_query(piece, to, d, j, turn, half):
        remote = copy_to(piece, q_out.at[s], q_send.at[turn, d, j], q_recv.at[s], (to, c))
        if d:
            remote.start()
            waits.append(remote)
        else:
            mine = (half == xl) & (j == core)

            @pl.when(mine)
            def _():
                q_out[s] = piece[...]

            @pl.when(jnp.logical_not(mine))
            def _():
                remote.start()
                remote.wait_send()

    early, late = xh, 1 - xh
    lax.fori_loop(early * 4, early * 4 + 4, norm_second, 0)
    w_far(1 - xl, 0)
    w_last(0)
    project_tiles(0, 3, early)
    own = [first_stage(0, early, 0)]
    project_tiles(3, 5, early)
    own.append(first_stage(1, early, 0))
    w_second(1, 1)
    m_ring(1 - xh)
    for d in (1, 3):
        pass_on(0, early, 0, d)
    m_end(1 - xh)
    lax.fori_loop(late * 4, late * 4 + 4, norm_second, 0)
    project_tiles(0, 3, late)
    own.append(first_stage(0, late, 1))
    pass_on(0, early, 0, 2)
    for d in (1, 3):
        pass_on(1, early, 0, d)
    project_tiles(3, 5, late)
    own.append(first_stage(1, late, 1))
    w_ring(xl, 1)
    pass_on(1, early, 0, 2)
    relay(0, early, 0, 0)
    w_ring(1 - xl, 1)
    for lane in (0, 1):
        for d in (1, 3):
            pass_on(lane, late, 1, d)
    for d in (1, 3):
        relay(0, early, 0, d)
    for lane in (0, 1):
        pass_on(lane, late, 1, 2)
    p_first()
    w_far(xl, 1)
    w_far(1 - xl, 1)
    w_last(1)
    project_tiles(5, 7, early)
    send_queries(early, 0)
    project_tiles(5, 7, late)
    send_queries(late, 1)
    p_second()
    relay(0, early, 0, 2)
    for d in (0, 1, 3, 2):
        relay(1, early, 0, d)
    p_third()
    for lane in (0, 1):
        for d in (0, 1, 3, 2):
            relay(lane, late, 1, d)
    for half in (0, 1):
        for zz in range(4):
            for side in (0, 1):
                for lane in (0, 1):
                    block_wait(lane, seq_at(zz, side, 1 - core), half)
    for one in own:
        one.wait()
    for d in range(1, 16):
        block = lax.rem(s + d, 16)
        copy_to(q_out.at[block], q_out.at[block], q_send.at[0, 0, 0], q_recv.at[block], (block, c)).wait_recv()
    own_p.wait()
    p_last()
    for one in waits:
        one.wait_send()


def front(*operands):
    dma = pltpu.SemaphoreType.DMA
    vm, anyw = pl.BlockSpec(memory_space=VMEM), pl.BlockSpec(memory_space=pl.ANY)
    return pl.pallas_call(
        front_kernel,
        out_shape=(
            jax.ShapeDtypeStruct((8, 64, 2560), BF16),
            jax.ShapeDtypeStruct((16, 160, 512), BF16),
            jax.ShapeDtypeStruct((16, 160, 512), BF16),
            jax.ShapeDtypeStruct((16, 160, 128), BF16),
            jax.ShapeDtypeStruct((2560, 640), BF16),
        ),
        in_specs=[pl.BlockSpec(memory_space=pltpu.SMEM), anyw, vm, anyw, anyw, anyw, anyw, vm, vm, vm, vm,
                  anyw, anyw, vm, anyw, anyw, anyw, anyw],
        out_specs=(vm, anyw, anyw, vm, anyw),
        scratch_shapes=[
            VMEM((8, 64, 2560), BF16),
            VMEM((2560, 640), BF16),
            VMEM((2560, 640), BF16),
            VMEM((2560, 256), BF16),
            VMEM((2560, 10), BF16),
            VMEM((640, 2560), BF16),
            VMEM((640, 160), BF16),
            VMEM((8, 128), F32),
            VMEM((5120, 1920), BF16),
            VMEM((512, 5120), BF16),
            VMEM((8, 64, 2560), BF16),
            VMEM((1920, 512), BF16),
            VMEM((512, 640), F32),
            VMEM((512, 640), F32),
            VMEM((512, 640), F32),
            VMEM((4, 64, 640), F32),
            VMEM((2, 64, 640), BF16),
            VMEM((2, 64, 640), BF16),
            VMEM((4, 64, 640), BF16),
            VMEM((2, 8, 640), F32),
            VMEM((2, 8, 640), F32),
            VMEM((4, 8, 640), F32),
            VMEM((512, 128), F32),
            VMEM((128, 512), F32),
            VMEM((512, 640), F32),
            VMEM((512, 128), BF16),
            VMEM((128, 512), BF16),
            VMEM((160, 640), BF16),
            VMEM((8, 1, 512), F32),
            VMEM((512, 128), F32),
            VMEM((512, 640), BF16),
            dma((11,)),
            dma((60,)),
            dma((16, 2, 2)),
            dma((15,)),
            dma((16,)),
            dma((10,)),
            dma((12,)),
            dma((7,)),
            dma((8,)),
            *ring_scratch(64, 2560),
            dma((18,)),
            dma((8, 2)),
            dma((2, 2, 3)),
            dma((2, 2, 4)),
            dma((2, 2, 4)),
            dma((2, 2, 4)),
            dma((16, 2)),
            dma((16, 2)),
            dma((2, 4, 2)),
            dma((16,)),
            dma((2, 2)),
            dma((1,)),
        ],
        compiler_params=pltpu.CompilerParams(
            collective_id=0, has_side_effects=True, vmem_limit_bytes=67043328
        ),
        name="front",
    )(*operands)


def boundary(segments, value):
    count = jnp.int32(0)
    for bit in range(12, -1, -1):
        step = 1 << bit
        count = jnp.where(segments[count + step - 1] < value, count + step, count)
    return jnp.where(segments[jnp.minimum(count, 8191)] < value, count + 1, count)


def attend_kernel(segments, q_in, k_in, v_in, out, landed, keys, values, k_sem, v_sem):
    quarter = lax.rem(lax.axis_index("seq"), 4)

    def loads(j):
        return [
            pltpu.make_async_copy(src.at[2 * j + side], dst.at[j, :, pl.ds(side * 512, 512)], sem.at[2 * j + side])
            for side in (0, 1) for src, dst, sem in ((k_in, landed, k_sem), (v_in, values, v_sem))
        ]

    for j in range(8):
        for one in loads(j):
            one.start()
    first, second = boundary(segments, 1), boundary(segments, 2)
    scale = (AP ** -0.5) * 1.4426950408889634
    lane = lax.broadcasted_iota(jnp.int32, (1, 256), 1)

    def tile(i, _):
        for one in loads(i):
            one.wait()
        keys[i] = landed[i].astype(F32).T.astype(BF16)
        queries = jnp.concatenate([q_in[2 * i], q_in[2 * i + 1]], axis=1)
        low_place = i * 1024 + quarter * 128
        place = low_place + lane + jnp.where(lane >= 128, 384, 0)
        begin = start_of(place, first, second)
        lowest = start_of(low_place, first, second) // 1024
        plain_from = jnp.minimum((start_of(low_place + 639, first, second) + 1023) // 1024, i)

        def step(j, carry, masked):
            top, total, acc = carry
            scores = jnp.dot(keys[j], queries, preferred_element_type=F32)
            if masked:
                key = j * 1024 + lax.broadcasted_iota(jnp.int32, (1024, 256), 0)
                visible = (key >= begin) & (key <= place)
                scores = jnp.where(visible, scores, -1e30)
            new_top = jnp.maximum(top, jnp.max(scores, axis=0, keepdims=True))
            weights = jnp.exp2((scores - new_top) * scale)
            if masked:
                weights = jnp.where(visible, weights, 0.0)
            keep = jnp.exp2((top - new_top) * scale)
            total = total * keep + jnp.sum(weights, axis=0, keepdims=True)
            acc = acc * keep + jnp.dot(values[j], weights.astype(BF16), preferred_element_type=F32)
            return new_top, total, acc

        carry = (jnp.full((1, 256), -1e30, F32), jnp.zeros((1, 256), F32), jnp.zeros((AP, 256), F32))
        carry = lax.fori_loop(lowest, plain_from, lambda j, t: step(j, t, True), carry)
        carry = lax.fori_loop(jnp.maximum(lowest, plain_from), i, lambda j, t: step(j, t, False), carry)
        top, total, acc = step(i, carry, True)
        context = (acc / total).astype(BF16)
        out[2 * i] = context[:, :128]
        out[2 * i + 1] = context[:, 128:]
        return 0

    lax.fori_loop(0, 8, tile, 0)


def attend(segments, q_in, k_in, v_in):
    vm, anyw = pl.BlockSpec(memory_space=VMEM), pl.BlockSpec(memory_space=pl.ANY)
    return pl.pallas_call(
        attend_kernel,
        out_shape=jax.ShapeDtypeStruct((16, 160, 128), BF16),
        in_specs=[pl.BlockSpec(memory_space=pltpu.SMEM), vm, anyw, anyw],
        out_specs=vm,
        scratch_shapes=[
            VMEM((8, 160, 1024), BF16),
            VMEM((8, 1024, 160), BF16),
            VMEM((8, 160, 1024), BF16),
            pltpu.SemaphoreType.DMA((16,)),
            pltpu.SemaphoreType.DMA((16,)),
        ],
        compiler_params=pltpu.CompilerParams(vmem_limit_bytes=LIMIT),
        name="attend",
    )(segments, q_in, k_in, v_in)


def finish_kernel(ctx, proj_t, out, gathered, part, in_send, in_recv, ring, fin, comb, across, rs_send, rs_recv, local_sem):
    s, c = lax.axis_index("seq"), lax.axis_index("chan")
    peers = chan_peers(s, c)
    greet([(s, p) for p in peers] + [(lax.rem(s + d, 16), c) for d in range(1, 16)])
    z = s // 4
    lanes = pl.ds(pl.multiple_of(lax.rem(s, 4) * 128, 128), 128)
    waits = []
    for d in range(16):
        to = lax.rem(s + d, 16)
        where = gathered.at[pl.ds(pl.multiple_of(z * 160, 32), 160), lanes]
        if d == 0:
            own = pltpu.make_async_copy(ctx.at[s], where, local_sem.at[0])
            own.start()
        else:
            one = copy_to(ctx.at[to], where, in_send.at[d - 1], in_recv.at[s], (to, c))
            one.start()
            waits.append(one)
    own.wait()
    for d in range(1, 16):
        block = lax.rem(s + d, 16)
        where = gathered.at[pl.ds(pl.multiple_of((block // 4) * 160, 32), 160),
                            pl.ds(pl.multiple_of(lax.rem(block, 4) * 128, 128), 128)]
        copy_to(ctx.at[0], where, in_send.at[0], in_recv.at[block], (block, c)).wait_recv()
    gather = ChanSum(s, c, part, ring, fin, comb, across, rs_send, rs_recv)

    def make(turn):
        def rows_of(n, _):
            p = gather.column(turn) * 4 + n
            at = pl.ds(pl.multiple_of(p * 320, 32), 320)
            part[p] = jnp.dot(proj_t[at, :], gathered[...], preferred_element_type=F32).astype(BF16)
            return 0

        lax.fori_loop(0, 4, rows_of, 0)

    make(0)
    gather.first(0)
    make(1)
    gather.second(0)
    gather.first(1)
    gather.second(1)
    gather.cross()
    gather.close()
    for n in range(2):
        at = pl.ds(n * 256, 256)
        out[at, :] = gather.result(at).T
    for one in waits + gather.sent:
        one.wait_send()


def finish(ctx, proj_t):
    dma = pltpu.SemaphoreType.DMA
    vm = pl.BlockSpec(memory_space=VMEM)
    return pl.pallas_call(
        finish_kernel,
        out_shape=jax.ShapeDtypeStruct((512, 320), F32),
        in_specs=[vm, vm],
        out_specs=vm,
        scratch_shapes=[
            VMEM((640, 512), BF16),
            VMEM((8, 320, 512), BF16),
            dma((15,)),
            dma((16,)),
            *ring_scratch(320, 512),
            dma((1,)),
        ],
        compiler_params=pltpu.CompilerParams(
            collective_id=2, has_side_effects=True, vmem_limit_bytes=40 * 1024 * 1024
        ),
        cost_estimate=pl.CostEstimate(flops=50_000_000_000, bytes_accessed=6_000_000, transcendentals=0),
        name="finish",
    )(ctx, proj_t)


def local(
    hidden,
    embedding,
    segments,
    input_norm_gain,
    gate_proj,
    input_proj,
    state_proj,
    step_proj,
    step_bias,
    decay_log,
    skip_gain,
    out_gain,
    out_proj,
    attn_gain,
    query_proj,
    key_proj,
    value_proj,
    attn_out,
):
    chan_index = lax.axis_index("chan")
    mixed, k_all, v_all, q_all, proj_t = front(
        segments, hidden.reshape(8, 64, 2560), input_norm_gain[None, :], input_proj, gate_proj, state_proj,
        step_proj, step_bias[None, :], decay_log[None, :], skip_gain[None, :], out_gain[None, :],
        out_proj, embedding.reshape(8, 64, 2560), attn_gain[None, :], key_proj, value_proj, query_proj,
        attn_out,
    )
    ctx = attend(segments, q_all, k_all, v_all)
    out_share = finish(ctx, proj_t)
    own_mixed = lax.dynamic_slice_in_dim(mixed.reshape(512, 2560), chan_index * 320, 320, 1)
    return (out_share + own_mixed.astype(jnp.float32)).astype(jnp.bfloat16)


def solution(mesh):
    in_specs = (
        P("seq", None),
        P("seq", None),
        P(),
        P(),
        P(None, "chan"),
        P(None, "chan"),
        P(),
        P(None, "chan"),
        P("chan"),
        P("chan"),
        P("chan"),
        P("chan"),
        P("chan", None),
        P(),
        P("seq", "chan"),
        P("seq", "chan"),
        P("seq", "chan"),
        P("chan", "seq"),
    )
    out_specs = P("seq", "chan")
    return jax.shard_map(local, mesh=mesh, in_specs=in_specs, out_specs=out_specs, check_vma=False)
```

```python
import jax
import jax.numpy as jnp
from jax import lax
from jax.experimental import pallas as pl
from jax.experimental.pallas import tpu as pltpu
from jax.sharding import PartitionSpec as P

N = 64
HEAD_CHANNELS = 64
AP = 160
EPSILON = 1e-05
MESH = pl.DeviceIdType.MESH
VMEM = pltpu.VMEM
F32 = jnp.float32
BF16 = jnp.bfloat16


def greet(peers):
    barrier = pltpu.get_barrier_semaphore()
    for peer in peers:
        pl.semaphore_signal(barrier, inc=1, device_id=peer, device_id_type=MESH)
    pl.semaphore_wait(barrier, len(peers))


def copy_to(src, dst, send, recv, where):
    return pltpu.make_async_remote_copy(
        src_ref=src, dst_ref=dst, send_sem=send, recv_sem=recv,
        device_id=where, device_id_type=MESH,
    )


OFFSETS = ((1, 2), (1, 1), (1, 3), (0, 2), (1, 0), (0, 1), (0, 3))


def chan_peers(s, c):
    half, place = c // 4, lax.rem(c, 4)
    return [lax.rem(half + a, 2) * 4 + lax.rem(place + b, 4) for a, b in OFFSETS]


def chan_sources(s, c):
    half, place = c // 4, lax.rem(c, 4)
    return [lax.rem(half + a, 2) * 4 + lax.rem(place + 4 - b, 4) for a, b in OFFSETS]


def seq_parts(s):
    return s // 4, lax.rem(s // 2, 2), lax.rem(s, 2)


def seq_at(z, xl, core):
    return z * 4 + xl * 2 + core


class ChanSum:
    def __init__(self, s, c, part, ring, fin, comb, across, send_sem, recv_sem):
        self.s, self.part, self.ring, self.fin = s, part, ring, fin
        self.comb, self.across, self.send_sem, self.recv_sem = comb, across, send_sem, recv_sem
        self.rows, self.width = part.shape[1] // 2, part.shape[2]
        self.xh, self.yy = c // 4, lax.rem(c, 4)
        self.up = lax.rem(self.yy + 1, 4)
        self.down = lax.rem(self.yy + 3, 4)
        self.far = lax.rem(self.yy + 2, 4)
        self.sent = []

    def column(self, turn):
        return 1 - self.xh if turn == 0 else self.xh

    def side(self, ref, half):
        return ref.at[pl.ds(half * self.rows, self.rows), :]

    def piece(self, turn, y, half):
        return self.side(self.part.at[self.column(turn) * 4 + y], half)

    def copy(self, i, src, dst, y, turn=1):
        to = self.column(turn) * 4 + y
        return copy_to(src, dst, self.send_sem.at[i], self.recv_sem.at[i], (self.s, to))

    def send(self, i, src, dst, y, turn=1):
        one = self.copy(i, src, dst, y, turn)
        one.start()
        self.sent.append(one)

    def wait(self, i, dst):
        self.copy(i, dst, dst, self.up).wait_recv()

    def first(self, turn):
        i = 6 * turn
        self.send(i, self.piece(turn, self.far, 0), self.ring.at[turn, 0], self.up)
        self.send(i + 2, self.piece(turn, self.far, 1), self.ring.at[turn, 1], self.down)
        self.send(i + 1, self.piece(turn, self.up, 1), self.side(self.fin.at[turn, 0], 1), self.up)
        self.send(i + 3, self.piece(turn, self.down, 0), self.side(self.fin.at[turn, 1], 0), self.down)

    def second(self, turn):
        for way, y in ((0, self.up), (1, self.down)):
            self.wait(6 * turn + 2 * way, self.ring.at[turn, way])
            mine, its, both = self.piece(turn, y, way), self.ring.at[turn, way], self.comb.at[turn, way]

            def add(n, _):
                at = pl.ds(pl.multiple_of(n * 256, 256), 256)
                both[:, at] = (mine[:, at].astype(F32) + its[:, at].astype(F32)).astype(BF16)
                return 0

            lax.fori_loop(0, self.width // 256, add, 0)
            self.send(6 * turn + 4 + way, both, self.side(self.fin.at[turn, way], way), y)

    def arrived(self, turn):
        i = 6 * turn
        for way in (0, 1):
            self.wait(i + 1 + 2 * way, self.side(self.fin.at[turn, way], 1 - way))
            self.wait(i + 4 + way, self.side(self.fin.at[turn, way], way))

    def total(self, turn, at):
        value = self.part[self.column(turn) * 4 + self.yy, :, at].astype(F32)
        return value + self.fin[turn, 0, :, at].astype(F32) + self.fin[turn, 1, :, at].astype(F32)

    def cross(self):
        self.arrived(0)
        own = self.column(0) * 4 + self.yy

        def add(n, _):
            at = pl.ds(pl.multiple_of(n * 256, 256), 256)
            self.part[own, :, at] = self.total(0, at).astype(BF16)
            return 0

        lax.fori_loop(0, self.width // 256, add, 0)
        self.send(12, self.part.at[own], self.across, self.yy, 0)

    def close(self):
        self.arrived(1)
        self.wait(12, self.across)

    def result(self, at):
        return self.total(1, at) + self.across[:, at].astype(F32)


def ring_scratch(rows, width):
    return [
        VMEM((2, 2, rows // 2, width), BF16),
        VMEM((2, 2, rows, width), BF16),
        VMEM((2, 2, rows // 2, width), BF16),
        VMEM((rows, width), BF16),
        pltpu.SemaphoreType.DMA((13,)),
        pltpu.SemaphoreType.DMA((13,)),
    ]


def start_of(place, first, second):
    return jnp.where(place >= second, second, jnp.where(place >= first, first, 0))


def silu(v):
    return v / (1.0 + jnp.exp(-v))


def front_kernel(segments, hidden, norm_gain, input_w, gate_w, state_w, step_w, bias, decay, skip, out_gain,
                 out_w, embedding, attn_gain, wk, wv, wq, p_in,
                 mixed_out, k_out, v_out, q_out, p_out,
                 mixed, hid, iw, gw, sw, dw, dwt, ow, vec, w, rows_in, part, flat_t, run_e, xs, ys, states, tx, rx, planes, tx_t, rx_t, planes_t,
                 run_rows, run_cols, step_e, bc_rows, bc_cols, pb, sq_all, sq_cols, weighted,
                 load_sem, w_send, w_recv, p_send, p_recv, st_send, st_recv,
                 sq_send, sq_recv, ring, fin, comb, across, rs_send, rs_recv, ag_send, ag_recv,
                 z_send, x_send, d_send, f_send, k_recv, v_recv, q_send, q_recv, local_sem, own_sem):
    s, c = lax.axis_index("seq"), lax.axis_index("chan")
    z, xl, core = seq_parts(s)
    peers, sources = chan_peers(s, c), chan_sources(s, c)
    up, down, far = lax.rem(z + 1, 4), lax.rem(z + 3, 4), lax.rem(z + 2, 4)
    waits = []

    def load(i, src, dst):
        one = pltpu.make_async_copy(src, dst, load_sem.at[i])
        one.start()
        return one

    own_rows = pl.ds(pl.multiple_of(s * 320, 64), 320)
    w_loads = [load(i, src, w.at[own_rows, pl.ds(i * 640, 640)]) for i, src in enumerate((wk, wv, wq))]
    l_hid = load(3, hidden, hid)
    l_sw = load(4, state_w, sw)
    l_dw = load(10, step_w, dw)
    l_iw = load(5, input_w, iw)
    l_pb = load(6, p_in, pb)
    l_gw = load(7, gate_w, gw)
    l_ow = load(8, out_w, ow)
    greet([(s, p) for p in peers] + [(lax.rem(s + d, 16), c) for d in range(1, 16)])

    used = [0, 0]
    sibling = seq_at(z, xl, 1 - core)

    def w_rows(block, half, group):
        rows = pl.ds(pl.multiple_of(block * 320 + half * 160, 32), 160)
        return w.at[rows, pl.ds(1280 * group, 1280 - 640 * group)]

    def w_to(block, half, group, to):
        rows = w_rows(block, half, group)
        one = copy_to(rows, rows, w_send.at[used[0]], w_recv.at[block, half, group], (to, c))
        used[0] += 1
        one.start()
        waits.append(one)

    def w_wait(block, half, group):
        rows = w_rows(block, half, group)
        copy_to(rows, rows, w_send.at[0], w_recv.at[block, half, group], (sibling, c)).wait_recv()

    def p_rows(block):
        return p_out.at[pl.ds(pl.multiple_of(block * 160, 32), 160), :]

    def p_to(block, to, src=None):
        rows = p_rows(block)
        one = copy_to(rows if src is None else src, rows, p_send.at[used[1]], p_recv.at[block], (to, c))
        used[1] += 1
        one.start()
        waits.append(one)

    def p_wait(block):
        rows = p_rows(block)
        copy_to(rows, rows, p_send.at[0], p_recv.at[block], (seq_at(z, xl, 1 - core), c)).wait_recv()

    def w_across(half, group):
        w_to(s, half, group, seq_at(z, 1 - xl, core))

    def w_first(half, group):
        w_to(s, half, group, seq_at(up, xl, core))
        w_to(s, half, group, seq_at(down, xl, core))
        w_to(s, half, group, sibling)

    def w_second(half, group):
        block = seq_at(z, 1 - xl, core)
        w_wait(block, half, group)
        w_to(block, half, group, seq_at(up, xl, core))
        w_to(block, half, group, seq_at(down, xl, core))
        w_to(block, half, group, sibling)

    def w_ring(side, group):
        for half in (0, 1):
            w_wait(seq_at(down, side, core), half, group)
            w_wait(seq_at(up, side, core), half, group)
            if half == 0:
                w_to(seq_at(down, side, core), 0, group, seq_at(up, xl, core))
        w_to(seq_at(up, side, core), 1, group, seq_at(down, xl, core))
        for half in (0, 1):
            w_to(seq_at(down, side, core), half, group, sibling)
            w_to(seq_at(up, side, core), half, group, sibling)

    def w_far(side, group):
        for half in (0, 1):
            w_wait(seq_at(far, side, core), half, group)
            w_to(seq_at(far, side, core), half, group, sibling)

    def w_last(group):
        for zz in range(4):
            for xx in range(2):
                for half in (0, 1):
                    w_wait(seq_at(zz, xx, 1 - core), half, group)

    def p_first():
        for to in (seq_at(z, 1 - xl, core), seq_at(up, xl, core), seq_at(down, xl, core), sibling):
            p_to(s, to, pb)

    def p_second():
        block = seq_at(z, 1 - xl, core)
        p_wait(block)
        for to in (seq_at(up, xl, core), seq_at(down, xl, core), sibling):
            p_to(block, to)
        p_wait(seq_at(down, xl, core))
        p_wait(seq_at(up, xl, core))
        p_to(seq_at(down, xl, core), seq_at(up, xl, core))
        p_to(seq_at(down, xl, core), sibling)
        p_to(seq_at(up, xl, core), sibling)

    def p_third():
        p_wait(seq_at(down, 1 - xl, core))
        p_wait(seq_at(up, 1 - xl, core))
        p_to(seq_at(down, 1 - xl, core), seq_at(up, xl, core))
        p_to(seq_at(down, 1 - xl, core), sibling)
        p_to(seq_at(up, 1 - xl, core), sibling)
        p_wait(seq_at(far, xl, core))
        p_to(seq_at(far, xl, core), sibling)

    def p_last():
        p_wait(seq_at(far, 1 - xl, core))
        p_to(seq_at(far, 1 - xl, core), sibling)
        for zz in range(4):
            for xx in range(2):
                p_wait(seq_at(zz, xx, 1 - core))

    for one in w_loads:
        one.wait()
    w_first(0, 0)
    w_first(0, 1)

    first, second = boundary(segments, 1), boundary(segments, 2)
    base = s * 512
    l_hid.wait()
    norm_row = norm_gain[...].reshape(1, 2560)
    out_row = out_gain[...].reshape(1, 640)

    def norm_first(p, _):
        at = pl.ds(pl.multiple_of(p * 64, 64), 64)
        value = hid[p].astype(F32)
        factor = lax.rsqrt(jnp.sum(value * value, axis=-1, keepdims=True) / 2560.0 + EPSILON)
        rows_in[at, pl.ds(0, 2560)] = (value * factor * norm_row).astype(BF16)
        return 0

    lax.fori_loop(0, 8, norm_first, 0)
    tokens = rows_in.at[:, pl.ds(0, 2560)]
    vec[...] = jnp.zeros((8, 128), F32)
    dwt[...] = jnp.zeros((128, 2560), BF16)
    vec[0:1, 0:10] = bias[...]
    vec[1:2, 0:10] = decay[...]
    vec[2:3, 0:10] = skip[...]
    l_sw.wait()
    l_dw.wait()
    dwt[0:10, :] = dw[...]
    bc = silu(jnp.dot(tokens[...], sw[...], preferred_element_type=F32))
    bc_rows[...] = bc.astype(BF16)
    bc_cols[...] = bc.T.astype(BF16)
    logits = lax.dot_general(tokens[...], dwt[...], (((1,), (1,)), ((), ())), preferred_element_type=F32) + vec[0:1, :]
    steps = jnp.maximum(logits, 0.0) + jnp.log1p(jnp.exp(-jnp.abs(logits)))
    rate = -jnp.exp(vec[1:2, :])
    lower = (lax.broadcasted_iota(jnp.int32, (512, 512), 0)
             >= lax.broadcasted_iota(jnp.int32, (512, 512), 1)).astype(F32)
    running = jnp.dot(lower, steps * rate, preferred_element_type=F32, precision=lax.Precision.HIGHEST)
    spread = (lax.broadcasted_iota(jnp.int32, (128, 640), 1) // 64
              == lax.broadcasted_iota(jnp.int32, (128, 640), 0)).astype(F32)
    run_rows[...] = running
    run_cols[...] = running.T
    wide_steps = jnp.dot(steps, spread, preferred_element_type=F32, precision=lax.Precision.HIGHEST)
    run_e[...] = jnp.dot(running, spread, preferred_element_type=F32, precision=lax.Precision.HIGHEST)
    step_e[...] = wide_steps
    skip_e = jnp.dot(vec[...], spread, preferred_element_type=F32, precision=lax.Precision.HIGHEST)[2:3, :]
    l_iw.wait()

    def input_tile(n, width):
        at = pl.ds(n, width)
        xs[:, at] = silu(jnp.dot(tokens[...], iw[:, at], preferred_element_type=F32))
        step_e[:, at] = xs[:, at] * step_e[:, at]

    input_tile(0, 256)
    input_tile(256, 256)
    input_tile(512, 128)

    states[0] = jnp.zeros((64, 640), F32)
    total = None
    for k in range(4):
        rows = slice(k * 128, k * 128 + 128)
        end = run_e[k * 128 + 127:k * 128 + 128, :]
        begin_end = start_of(base + k * 128 + 127, first, second)
        place = base + k * 128 + lax.broadcasted_iota(jnp.int32, (128, 1), 0)
        keep = jnp.where(place >= begin_end, jnp.exp(end - run_e[rows, :]), 0.0)
        own = jnp.dot(bc_cols[:64, rows], (step_e[rows, :] * keep).astype(BF16), preferred_element_type=F32)
        gap = end if k == 0 else end - run_e[k * 128 - 1:k * 128, :]
        through = jnp.where(base + k * 128 - 1 >= begin_end, jnp.exp(gap), 0.0)
        if k == 0:
            total = through
            states[1] = own
        else:
            total = total * through
            if k < 3:
                states[k + 1] = through * states[k] + own
            else:
                tx[0] = (through * states[k] + own).astype(BF16)
    tx_t[0] = jnp.broadcast_to(total, (8, 640))

    def state_to(i, to):
        pair = [
            copy_to(tx_t.at[i], rx_t.at[i], st_send.at[2 * i], st_recv.at[2 * i], (to, c)),
            copy_to(tx.at[i], rx.at[i], st_send.at[2 * i + 1], st_recv.at[2 * i + 1], (to, c)),
        ]
        for one in pair:
            one.start()
            waits.append(one)
        return pair

    def joined(i, low):
        mine_s, mine_t = tx[i].astype(F32), tx_t[i, 0:1, :]
        its_s, its_t = rx[i].astype(F32), rx_t[i, 0:1, :]
        first_s, first_t = jnp.where(low, mine_s, its_s), jnp.where(low, mine_t, its_t)
        last_s, last_t = jnp.where(low, its_s, mine_s), jnp.where(low, its_t, mine_t)
        return (last_t * first_s + last_s).astype(BF16), jnp.broadcast_to(first_t * last_t, (8, 640))

    for one in state_to(0, sibling):
        one.wait_recv()
    tx[1], tx_t[1] = joined(0, core == 0)
    pair = state_to(1, seq_at(z, 1 - xl, core))
    for group in (0, 1):
        w_across(0, group)
        w_across(1, group)

    def chunk(k, _):
        at = pl.ds(pl.multiple_of(k * 128, 128), 128)
        place = base + k * 128 + lax.broadcasted_iota(jnp.int32, (128, 1), 0)
        key = base + k * 128 + lax.broadcasted_iota(jnp.int32, (1, 128), 1)
        begin = start_of(place, first, second)
        allowed = (key >= begin) & (key <= place)
        cross = jnp.dot(bc_rows[at, 64:128], bc_cols[0:64, at], preferred_element_type=F32)
        cross = jnp.where(allowed, cross, 0.0)
        lane = lax.broadcasted_iota(jnp.int32, (128, 128), 1)
        for pair in range(5):
            lanes = pl.ds(pair * 128, 128)
            scaled = step_e[at, lanes].astype(BF16)
            halves = []
            for h in (2 * pair, 2 * pair + 1):
                gap = run_rows[at, h:h + 1] - run_cols[h:h + 1, at]
                decay = jnp.exp(jnp.where(allowed, gap, -1e30))
                halves.append(jnp.dot((decay * cross).astype(BF16), scaled, preferred_element_type=F32))
            ys[at, lanes] = jnp.where(lane < 64, halves[0], halves[1])
        return 0

    lax.fori_loop(0, 2, chunk, 0)
    for one in pair:
        one.wait_recv()
    planes[z], planes_t[z] = joined(1, xl == 0)
    for d in (2, 1, 3):
        to = (seq_at(lax.rem(z + d, 4), xl, core), c)
        for one in (
            copy_to(planes_t.at[z], planes_t.at[z], st_send.at[2 + 2 * d], st_recv.at[4 + 2 * z], to),
            copy_to(planes.at[z], planes.at[z], st_send.at[3 + 2 * d], st_recv.at[5 + 2 * z], to),
        ):
            one.start()
            waits.append(one)
    w_first(1, 0)
    l_pb.wait()
    own_p = pltpu.make_async_copy(pb, p_rows(s), own_sem.at[0])
    own_p.start()
    lax.fori_loop(2, 4, chunk, 0)

    for k in range(1, 4):
        rows = slice(k * 128, k * 128 + 128)
        place = base + k * 128 + lax.broadcasted_iota(jnp.int32, (128, 1), 0)
        begin = start_of(place, first, second)
        enter = jnp.where(base + k * 128 - 1 >= begin,
                          jnp.exp(run_e[rows, :] - run_e[k * 128 - 1:k * 128, :]), 0.0)
        ys[rows, :] += enter * jnp.dot(bc_rows[rows, 64:128], states[k].astype(BF16), preferred_element_type=F32)

    l_gw.wait()
    for n, width in ((0, 256), (256, 256), (512, 128)):
        at = pl.ds(n, width)
        step_e[:, at] = silu(jnp.dot(tokens[...], gw[:, at], preferred_element_type=F32))

    enter_s = jnp.zeros((64, 640), F32)
    for d in (1, 2, 3):
        zz = lax.rem(z + d, 4)
        of = (seq_at(zz, xl, core), c)
        copy_to(planes_t.at[zz], planes_t.at[zz], st_send.at[0], st_recv.at[4 + 2 * zz], of).wait_recv()
        copy_to(planes.at[zz], planes.at[zz], st_send.at[0], st_recv.at[5 + 2 * zz], of).wait_recv()
    for zz in range(3):
        enter_s = jnp.where(zz < z, planes_t[zz, 0:1, :] * enter_s + planes[zz].astype(F32), enter_s)
    for i, low in ((1, xl == 0), (0, core == 0)):
        first_s = jnp.where(low, tx[i].astype(F32), rx[i].astype(F32))
        first_t = jnp.where(low, tx_t[i, 0:1, :], rx_t[i, 0:1, :])
        enter_s = jnp.where(low, enter_s, first_t * enter_s + first_s)
    states[0] = enter_s

    def gating(k, _):
        at = pl.ds(pl.multiple_of(k * 128, 128), 128)
        place = base + k * 128 + lax.broadcasted_iota(jnp.int32, (128, 1), 0)
        begin = start_of(place, first, second)
        enter = jnp.where(base - 1 >= begin, jnp.exp(run_e[at, :]), 0.0)
        y = ys[at, :] + enter * jnp.dot(bc_rows[at, 64:128], states[0].astype(BF16), preferred_element_type=F32)
        y = y + xs[at, :] * skip_e
        gated = y * step_e[at, :]
        sq_cols[at, :] = jnp.broadcast_to(jnp.sum(gated * gated, axis=-1, keepdims=True), (128, 128))
        weighted[at, :] = (gated * out_row).astype(BF16)
        return 0

    w_second(0, 0)
    lax.fori_loop(0, 4, gating, 0)
    sq_all[c] = sq_cols[...].T[0:1, :]
    l_ow.wait()

    gather = ChanSum(s, c, part, ring, fin, comb, across, rs_send, rs_recv)

    def make(turn):
        rows = pl.ds(pl.multiple_of(gather.column(turn) * 256, 256), 256)
        first_piece = gather.column(turn) * 4

        def columns(n, _):
            at = pl.ds(pl.multiple_of(n * 256, 256), 256)
            tile = jnp.dot(weighted[rows, :], ow[:, at], preferred_element_type=F32)
            part[pl.ds(first_piece, 4), :, at] = tile.astype(BF16).reshape(4, 64, 256)
            return 0

        lax.fori_loop(0, 10, columns, 0)

    make(0)
    gather.first(0)
    for i, p in enumerate(peers):
        few = copy_to(sq_all.at[c], sq_all.at[c], sq_send.at[i], sq_recv.at[c], (s, p))
        few.start()
        waits.append(few)
    make(1)
    gather.second(0)
    gather.first(1)
    w_second(1, 0)
    w_ring(xl, 0)
    gather.second(1)
    gather.cross()
    for i, p in enumerate(sources):
        copy_to(sq_all.at[p], sq_all.at[p], sq_send.at[0], sq_recv.at[p], (s, p)).wait_recv()
    gather.close()
    own64 = pl.ds(pl.multiple_of(c * 64, 64), 64)
    squares = sq_all[0]
    for i in range(1, 8):
        squares = squares + sq_all[i]
    sq_cols[...] = jnp.broadcast_to(squares, (128, 512)).T
    factor = lax.rsqrt(sq_cols[own64, 0:1] / 5120.0 + EPSILON)

    def gather_sum(n, _):
        at = pl.ds(pl.multiple_of(n * 256, 256), 256)
        mixed[c, :, at] = (hid[c, :, at].astype(F32) + gather.result(at) * factor).astype(BF16)
        return 0

    lax.fori_loop(0, 10, gather_sum, 0)
    xh, yy = c // 4, lax.rem(c, 4)
    y_up, y_down, y_far = lax.rem(yy + 1, 4), lax.rem(yy + 3, 4), lax.rem(yy + 2, 4)
    shared = [0]

    def m_rows(piece, side):
        return mixed.at[piece, pl.ds(side * 32, 32), :]

    def m_to(piece, side, to):
        rows = m_rows(piece, side)
        one = copy_to(rows, rows, ag_send.at[shared[0]], ag_recv.at[piece, side], (s, to))
        shared[0] += 1
        one.start()
        waits.append(one)

    def m_wait(piece, side):
        rows = m_rows(piece, side)
        copy_to(rows, rows, ag_send.at[0], ag_recv.at[piece, side], (s, (1 - xh) * 4 + yy)).wait_recv()

    def m_spread(piece):
        for side in (0, 1):
            m_to(piece, side, xh * 4 + y_up)
            m_to(piece, side, xh * 4 + y_down)

    def m_ring(col):
        for side in (0, 1):
            m_wait(col * 4 + y_down, side)
            m_wait(col * 4 + y_up, side)
            if side == 0:
                m_to(col * 4 + y_down, 0, xh * 4 + y_up)
        m_to(col * 4 + y_up, 1, xh * 4 + y_down)

    def m_end(col):
        for side in (0, 1):
            m_wait(col * 4 + y_far, side)

    for side in (0, 1):
        m_to(c, side, (1 - xh) * 4 + yy)
    m_spread(c)
    for one in gather.sent:
        one.wait_send()
    l_emb = load(9, embedding, part)
    w_ring(1 - xl, 0)
    w_first(1, 1)
    w_second(0, 1)
    m_ring(xh)
    for side in (0, 1):
        m_wait((1 - xh) * 4 + yy, side)
    m_spread((1 - xh) * 4 + yy)
    l_emb.wait()
    w_far(xl, 0)
    m_end(xh)

    def norm_second(p, _):
        at = pl.ds(pl.multiple_of(p * 64, 64), 64)
        top = mixed[p].astype(F32)
        low = part[p].astype(F32)
        mean = (jnp.sum(top * top, axis=-1, keepdims=True)
                + jnp.sum(low * low, axis=-1, keepdims=True)) / 5120.0
        scale = lax.rsqrt(mean + EPSILON)
        rows_in[at, pl.ds(0, 2560)] = (top * scale * attn_gain[:, pl.ds(0, 2560)]).astype(BF16)
        rows_in[at, pl.ds(2560, 2560)] = (low * scale * attn_gain[:, pl.ds(2560, 2560)]).astype(BF16)
        return 0

    def project_tiles(low, high, half):
        tokens_at = pl.ds(pl.multiple_of(half * 256, 256), 256)

        def project_tile(n, _):
            at = pl.ds(pl.multiple_of(n * 256, 256), 256)
            value = jnp.dot(rows_in[tokens_at, :], w[:, at], preferred_element_type=F32)
            flat_t[at, tokens_at] = value.T.astype(BF16)
            return 0

        lax.fori_loop(low, high, project_tile, 0)
        if high == 7:
            last = pl.ds(1792, 128)
            value = jnp.dot(rows_in[tokens_at, :], w[:, last], preferred_element_type=F32)
            flat_t[last, tokens_at] = value.T.astype(BF16)

    outs, recvs = (k_out, v_out), (k_recv, v_recv)

    def landing(lane, block, half):
        return outs[lane].at[block, :, pl.ds(pl.multiple_of(half * 256, 256), 256)]

    def head_rows(lane, head, half):
        return flat_t.at[pl.ds(pl.multiple_of(lane * 640 + head * 160, 32), 160),
                         pl.ds(pl.multiple_of(half * 256, 256), 256)]

    def first_stage(lane, half, turn):
        mine = pltpu.make_async_copy(head_rows(lane, z, half), landing(lane, s, half), local_sem.at[lane, turn])
        mine.start()
        for d in (2, 1, 3):
            to = lax.rem(z + d, 4)
            one = copy_to(head_rows(lane, to, half), landing(lane, s, half), z_send.at[lane, turn, d - 1],
                          recvs[lane].at[s, half], (seq_at(to, xl, core), c))
            one.start()
            waits.append(one)
        for there, sem in ((seq_at(z, 1 - xl, core), x_send), (sibling, d_send)):
            one = copy_to(head_rows(lane, z, half), landing(lane, s, half), sem.at[lane, turn, 0],
                          recvs[lane].at[s, half], (there, c))
            one.start()
            waits.append(one)
        return mine

    def block_wait(lane, block, half):
        rows = landing(lane, block, half)
        copy_to(rows, rows, z_send.at[0, 0, 0], recvs[lane].at[block, half], (sibling, c)).wait_recv()

    def block_to(lane, block, half, sem, there):
        rows = landing(lane, block, half)
        one = copy_to(rows, rows, sem, recvs[lane].at[block, half], (there, c))
        one.start()
        waits.append(one)

    def pass_on(lane, half, turn, d):
        block = seq_at(lax.rem(z + 4 - d, 4), xl, core)
        block_wait(lane, block, half)
        block_to(lane, block, half, x_send.at[lane, turn, d], seq_at(z, 1 - xl, core))
        block_to(lane, block, half, d_send.at[lane, turn, d], sibling)

    def relay(lane, half, turn, d):
        block = seq_at(lax.rem(z + 4 - d, 4), 1 - xl, core)
        block_wait(lane, block, half)
        block_to(lane, block, half, f_send.at[lane, turn, d], sibling)

    def send_queries(half, turn):
        for d in range(4):
            for j in range(2):
                to_z = lax.rem(z + d, 4)
                to = seq_at(to_z, half, j)
                piece = flat_t.at[pl.ds(pl.multiple_of(1280 + to_z * 160, 32), 160),
                                  pl.ds(pl.multiple_of(half * 256 + j * 128, 128), 128)]
                send_query(piece, to, d, j, turn, half)

    def send_query(piece, to, d, j, turn, half):
        remote = copy_to(piece, q_out.at[s], q_send.at[turn, d, j], q_recv.at[s], (to, c))
        if d:
            remote.start()
            waits.append(remote)
        else:
            here = pltpu.make_async_copy(piece, q_out.at[s], own_sem.at[2])
            mine = (half == xl) & (j == core)
            near.append((mine, here, remote))

            @pl.when(mine)
            def _():
                here.start()

            @pl.when(jnp.logical_not(mine))
            def _():
                remote.start()

    near = []
    early, late = xh, 1 - xh
    lax.fori_loop(early * 4, early * 4 + 4, norm_second, 0)
    w_far(1 - xl, 0)
    w_last(0)
    project_tiles(0, 3, early)
    own = [first_stage(0, early, 0)]
    project_tiles(3, 5, early)
    own.append(first_stage(1, early, 0))
    w_second(1, 1)
    m_ring(1 - xh)
    for d in (1, 3):
        pass_on(0, early, 0, d)
    m_end(1 - xh)
    kept = pltpu.make_async_copy(mixed, mixed_out, own_sem.at[1])
    kept.start()
    lax.fori_loop(late * 4, late * 4 + 4, norm_second, 0)
    project_tiles(0, 3, late)
    own.append(first_stage(0, late, 1))
    pass_on(0, early, 0, 2)
    for d in (1, 3):
        pass_on(1, early, 0, d)
    project_tiles(3, 5, late)
    own.append(first_stage(1, late, 1))
    w_ring(xl, 1)
    pass_on(1, early, 0, 2)
    relay(0, early, 0, 0)
    w_ring(1 - xl, 1)
    for lane in (0, 1):
        for d in (1, 3):
            pass_on(lane, late, 1, d)
    for d in (1, 3):
        relay(0, early, 0, d)
    for lane in (0, 1):
        pass_on(lane, late, 1, 2)
    p_first()
    w_far(xl, 1)
    w_far(1 - xl, 1)
    w_last(1)
    project_tiles(5, 7, early)
    send_queries(early, 0)
    project_tiles(5, 7, late)
    send_queries(late, 1)
    p_second()
    relay(0, early, 0, 2)
    for d in (0, 1, 3, 2):
        relay(1, early, 0, d)
    for lane in (0, 1):
        for d in (0, 1, 3, 2):
            relay(lane, late, 1, d)
    p_third()
    for half in (0, 1):
        for zz in range(4):
            for side in (0, 1):
                for lane in (0, 1):
                    block_wait(lane, seq_at(zz, side, 1 - core), half)
    for one in own:
        one.wait()
    for d in range(1, 16):
        block = lax.rem(s + d, 16)
        copy_to(q_out.at[block], q_out.at[block], q_send.at[0, 0, 0], q_recv.at[block], (block, c)).wait_recv()
    own_p.wait()
    kept.wait()
    p_last()
    for mine, here, remote in near:
        @pl.when(mine)
        def _():
            here.wait()

        @pl.when(jnp.logical_not(mine))
        def _():
            remote.wait_send()

    for one in waits:
        one.wait_send()


def front(*operands):
    dma = pltpu.SemaphoreType.DMA
    vm, anyw = pl.BlockSpec(memory_space=VMEM), pl.BlockSpec(memory_space=pl.ANY)
    return pl.pallas_call(
        front_kernel,
        out_shape=(
            jax.ShapeDtypeStruct((8, 64, 2560), BF16),
            jax.ShapeDtypeStruct((16, 160, 512), BF16),
            jax.ShapeDtypeStruct((16, 160, 512), BF16),
            jax.ShapeDtypeStruct((16, 160, 128), BF16),
            jax.ShapeDtypeStruct((2560, 640), BF16),
        ),
        in_specs=[pl.BlockSpec(memory_space=pltpu.SMEM), anyw, vm, anyw, anyw, anyw, anyw, vm, vm, vm, vm,
                  anyw, anyw, vm, anyw, anyw, anyw, anyw],
        out_specs=(anyw, anyw, anyw, anyw, anyw),
        scratch_shapes=[
            VMEM((8, 64, 2560), BF16),
            VMEM((8, 64, 2560), BF16),
            VMEM((2560, 640), BF16),
            VMEM((2560, 640), BF16),
            VMEM((2560, 128), BF16),
            VMEM((10, 2560), BF16),
            VMEM((128, 2560), BF16),
            VMEM((640, 2560), BF16),
            VMEM((8, 128), F32),
            VMEM((5120, 1920), BF16),
            VMEM((512, 5120), BF16),
            VMEM((8, 64, 2560), BF16),
            VMEM((1920, 512), BF16),
            VMEM((512, 640), F32),
            VMEM((512, 640), F32),
            VMEM((512, 640), F32),
            VMEM((4, 64, 640), F32),
            VMEM((2, 64, 640), BF16),
            VMEM((2, 64, 640), BF16),
            VMEM((4, 64, 640), BF16),
            VMEM((2, 8, 640), F32),
            VMEM((2, 8, 640), F32),
            VMEM((4, 8, 640), F32),
            VMEM((512, 128), F32),
            VMEM((128, 512), F32),
            VMEM((512, 640), F32),
            VMEM((512, 128), BF16),
            VMEM((128, 512), BF16),
            VMEM((160, 640), BF16),
            VMEM((8, 1, 512), F32),
            VMEM((512, 128), F32),
            VMEM((512, 640), BF16),
            dma((11,)),
            dma((60,)),
            dma((16, 2, 2)),
            dma((15,)),
            dma((16,)),
            dma((10,)),
            dma((12,)),
            dma((7,)),
            dma((8,)),
            *ring_scratch(64, 2560),
            dma((18,)),
            dma((8, 2)),
            dma((2, 2, 3)),
            dma((2, 2, 4)),
            dma((2, 2, 4)),
            dma((2, 2, 4)),
            dma((16, 2)),
            dma((16, 2)),
            dma((2, 4, 2)),
            dma((16,)),
            dma((2, 2)),
            dma((3,)),
        ],
        compiler_params=pltpu.CompilerParams(
            collective_id=0, has_side_effects=True, vmem_limit_bytes=67043328
        ),
        name="front",
    )(*operands)


def boundary(segments, value):
    count = jnp.int32(0)
    for bit in range(12, -1, -1):
        step = 1 << bit
        count = jnp.where(segments[count + step - 1] < value, count + step, count)
    return jnp.where(segments[jnp.minimum(count, 8191)] < value, count + 1, count)


def attend_kernel(segments, q_hbm, k_in, v_in, out, q_in, landed, keys, values, q_sem, k_sem, v_sem):
    quarter = lax.rem(lax.axis_index("seq"), 4)

    def loads(j):
        return [
            pltpu.make_async_copy(src.at[4 * j + side], dst.at[j, :, pl.ds(side * 512, 512)], sem.at[4 * j + side])
            for side in range(4) for src, dst, sem in ((k_in, landed, k_sem), (v_in, values, v_sem))
        ]

    q_load = pltpu.make_async_copy(q_hbm, q_in, q_sem)
    q_load.start()
    for j in range(4):
        for one in loads(j):
            one.start()
    first, second = boundary(segments, 1), boundary(segments, 2)
    scale = (AP ** -0.5) * 1.4426950408889634
    lane = lax.broadcasted_iota(jnp.int32, (1, 512), 1)
    q_load.wait()

    def tile(i, _):
        for n in range(1):
            for one in loads(i * 1 + n):
                one.wait()
            keys[i * 1 + n] = landed[i * 1 + n].astype(F32).T.astype(BF16)
        queries = jnp.concatenate([q_in[4 * i + n] for n in range(4)], axis=1)
        low_place = i * 2048 + quarter * 128
        place = low_place + lane + 384 * (lane // 128)
        begin = start_of(place, first, second)
        lowest = start_of(low_place, first, second) // 2048
        last_begin = start_of(low_place + 1663, first, second)
        plain_from = jnp.minimum((last_begin + 2047) // 2048, i * 1)

        def step(j, carry, causal, reset):
            top, total, acc = carry
            scores = jnp.dot(keys[j], queries, preferred_element_type=F32)
            if causal or reset:
                key = j * 2048 + lax.broadcasted_iota(jnp.int32, (2048, 512), 0)
                visible = key >= begin
                if causal:
                    visible = visible & (key <= place)
                scores = jnp.where(visible, scores, -1e30)
            new_top = jnp.maximum(top, jnp.max(scores, axis=0, keepdims=True))
            weights = jnp.exp2((scores - new_top) * scale)
            keep = jnp.exp2((top - new_top) * scale)
            total = total * keep + jnp.sum(weights, axis=0, keepdims=True)
            acc = acc * keep + jnp.dot(values[j], weights.astype(BF16), preferred_element_type=F32)
            return new_top, total, acc

        carry = (jnp.full((1, 512), -1e29, F32), jnp.zeros((1, 512), F32), jnp.zeros((AP, 512), F32))
        carry = lax.fori_loop(lowest, plain_from, lambda j, t: step(j, t, False, True), carry)
        carry = lax.fori_loop(
            jnp.maximum(lowest, plain_from), i * 1, lambda j, t: step(j, t, False, False), carry)
        top, total, acc = lax.fori_loop(
            jnp.maximum(lowest, i * 1), i * 1 + 1, lambda j, t: step(j, t, True, True), carry)
        context = (acc / total).astype(BF16)
        for n in range(4):
            out[4 * i + n] = context[:, n * 128:n * 128 + 128]
        return 0

    lax.fori_loop(0, 4, tile, 0)


def attend(segments, q_in, k_in, v_in):
    vm, anyw = pl.BlockSpec(memory_space=VMEM), pl.BlockSpec(memory_space=pl.ANY)
    return pl.pallas_call(
        attend_kernel,
        out_shape=jax.ShapeDtypeStruct((16, 160, 128), BF16),
        in_specs=[pl.BlockSpec(memory_space=pltpu.SMEM), anyw, anyw, anyw],
        out_specs=vm,
        scratch_shapes=[
            VMEM((16, 160, 128), BF16),
            VMEM((4, 160, 2048), BF16),
            VMEM((4, 2048, 160), BF16),
            VMEM((4, 160, 2048), BF16),
            pltpu.SemaphoreType.DMA,
            pltpu.SemaphoreType.DMA((16,)),
            pltpu.SemaphoreType.DMA((16,)),
        ],
        compiler_params=pltpu.CompilerParams(vmem_limit_bytes=67043328),
        name="attend",
    )(segments, q_in, k_in, v_in)


def finish_kernel(ctx, proj_in, mixed, out, proj_t, own_in, gathered, part, in_send, in_recv, ring, fin, comb, across, rs_send, rs_recv, local_sem):
    s, c = lax.axis_index("seq"), lax.axis_index("chan")
    peers = chan_peers(s, c)
    proj_load = pltpu.make_async_copy(proj_in, proj_t, local_sem.at[1])
    proj_load.start()
    window = pl.ds(pl.multiple_of(c * 5 // 2 * 128, 128), 384)
    own_load = pltpu.make_async_copy(mixed.at[:, window], own_in, local_sem.at[2])
    own_load.start()
    greet([(s, p) for p in peers] + [(lax.rem(s + d, 16), c) for d in range(1, 16)])
    z = s // 4
    lanes = pl.ds(pl.multiple_of(lax.rem(s, 4) * 128, 128), 128)
    waits = []
    for d in range(16):
        to = lax.rem(s + d, 16)
        where = gathered.at[pl.ds(pl.multiple_of(z * 160, 32), 160), lanes]
        if d == 0:
            own = pltpu.make_async_copy(ctx.at[s], where, local_sem.at[0])
            own.start()
        else:
            one = copy_to(ctx.at[to], where, in_send.at[d - 1], in_recv.at[s], (to, c))
            one.start()
            waits.append(one)
    own.wait()
    for d in range(1, 16):
        block = lax.rem(s + d, 16)
        where = gathered.at[pl.ds(pl.multiple_of((block // 4) * 160, 32), 160),
                            pl.ds(pl.multiple_of(lax.rem(block, 4) * 128, 128), 128)]
        copy_to(ctx.at[0], where, in_send.at[0], in_recv.at[block], (block, c)).wait_recv()
    gather = ChanSum(s, c, part, ring, fin, comb, across, rs_send, rs_recv)

    def make(turn):
        def rows_of(n, _):
            p = gather.column(turn) * 4 + n
            at = pl.ds(pl.multiple_of(p * 320, 32), 320)
            part[p] = jnp.dot(proj_t[at, :], gathered[...], preferred_element_type=F32).astype(BF16)
            return 0

        lax.fori_loop(0, 4, rows_of, 0)

    proj_load.wait()
    make(0)
    gather.first(0)
    make(1)
    gather.second(0)
    gather.first(1)
    gather.second(1)
    gather.cross()
    own_load.wait()
    own_t_all = [own_in[n * 256:(n + 1) * 256, :].astype(F32).T for n in range(2)]
    gather.close()
    odd = lax.rem(c, 2) == 1
    for n in range(2):
        at = pl.ds(n * 256, 256)
        own_t = own_t_all[n]
        out[:, at] = (gather.result(at) + jnp.where(odd, own_t[64:, :], own_t[:320, :])).astype(BF16)
    for one in waits + gather.sent:
        one.wait_send()


def finish(ctx, proj_t, mixed):
    dma = pltpu.SemaphoreType.DMA
    vm, anyw = pl.BlockSpec(memory_space=VMEM), pl.BlockSpec(memory_space=pl.ANY)
    return pl.pallas_call(
        finish_kernel,
        out_shape=jax.ShapeDtypeStruct((320, 512), BF16),
        in_specs=[anyw, anyw, anyw],
        out_specs=vm,
        scratch_shapes=[
            VMEM((2560, 640), BF16),
            VMEM((512, 384), BF16),
            VMEM((640, 512), BF16),
            VMEM((8, 320, 512), BF16),
            dma((15,)),
            dma((16,)),
            *ring_scratch(320, 512),
            dma((3,)),
        ],
        compiler_params=pltpu.CompilerParams(
            collective_id=2, has_side_effects=True, vmem_limit_bytes=67043328
        ),
        cost_estimate=pl.CostEstimate(flops=50_000_000_000, bytes_accessed=6_000_000, transcendentals=0),
        name="finish",
    )(ctx, proj_t, mixed)


def local(
    hidden,
    embedding,
    segments,
    input_norm_gain,
    gate_proj,
    input_proj,
    state_proj,
    step_proj,
    step_bias,
    decay_log,
    skip_gain,
    out_gain,
    out_proj,
    attn_gain,
    query_proj,
    key_proj,
    value_proj,
    attn_out,
):
    mixed, k_all, v_all, q_all, proj_t = front(
        segments, hidden.reshape(8, 64, 2560), input_norm_gain, input_proj, gate_proj, state_proj,
        step_proj.T, step_bias[None, :], decay_log[None, :], skip_gain[None, :], out_gain,
        out_proj, embedding.reshape(8, 64, 2560), attn_gain[None, :], key_proj, value_proj, query_proj,
        attn_out.T,
    )
    ctx = attend(segments, q_all, k_all, v_all)
    return finish(ctx, proj_t, mixed.reshape(512, 2560)).T


def solution(mesh):
    in_specs = (
        P("seq", None),
        P("seq", None),
        P(),
        P(),
        P(None, "chan"),
        P(None, "chan"),
        P(),
        P(None, "chan"),
        P("chan"),
        P("chan"),
        P("chan"),
        P("chan"),
        P("chan", None),
        P(),
        P("seq", "chan"),
        P("seq", "chan"),
        P("seq", "chan"),
        P("chan", "seq"),
    )
    out_specs = P("seq", "chan")
    return jax.shard_map(local, mesh=mesh, in_specs=in_specs, out_specs=out_specs, check_vma=False)
```

```python
import jax
import jax.numpy as jnp
from jax import lax
from jax.experimental import pallas as pl
from jax.experimental.pallas import tpu as pltpu
from jax.sharding import PartitionSpec as P

N = 64
HEAD_CHANNELS = 64
AP = 160
EPSILON = 1e-05
MESH = pl.DeviceIdType.MESH
VMEM = pltpu.VMEM
F32 = jnp.float32
BF16 = jnp.bfloat16


def greet(peers):
    barrier = pltpu.get_barrier_semaphore()
    for peer in peers:
        pl.semaphore_signal(barrier, inc=1, device_id=peer, device_id_type=MESH)
    pl.semaphore_wait(barrier, len(peers))


def copy_to(src, dst, send, recv, where):
    return pltpu.make_async_remote_copy(
        src_ref=src, dst_ref=dst, send_sem=send, recv_sem=recv,
        device_id=where, device_id_type=MESH,
    )


OFFSETS = ((1, 2), (1, 1), (1, 3), (0, 2), (1, 0), (0, 1), (0, 3))


def chan_peers(s, c):
    half, place = c // 4, lax.rem(c, 4)
    return [lax.rem(half + a, 2) * 4 + lax.rem(place + b, 4) for a, b in OFFSETS]


def chan_sources(s, c):
    half, place = c // 4, lax.rem(c, 4)
    return [lax.rem(half + a, 2) * 4 + lax.rem(place + 4 - b, 4) for a, b in OFFSETS]


def seq_parts(s):
    return s // 4, lax.rem(s // 2, 2), lax.rem(s, 2)


def seq_at(z, xl, core):
    return z * 4 + xl * 2 + core


class ChanSum:
    def __init__(self, s, c, part, ring, fin, comb, across, send_sem, recv_sem):
        self.s, self.part, self.ring, self.fin = s, part, ring, fin
        self.comb, self.across, self.send_sem, self.recv_sem = comb, across, send_sem, recv_sem
        self.rows, self.width = part.shape[1] // 2, part.shape[2]
        self.xh, self.yy = c // 4, lax.rem(c, 4)
        self.up = lax.rem(self.yy + 1, 4)
        self.down = lax.rem(self.yy + 3, 4)
        self.far = lax.rem(self.yy + 2, 4)
        self.sent = []

    def column(self, turn):
        return 1 - self.xh if turn == 0 else self.xh

    def side(self, ref, half):
        return ref.at[pl.ds(half * self.rows, self.rows), :]

    def piece(self, turn, y, half):
        return self.side(self.part.at[self.column(turn) * 4 + y], half)

    def copy(self, i, src, dst, y, turn=1):
        to = self.column(turn) * 4 + y
        return copy_to(src, dst, self.send_sem.at[i], self.recv_sem.at[i], (self.s, to))

    def send(self, i, src, dst, y, turn=1):
        one = self.copy(i, src, dst, y, turn)
        one.start()
        self.sent.append(one)

    def wait(self, i, dst):
        self.copy(i, dst, dst, self.up).wait_recv()

    def first(self, turn):
        i = 6 * turn
        self.send(i, self.piece(turn, self.far, 0), self.ring.at[turn, 0], self.up)
        self.send(i + 2, self.piece(turn, self.far, 1), self.ring.at[turn, 1], self.down)
        self.send(i + 1, self.piece(turn, self.up, 1), self.side(self.fin.at[turn, 0], 1), self.up)
        self.send(i + 3, self.piece(turn, self.down, 0), self.side(self.fin.at[turn, 1], 0), self.down)

    def second(self, turn):
        for way, y in ((0, self.up), (1, self.down)):
            self.wait(6 * turn + 2 * way, self.ring.at[turn, way])
            mine, its, both = self.piece(turn, y, way), self.ring.at[turn, way], self.comb.at[turn, way]

            def add(n, _):
                at = pl.ds(pl.multiple_of(n * 256, 256), 256)
                both[:, at] = (mine[:, at].astype(F32) + its[:, at].astype(F32)).astype(BF16)
                return 0

            lax.fori_loop(0, self.width // 256, add, 0)
            self.send(6 * turn + 4 + way, both, self.side(self.fin.at[turn, way], way), y)

    def arrived(self, turn):
        i = 6 * turn
        for way in (0, 1):
            self.wait(i + 1 + 2 * way, self.side(self.fin.at[turn, way], 1 - way))
            self.wait(i + 4 + way, self.side(self.fin.at[turn, way], way))

    def total(self, turn, at):
        value = self.part[self.column(turn) * 4 + self.yy, :, at].astype(F32)
        return value + self.fin[turn, 0, :, at].astype(F32) + self.fin[turn, 1, :, at].astype(F32)

    def cross(self):
        self.arrived(0)
        own = self.column(0) * 4 + self.yy

        def add(n, _):
            at = pl.ds(pl.multiple_of(n * 256, 256), 256)
            self.part[own, :, at] = self.total(0, at).astype(BF16)
            return 0

        lax.fori_loop(0, self.width // 256, add, 0)
        self.send(12, self.part.at[own], self.across, self.yy, 0)

    def close(self):
        self.arrived(1)
        self.wait(12, self.across)

    def result(self, at):
        return self.total(1, at) + self.across[:, at].astype(F32)


def ring_scratch(rows, width):
    return [
        VMEM((2, 2, rows // 2, width), BF16),
        VMEM((2, 2, rows, width), BF16),
        VMEM((2, 2, rows // 2, width), BF16),
        VMEM((rows, width), BF16),
        pltpu.SemaphoreType.DMA((13,)),
        pltpu.SemaphoreType.DMA((13,)),
    ]


def start_of(place, first, second):
    return jnp.where(place >= second, second, jnp.where(place >= first, first, 0))


def three_parts(value):
    high = value.astype(BF16)
    rest = value - high.astype(F32)
    middle = rest.astype(BF16)
    low = (rest - middle.astype(F32)).astype(BF16)
    return jnp.concatenate([high, middle, low], axis=1)


def silu(v):
    return v / (1.0 + jnp.exp(-v))


def front_kernel(segments, hidden, norm_gain, input_w, gate_w, state_w, step_w, bias, decay, skip, out_gain,
                 out_w, embedding, attn_gain, wk, wv, wq, p_in,
                 mixed_out, k_out, v_out, q_out, p_out,
                 mixed, hid, iw, gw, sw, dw, dwt, ow, vec, w, rows_in, part, flat_t, run_e, xs, ys, states, tx, rx, planes, tx_t, rx_t, planes_t,
                 run_rows, run_cols, step_e, bc_rows, bc_cols, pb, sq_all, sq_cols, weighted,
                 load_sem, w_send, w_recv, p_send, p_recv, st_send, st_recv,
                 sq_send, sq_recv, ring, fin, comb, across, rs_send, rs_recv, ag_send, ag_recv,
                 z_send, x_send, d_send, f_send, k_recv, v_recv, q_send, q_recv, local_sem, own_sem):
    s, c = lax.axis_index("seq"), lax.axis_index("chan")
    z, xl, core = seq_parts(s)
    peers, sources = chan_peers(s, c), chan_sources(s, c)
    up, down, far = lax.rem(z + 1, 4), lax.rem(z + 3, 4), lax.rem(z + 2, 4)
    waits = []

    def load(i, src, dst):
        one = pltpu.make_async_copy(src, dst, load_sem.at[i])
        one.start()
        return one

    own_rows = pl.ds(pl.multiple_of(s * 320, 64), 320)
    w_loads = [load(i, src, w.at[own_rows, pl.ds(i * 640, 640)]) for i, src in enumerate((wk, wv, wq))]
    l_hid = load(3, hidden, hid)
    l_sw = load(4, state_w, sw)
    l_dw = load(10, step_w, dw)
    l_iw = load(5, input_w, iw)
    l_pb = load(6, p_in, pb)
    l_gw = load(7, gate_w, gw)
    l_ow = load(8, out_w, ow)
    greet([(s, p) for p in peers] + [(lax.rem(s + d, 16), c) for d in range(1, 16)])

    used = [0, 0]
    sibling = seq_at(z, xl, 1 - core)

    def w_rows(block, half, group):
        rows = pl.ds(pl.multiple_of(block * 320 + half * 160, 32), 160)
        return w.at[rows, pl.ds(1280 * group, 1280 - 640 * group)]

    def w_to(block, half, group, to):
        rows = w_rows(block, half, group)
        one = copy_to(rows, rows, w_send.at[used[0]], w_recv.at[block, half, group], (to, c))
        used[0] += 1
        one.start()
        waits.append(one)

    def w_wait(block, half, group):
        rows = w_rows(block, half, group)
        copy_to(rows, rows, w_send.at[0], w_recv.at[block, half, group], (sibling, c)).wait_recv()

    def p_rows(block, half):
        return p_out.at[pl.ds(pl.multiple_of(block * 160 + half * 80, 16), 80), :]

    def p_to(block, half, to, src=None):
        rows = p_rows(block, half)
        one = copy_to(rows if src is None else src, rows, p_send.at[used[1]], p_recv.at[block, half], (to, c))
        used[1] += 1
        one.start()
        waits.append(one)

    def p_wait(block, half):
        rows = p_rows(block, half)
        copy_to(rows, rows, p_send.at[0], p_recv.at[block, half], (sibling, c)).wait_recv()

    def w_across(half, group):
        w_to(s, half, group, seq_at(z, 1 - xl, core))

    def w_first(half, group):
        w_to(s, half, group, seq_at(up, xl, core))
        w_to(s, half, group, seq_at(down, xl, core))
        w_to(s, half, group, sibling)

    def w_second(half, group):
        block = seq_at(z, 1 - xl, core)
        w_wait(block, half, group)
        w_to(block, half, group, seq_at(up, xl, core))
        w_to(block, half, group, seq_at(down, xl, core))
        w_to(block, half, group, sibling)

    def w_ring(side, group):
        for half in (0, 1):
            w_wait(seq_at(down, side, core), half, group)
            w_wait(seq_at(up, side, core), half, group)
            if half == 0:
                w_to(seq_at(down, side, core), 0, group, seq_at(up, xl, core))
        w_to(seq_at(up, side, core), 1, group, seq_at(down, xl, core))
        for half in (0, 1):
            w_to(seq_at(down, side, core), half, group, sibling)
            w_to(seq_at(up, side, core), half, group, sibling)

    def w_far(side, group):
        for half in (0, 1):
            w_wait(seq_at(far, side, core), half, group)
            w_to(seq_at(far, side, core), half, group, sibling)

    def w_last(group):
        for zz in range(4):
            for xx in range(2):
                for half in (0, 1):
                    w_wait(seq_at(zz, xx, 1 - core), half, group)

    def p_first():
        for half in (0, 1):
            for to in (seq_at(z, 1 - xl, core), seq_at(up, xl, core), seq_at(down, xl, core), sibling):
                p_to(s, half, to, pb.at[pl.ds(half * 80, 80), :])

    def p_second():
        block = seq_at(z, 1 - xl, core)
        for half in (0, 1):
            p_wait(block, half)
            for to in (seq_at(up, xl, core), seq_at(down, xl, core), sibling):
                p_to(block, half, to)
        p_ring(xl)

    def p_ring(side):
        for half in (0, 1):
            p_wait(seq_at(down, side, core), half)
            p_wait(seq_at(up, side, core), half)
        p_to(seq_at(down, side, core), 0, seq_at(up, xl, core))
        p_to(seq_at(up, side, core), 1, seq_at(down, xl, core))
        for half in (0, 1):
            p_to(seq_at(down, side, core), half, sibling)
            p_to(seq_at(up, side, core), half, sibling)

    def p_third():
        p_ring(1 - xl)
        for half in (0, 1):
            p_wait(seq_at(far, xl, core), half)
            p_to(seq_at(far, xl, core), half, sibling)

    def p_last():
        for half in (0, 1):
            p_wait(seq_at(far, 1 - xl, core), half)
            p_to(seq_at(far, 1 - xl, core), half, sibling)
        for zz in range(4):
            for xx in range(2):
                for half in (0, 1):
                    p_wait(seq_at(zz, xx, 1 - core), half)

    for one in w_loads:
        one.wait()
    w_first(0, 0)
    w_first(0, 1)

    first, second = boundary(segments, 1), boundary(segments, 2)
    base = s * 512
    l_hid.wait()
    norm_row = norm_gain[...].reshape(1, 2560)
    out_row = out_gain[...].reshape(1, 640)

    def norm_first(p, _):
        at = pl.ds(pl.multiple_of(p * 64, 64), 64)
        value = hid[p].astype(F32)
        factor = lax.rsqrt(jnp.sum(value * value, axis=-1, keepdims=True) / 2560.0 + EPSILON)
        rows_in[at, pl.ds(0, 2560)] = (value * factor * norm_row).astype(BF16)
        return 0

    lax.fori_loop(0, 8, norm_first, 0)
    tokens = rows_in.at[:, pl.ds(0, 2560)]
    vec[...] = jnp.zeros((8, 128), F32)
    dwt[...] = jnp.zeros((128, 2560), BF16)
    vec[0:1, 0:10] = bias[...]
    vec[1:2, 0:10] = decay[...]
    vec[2:3, 0:10] = skip[...]
    l_sw.wait()
    l_dw.wait()
    dwt[0:10, :] = dw[...]
    bc = silu(jnp.dot(tokens[...], sw[...], preferred_element_type=F32))
    bc_rows[...] = bc.astype(BF16)
    bc_cols[...] = bc.T.astype(BF16)
    logits = lax.dot_general(tokens[...], dwt[...], (((1,), (1,)), ((), ())), preferred_element_type=F32) + vec[0:1, :]
    steps = jnp.maximum(logits, 0.0) + jnp.log1p(jnp.exp(-jnp.abs(logits)))
    rate = -jnp.exp(vec[1:2, :])
    lower = (lax.broadcasted_iota(jnp.int32, (512, 512), 0)
             >= lax.broadcasted_iota(jnp.int32, (512, 512), 1)).astype(F32).astype(BF16)
    sums = jnp.dot(lower, three_parts(steps * rate), preferred_element_type=F32)
    running = sums[:, :128] + sums[:, 128:256] + sums[:, 256:]
    spread = (lax.broadcasted_iota(jnp.int32, (384, 640), 1) // 64
              == lax.rem(lax.broadcasted_iota(jnp.int32, (384, 640), 0), 128)).astype(F32).astype(BF16)
    run_rows[...] = running
    run_cols[...] = running.T
    run_e[...] = jnp.dot(three_parts(running), spread, preferred_element_type=F32)
    step_e[...] = jnp.dot(three_parts(steps), spread, preferred_element_type=F32)
    skip_e = jnp.dot(three_parts(vec[...]), spread, preferred_element_type=F32)[2:3, :]
    l_iw.wait()

    def input_tile(n, width):
        at = pl.ds(n, width)
        xs[:, at] = silu(jnp.dot(tokens[...], iw[:, at], preferred_element_type=F32))
        step_e[:, at] = xs[:, at] * step_e[:, at]

    input_tile(0, 256)
    input_tile(256, 256)
    input_tile(512, 128)

    states[0] = jnp.zeros((64, 640), F32)
    total = None
    for k in range(4):
        rows = slice(k * 128, k * 128 + 128)
        end = run_e[k * 128 + 127:k * 128 + 128, :]
        begin_end = start_of(base + k * 128 + 127, first, second)
        place = base + k * 128 + lax.broadcasted_iota(jnp.int32, (128, 1), 0)
        keep = jnp.where(place >= begin_end, jnp.exp(end - run_e[rows, :]), 0.0)
        own = jnp.dot(bc_cols[:64, rows], (step_e[rows, :] * keep).astype(BF16), preferred_element_type=F32)
        gap = end if k == 0 else end - run_e[k * 128 - 1:k * 128, :]
        through = jnp.where(base + k * 128 - 1 >= begin_end, jnp.exp(gap), 0.0)
        if k == 0:
            total = through
            states[1] = own
        else:
            total = total * through
            if k < 3:
                states[k + 1] = through * states[k] + own
            else:
                tx[0] = (through * states[k] + own).astype(BF16)
    tx_t[0] = jnp.broadcast_to(total, (8, 640))

    def state_to(i, to):
        pair = [
            copy_to(tx_t.at[i], rx_t.at[i], st_send.at[2 * i], st_recv.at[2 * i], (to, c)),
            copy_to(tx.at[i], rx.at[i], st_send.at[2 * i + 1], st_recv.at[2 * i + 1], (to, c)),
        ]
        for one in pair:
            one.start()
            waits.append(one)
        return pair

    def joined(i, low):
        mine_s, mine_t = tx[i].astype(F32), tx_t[i, 0:1, :]
        its_s, its_t = rx[i].astype(F32), rx_t[i, 0:1, :]
        first_s, first_t = jnp.where(low, mine_s, its_s), jnp.where(low, mine_t, its_t)
        last_s, last_t = jnp.where(low, its_s, mine_s), jnp.where(low, its_t, mine_t)
        return (last_t * first_s + last_s).astype(BF16), jnp.broadcast_to(first_t * last_t, (8, 640))

    for one in state_to(0, sibling):
        one.wait_recv()
    tx[1], tx_t[1] = joined(0, core == 0)
    pair = state_to(1, seq_at(z, 1 - xl, core))
    for group in (0, 1):
        w_across(0, group)
        w_across(1, group)

    def chunk(k, _):
        at = pl.ds(pl.multiple_of(k * 128, 128), 128)
        place = base + k * 128 + lax.broadcasted_iota(jnp.int32, (128, 1), 0)
        key = base + k * 128 + lax.broadcasted_iota(jnp.int32, (1, 128), 1)
        begin = start_of(place, first, second)
        allowed = (key >= begin) & (key <= place)
        cross = jnp.dot(bc_rows[at, 64:128], bc_cols[0:64, at], preferred_element_type=F32)
        cross = jnp.where(allowed, cross, 0.0)
        lane = lax.broadcasted_iota(jnp.int32, (128, 128), 1)
        for pair in range(5):
            lanes = pl.ds(pair * 128, 128)
            scaled = step_e[at, lanes].astype(BF16)
            halves = []
            for h in (2 * pair, 2 * pair + 1):
                gap = run_rows[at, h:h + 1] - run_cols[h:h + 1, at]
                decay = jnp.exp(jnp.where(allowed, gap, -1e30))
                halves.append(jnp.dot((decay * cross).astype(BF16), scaled, preferred_element_type=F32))
            ys[at, lanes] = jnp.where(lane < 64, halves[0], halves[1])
        return 0

    lax.fori_loop(0, 2, chunk, 0)
    for one in pair:
        one.wait_recv()
    planes[z], planes_t[z] = joined(1, xl == 0)
    for d in (2, 1, 3):
        to = (seq_at(lax.rem(z + d, 4), xl, core), c)
        for one in (
            copy_to(planes_t.at[z], planes_t.at[z], st_send.at[2 + 2 * d], st_recv.at[4 + 2 * z], to),
            copy_to(planes.at[z], planes.at[z], st_send.at[3 + 2 * d], st_recv.at[5 + 2 * z], to),
        ):
            one.start()
            waits.append(one)
    w_first(1, 0)
    l_pb.wait()
    own_p = pltpu.make_async_copy(
        pb, p_out.at[pl.ds(pl.multiple_of(s * 160, 32), 160), :], own_sem.at[0])
    own_p.start()
    lax.fori_loop(2, 4, chunk, 0)

    for k in range(1, 4):
        rows = slice(k * 128, k * 128 + 128)
        place = base + k * 128 + lax.broadcasted_iota(jnp.int32, (128, 1), 0)
        begin = start_of(place, first, second)
        enter = jnp.where(base + k * 128 - 1 >= begin,
                          jnp.exp(run_e[rows, :] - run_e[k * 128 - 1:k * 128, :]), 0.0)
        ys[rows, :] += enter * jnp.dot(bc_rows[rows, 64:128], states[k].astype(BF16), preferred_element_type=F32)

    l_gw.wait()
    for n, width in ((0, 256), (256, 256), (512, 128)):
        at = pl.ds(n, width)
        step_e[:, at] = silu(jnp.dot(tokens[...], gw[:, at], preferred_element_type=F32))

    enter_s = jnp.zeros((64, 640), F32)
    for d in (1, 2, 3):
        zz = lax.rem(z + d, 4)
        of = (seq_at(zz, xl, core), c)
        copy_to(planes_t.at[zz], planes_t.at[zz], st_send.at[0], st_recv.at[4 + 2 * zz], of).wait_recv()
        copy_to(planes.at[zz], planes.at[zz], st_send.at[0], st_recv.at[5 + 2 * zz], of).wait_recv()
    for zz in range(3):
        enter_s = jnp.where(zz < z, planes_t[zz, 0:1, :] * enter_s + planes[zz].astype(F32), enter_s)
    for i, low in ((1, xl == 0), (0, core == 0)):
        first_s = jnp.where(low, tx[i].astype(F32), rx[i].astype(F32))
        first_t = jnp.where(low, tx_t[i, 0:1, :], rx_t[i, 0:1, :])
        enter_s = jnp.where(low, enter_s, first_t * enter_s + first_s)
    states[0] = enter_s

    def gating(k, _):
        at = pl.ds(pl.multiple_of(k * 128, 128), 128)
        place = base + k * 128 + lax.broadcasted_iota(jnp.int32, (128, 1), 0)
        begin = start_of(place, first, second)
        enter = jnp.where(base - 1 >= begin, jnp.exp(run_e[at, :]), 0.0)
        y = ys[at, :] + enter * jnp.dot(bc_rows[at, 64:128], states[0].astype(BF16), preferred_element_type=F32)
        y = y + xs[at, :] * skip_e
        gated = y * step_e[at, :]
        sq_cols[at, :] = jnp.broadcast_to(jnp.sum(gated * gated, axis=-1, keepdims=True), (128, 128))
        weighted[at, :] = (gated * out_row).astype(BF16)
        return 0

    w_second(0, 0)
    lax.fori_loop(0, 4, gating, 0)
    sq_all[c] = sq_cols[...].T[0:1, :]
    l_ow.wait()

    gather = ChanSum(s, c, part, ring, fin, comb, across, rs_send, rs_recv)

    def make(turn):
        rows = pl.ds(pl.multiple_of(gather.column(turn) * 256, 256), 256)
        first_piece = gather.column(turn) * 4

        def columns(n, _):
            at = pl.ds(pl.multiple_of(n * 256, 256), 256)
            tile = jnp.dot(weighted[rows, :], ow[:, at], preferred_element_type=F32)
            part[pl.ds(first_piece, 4), :, at] = tile.astype(BF16).reshape(4, 64, 256)
            return 0

        lax.fori_loop(0, 10, columns, 0)

    make(0)
    gather.first(0)
    for i, p in enumerate(peers):
        few = copy_to(sq_all.at[c], sq_all.at[c], sq_send.at[i], sq_recv.at[c], (s, p))
        few.start()
        waits.append(few)
    make(1)
    gather.second(0)
    gather.first(1)
    w_second(1, 0)
    w_ring(xl, 0)
    w_first(1, 1)
    gather.cross()
    gather.second(1)
    for i, p in enumerate(sources):
        copy_to(sq_all.at[p], sq_all.at[p], sq_send.at[0], sq_recv.at[p], (s, p)).wait_recv()
    gather.close()
    own64 = pl.ds(pl.multiple_of(c * 64, 64), 64)
    squares = sq_all[0]
    for i in range(1, 8):
        squares = squares + sq_all[i]
    sq_cols[...] = jnp.broadcast_to(squares, (128, 512)).T
    factor = lax.rsqrt(sq_cols[own64, 0:1] / 5120.0 + EPSILON)

    def gather_sum(n, _):
        at = pl.ds(pl.multiple_of(n * 256, 256), 256)
        mixed[c, :, at] = (hid[c, :, at].astype(F32) + gather.result(at) * factor).astype(BF16)
        return 0

    lax.fori_loop(0, 10, gather_sum, 0)
    xh, yy = c // 4, lax.rem(c, 4)
    y_up, y_down, y_far = lax.rem(yy + 1, 4), lax.rem(yy + 3, 4), lax.rem(yy + 2, 4)
    shared = [0]

    def m_rows(piece, side):
        return mixed.at[piece, pl.ds(side * 32, 32), :]

    def m_to(piece, side, to):
        rows = m_rows(piece, side)
        one = copy_to(rows, rows, ag_send.at[shared[0]], ag_recv.at[piece, side], (s, to))
        shared[0] += 1
        one.start()
        waits.append(one)

    def m_wait(piece, side):
        rows = m_rows(piece, side)
        copy_to(rows, rows, ag_send.at[0], ag_recv.at[piece, side], (s, (1 - xh) * 4 + yy)).wait_recv()

    def m_spread(piece):
        for side in (0, 1):
            m_to(piece, side, xh * 4 + y_up)
            m_to(piece, side, xh * 4 + y_down)

    def m_ring(col):
        for side in (0, 1):
            m_wait(col * 4 + y_down, side)
            m_wait(col * 4 + y_up, side)
            if side == 0:
                m_to(col * 4 + y_down, 0, xh * 4 + y_up)
        m_to(col * 4 + y_up, 1, xh * 4 + y_down)

    def m_end(col):
        for side in (0, 1):
            m_wait(col * 4 + y_far, side)

    for side in (0, 1):
        m_to(c, side, (1 - xh) * 4 + yy)
    m_spread(c)
    for one in gather.sent:
        one.wait_send()
    l_emb = load(9, embedding, part)
    w_ring(1 - xl, 0)
    w_second(0, 1)
    m_ring(xh)
    for side in (0, 1):
        m_wait((1 - xh) * 4 + yy, side)
    m_spread((1 - xh) * 4 + yy)
    l_emb.wait()
    w_far(xl, 0)
    m_end(xh)

    def norm_second(p, _):
        at = pl.ds(pl.multiple_of(p * 64, 64), 64)
        top = mixed[p].astype(F32)
        low = part[p].astype(F32)
        mean = (jnp.sum(top * top, axis=-1, keepdims=True)
                + jnp.sum(low * low, axis=-1, keepdims=True)) / 5120.0
        scale = lax.rsqrt(mean + EPSILON)
        rows_in[at, pl.ds(0, 2560)] = (top * scale * attn_gain[:, pl.ds(0, 2560)]).astype(BF16)
        rows_in[at, pl.ds(2560, 2560)] = (low * scale * attn_gain[:, pl.ds(2560, 2560)]).astype(BF16)
        return 0

    def project_tiles(low, high, half):
        tokens_at = pl.ds(pl.multiple_of(half * 256, 256), 256)

        def project_tile(n, _):
            at = pl.ds(pl.multiple_of(n * 256, 256), 256)
            value = jnp.dot(rows_in[tokens_at, :], w[:, at], preferred_element_type=F32)
            flat_t[at, tokens_at] = value.T.astype(BF16)
            return 0

        lax.fori_loop(low, high, project_tile, 0)
        if high == 7:
            last = pl.ds(1792, 128)
            value = jnp.dot(rows_in[tokens_at, :], w[:, last], preferred_element_type=F32)
            flat_t[last, tokens_at] = value.T.astype(BF16)

    outs, recvs = (k_out, v_out), (k_recv, v_recv)

    def landing(lane, block, half):
        return outs[lane].at[block, :, pl.ds(pl.multiple_of(half * 256, 256), 256)]

    def head_rows(lane, head, half):
        return flat_t.at[pl.ds(pl.multiple_of(lane * 640 + head * 160, 32), 160),
                         pl.ds(pl.multiple_of(half * 256, 256), 256)]

    def first_stage(lane, half, turn):
        mine = pltpu.make_async_copy(head_rows(lane, z, half), landing(lane, s, half), local_sem.at[lane, turn])
        mine.start()
        for d in (2, 1, 3):
            to = lax.rem(z + d, 4)
            one = copy_to(head_rows(lane, to, half), landing(lane, s, half), z_send.at[lane, turn, d - 1],
                          recvs[lane].at[s, half], (seq_at(to, xl, core), c))
            one.start()
            waits.append(one)
        for there, sem in ((seq_at(z, 1 - xl, core), x_send), (sibling, d_send)):
            one = copy_to(head_rows(lane, z, half), landing(lane, s, half), sem.at[lane, turn, 0],
                          recvs[lane].at[s, half], (there, c))
            one.start()
            waits.append(one)
        return mine

    def block_wait(lane, block, half):
        rows = landing(lane, block, half)
        copy_to(rows, rows, z_send.at[0, 0, 0], recvs[lane].at[block, half], (sibling, c)).wait_recv()

    def block_to(lane, block, half, sem, there):
        rows = landing(lane, block, half)
        one = copy_to(rows, rows, sem, recvs[lane].at[block, half], (there, c))
        one.start()
        waits.append(one)

    def pass_on(lane, half, turn, d):
        block = seq_at(lax.rem(z + 4 - d, 4), xl, core)
        block_wait(lane, block, half)
        block_to(lane, block, half, x_send.at[lane, turn, d], seq_at(z, 1 - xl, core))
        block_to(lane, block, half, d_send.at[lane, turn, d], sibling)

    def relay(lane, half, turn, d):
        block = seq_at(lax.rem(z + 4 - d, 4), 1 - xl, core)
        block_wait(lane, block, half)
        block_to(lane, block, half, f_send.at[lane, turn, d], sibling)

    def send_queries(half, turn):
        for d in range(4):
            for j in range(2):
                to_z = lax.rem(z + d, 4)
                to = seq_at(to_z, half, j)
                piece = flat_t.at[pl.ds(pl.multiple_of(1280 + to_z * 160, 32), 160),
                                  pl.ds(pl.multiple_of(half * 256 + j * 128, 128), 128)]
                send_query(piece, to, d, j, turn, half)

    def send_query(piece, to, d, j, turn, half):
        remote = copy_to(piece, q_out.at[s], q_send.at[turn, d, j], q_recv.at[s], (to, c))
        if d:
            remote.start()
            waits.append(remote)
        else:
            here = pltpu.make_async_copy(piece, q_out.at[s], own_sem.at[2])
            mine = (half == xl) & (j == core)
            near.append((mine, here, remote))

            @pl.when(mine)
            def _():
                here.start()

            @pl.when(jnp.logical_not(mine))
            def _():
                remote.start()

    near = []
    early, late = xh, 1 - xh
    lax.fori_loop(early * 4, early * 4 + 4, norm_second, 0)
    w_far(1 - xl, 0)
    w_last(0)
    project_tiles(0, 3, early)
    own = [first_stage(0, early, 0)]
    project_tiles(3, 5, early)
    own.append(first_stage(1, early, 0))
    w_second(1, 1)
    p_first()
    m_ring(1 - xh)
    for d in (1, 3):
        pass_on(0, early, 0, d)
    m_end(1 - xh)
    kept = pltpu.make_async_copy(mixed, mixed_out, own_sem.at[1])
    kept.start()
    lax.fori_loop(late * 4, late * 4 + 4, norm_second, 0)
    project_tiles(0, 3, late)
    own.append(first_stage(0, late, 1))
    pass_on(0, early, 0, 2)
    for d in (1, 3):
        pass_on(1, early, 0, d)
    project_tiles(3, 5, late)
    own.append(first_stage(1, late, 1))
    w_ring(xl, 1)
    pass_on(1, early, 0, 2)
    relay(0, early, 0, 0)
    w_ring(1 - xl, 1)
    for lane in (0, 1):
        for d in (1, 3):
            pass_on(lane, late, 1, d)
    for d in (1, 3):
        relay(0, early, 0, d)
    for lane in (0, 1):
        pass_on(lane, late, 1, 2)
    p_second()
    w_far(xl, 1)
    w_far(1 - xl, 1)
    w_last(1)
    project_tiles(5, 7, early)
    send_queries(early, 0)
    project_tiles(5, 7, late)
    send_queries(late, 1)
    relay(0, early, 0, 2)
    for d in (0, 1, 3, 2):
        relay(1, early, 0, d)
    for lane in (0, 1):
        for d in (0, 1, 3, 2):
            relay(lane, late, 1, d)
    p_third()
    for half in (0, 1):
        for zz in range(4):
            for side in (0, 1):
                for lane in (0, 1):
                    block_wait(lane, seq_at(zz, side, 1 - core), half)
    for one in own:
        one.wait()
    for d in range(1, 16):
        block = lax.rem(s + d, 16)
        copy_to(q_out.at[block], q_out.at[block], q_send.at[0, 0, 0], q_recv.at[block], (block, c)).wait_recv()
    own_p.wait()
    kept.wait()
    p_last()
    for mine, here, remote in near:
        @pl.when(mine)
        def _():
            here.wait()

        @pl.when(jnp.logical_not(mine))
        def _():
            remote.wait_send()

    for one in waits:
        one.wait_send()


def front(*operands):
    dma = pltpu.SemaphoreType.DMA
    vm, anyw = pl.BlockSpec(memory_space=VMEM), pl.BlockSpec(memory_space=pl.ANY)
    return pl.pallas_call(
        front_kernel,
        out_shape=(
            jax.ShapeDtypeStruct((8, 64, 2560), BF16),
            jax.ShapeDtypeStruct((16, 160, 512), BF16),
            jax.ShapeDtypeStruct((16, 160, 512), BF16),
            jax.ShapeDtypeStruct((16, 160, 128), BF16),
            jax.ShapeDtypeStruct((2560, 640), BF16),
        ),
        in_specs=[pl.BlockSpec(memory_space=pltpu.SMEM), anyw, vm, anyw, anyw, anyw, anyw, vm, vm, vm, vm,
                  anyw, anyw, vm, anyw, anyw, anyw, anyw],
        out_specs=(anyw, anyw, anyw, anyw, anyw),
        scratch_shapes=[
            VMEM((8, 64, 2560), BF16),
            VMEM((8, 64, 2560), BF16),
            VMEM((2560, 640), BF16),
            VMEM((2560, 640), BF16),
            VMEM((2560, 128), BF16),
            VMEM((10, 2560), BF16),
            VMEM((128, 2560), BF16),
            VMEM((640, 2560), BF16),
            VMEM((8, 128), F32),
            VMEM((5120, 1920), BF16),
            VMEM((512, 5120), BF16),
            VMEM((8, 64, 2560), BF16),
            VMEM((1920, 512), BF16),
            VMEM((512, 640), F32),
            VMEM((512, 640), F32),
            VMEM((512, 640), F32),
            VMEM((4, 64, 640), F32),
            VMEM((2, 64, 640), BF16),
            VMEM((2, 64, 640), BF16),
            VMEM((4, 64, 640), BF16),
            VMEM((2, 8, 640), F32),
            VMEM((2, 8, 640), F32),
            VMEM((4, 8, 640), F32),
            VMEM((512, 128), F32),
            VMEM((128, 512), F32),
            VMEM((512, 640), F32),
            VMEM((512, 128), BF16),
            VMEM((128, 512), BF16),
            VMEM((160, 640), BF16),
            VMEM((8, 1, 512), F32),
            VMEM((512, 128), F32),
            VMEM((512, 640), BF16),
            dma((11,)),
            dma((60,)),
            dma((16, 2, 2)),
            dma((30,)),
            dma((16, 2)),
            dma((10,)),
            dma((12,)),
            dma((7,)),
            dma((8,)),
            *ring_scratch(64, 2560),
            dma((18,)),
            dma((8, 2)),
            dma((2, 2, 3)),
            dma((2, 2, 4)),
            dma((2, 2, 4)),
            dma((2, 2, 4)),
            dma((16, 2)),
            dma((16, 2)),
            dma((2, 4, 2)),
            dma((16,)),
            dma((2, 2)),
            dma((3,)),
        ],
        compiler_params=pltpu.CompilerParams(
            collective_id=0, has_side_effects=True, vmem_limit_bytes=67043328
        ),
        name="front",
    )(*operands)


def boundary(segments, value):
    count = jnp.int32(0)
    for bit in range(12, -1, -1):
        step = 1 << bit
        count = jnp.where(segments[count + step - 1] < value, count + step, count)
    return jnp.where(segments[jnp.minimum(count, 8191)] < value, count + 1, count)


def attend_kernel(segments, q_hbm, k_in, v_in, out, q_in, landed, keys, values, q_sem, k_sem, v_sem):
    quarter = lax.rem(lax.axis_index("seq"), 4)

    def loads(j):
        return [
            pltpu.make_async_copy(src.at[4 * j + side], dst.at[j, :, pl.ds(side * 512, 512)], sem.at[4 * j + side])
            for side in range(4) for src, dst, sem in ((k_in, landed, k_sem), (v_in, values, v_sem))
        ]

    q_load = pltpu.make_async_copy(q_hbm, q_in, q_sem)
    q_load.start()
    for j in range(4):
        for one in loads(j):
            one.start()
    first, second = boundary(segments, 1), boundary(segments, 2)
    scale = (AP ** -0.5) * 1.4426950408889634
    lane = lax.broadcasted_iota(jnp.int32, (1, 512), 1)
    q_load.wait()

    def tile(i, _):
        for n in range(1):
            for one in loads(i * 1 + n):
                one.wait()
            keys[i * 1 + n] = landed[i * 1 + n].astype(F32).T.astype(BF16)
        queries = jnp.concatenate([q_in[4 * i + n] for n in range(4)], axis=1)
        low_place = i * 2048 + quarter * 128
        place = low_place + lane + 384 * (lane // 128)
        begin = start_of(place, first, second)
        lowest = start_of(low_place, first, second) // 2048
        last_begin = start_of(low_place + 1663, first, second)
        plain_from = jnp.minimum((last_begin + 2047) // 2048, i * 1)

        def step(j, carry, causal, reset):
            top, total, acc = carry
            scores = jnp.dot(keys[j], queries, preferred_element_type=F32)
            if causal or reset:
                key = j * 2048 + lax.broadcasted_iota(jnp.int32, (2048, 512), 0)
                visible = key >= begin
                if causal:
                    visible = visible & (key <= place)
                scores = jnp.where(visible, scores, -1e30)
            new_top = jnp.maximum(top, jnp.max(scores, axis=0, keepdims=True))
            weights = jnp.exp2((scores - new_top) * scale)
            keep = jnp.exp2((top - new_top) * scale)
            total = total * keep + jnp.sum(weights, axis=0, keepdims=True)
            acc = acc * keep + jnp.dot(values[j], weights.astype(BF16), preferred_element_type=F32)
            return new_top, total, acc

        carry = (jnp.full((1, 512), -1e29, F32), jnp.zeros((1, 512), F32), jnp.zeros((AP, 512), F32))
        carry = lax.fori_loop(lowest, plain_from, lambda j, t: step(j, t, False, True), carry)
        carry = lax.fori_loop(
            jnp.maximum(lowest, plain_from), i * 1, lambda j, t: step(j, t, False, False), carry)
        top, total, acc = lax.fori_loop(
            jnp.maximum(lowest, i * 1), i * 1 + 1, lambda j, t: step(j, t, True, True), carry)
        context = (acc / total).astype(BF16)
        for n in range(4):
            out[4 * i + n] = context[:, n * 128:n * 128 + 128]
        return 0

    lax.fori_loop(0, 4, tile, 0)


def attend(segments, q_in, k_in, v_in):
    vm, anyw = pl.BlockSpec(memory_space=VMEM), pl.BlockSpec(memory_space=pl.ANY)
    return pl.pallas_call(
        attend_kernel,
        out_shape=jax.ShapeDtypeStruct((16, 160, 128), BF16),
        in_specs=[pl.BlockSpec(memory_space=pltpu.SMEM), anyw, anyw, anyw],
        out_specs=vm,
        scratch_shapes=[
            VMEM((16, 160, 128), BF16),
            VMEM((4, 160, 2048), BF16),
            VMEM((4, 2048, 160), BF16),
            VMEM((4, 160, 2048), BF16),
            pltpu.SemaphoreType.DMA,
            pltpu.SemaphoreType.DMA((16,)),
            pltpu.SemaphoreType.DMA((16,)),
        ],
        compiler_params=pltpu.CompilerParams(vmem_limit_bytes=67043328),
        name="attend",
    )(segments, q_in, k_in, v_in)


def finish_kernel(ctx, proj_in, mixed, out, proj_t, own_in, gathered, part, in_send, in_recv, ring, fin, comb, across, rs_send, rs_recv, local_sem):
    s, c = lax.axis_index("seq"), lax.axis_index("chan")
    peers = chan_peers(s, c)
    proj_load = pltpu.make_async_copy(proj_in, proj_t, local_sem.at[1])
    proj_load.start()
    window = pl.ds(pl.multiple_of(c * 5 // 2 * 128, 128), 384)
    own_load = pltpu.make_async_copy(mixed.at[:, window], own_in, local_sem.at[2])
    own_load.start()
    greet([(s, p) for p in peers] + [(lax.rem(s + d, 16), c) for d in range(1, 16)])
    z = s // 4
    lanes = pl.ds(pl.multiple_of(lax.rem(s, 4) * 128, 128), 128)
    waits = []
    for d in range(16):
        to = lax.rem(s + d, 16)
        where = gathered.at[pl.ds(pl.multiple_of(z * 160, 32), 160), lanes]
        if d == 0:
            own = pltpu.make_async_copy(ctx.at[s], where, local_sem.at[0])
            own.start()
        else:
            one = copy_to(ctx.at[to], where, in_send.at[d - 1], in_recv.at[s], (to, c))
            one.start()
            waits.append(one)
    own.wait()
    for d in range(1, 16):
        block = lax.rem(s + d, 16)
        where = gathered.at[pl.ds(pl.multiple_of((block // 4) * 160, 32), 160),
                            pl.ds(pl.multiple_of(lax.rem(block, 4) * 128, 128), 128)]
        copy_to(ctx.at[0], where, in_send.at[0], in_recv.at[block], (block, c)).wait_recv()
    gather = ChanSum(s, c, part, ring, fin, comb, across, rs_send, rs_recv)

    def make(turn):
        def rows_of(n, _):
            p = gather.column(turn) * 4 + n
            at = pl.ds(pl.multiple_of(p * 320, 32), 320)
            part[p] = jnp.dot(proj_t[at, :], gathered[...], preferred_element_type=F32).astype(BF16)
            return 0

        lax.fori_loop(0, 4, rows_of, 0)

    proj_load.wait()
    make(0)
    gather.first(0)
    make(1)
    gather.second(0)
    gather.first(1)
    gather.cross()
    gather.second(1)
    own_load.wait()
    own_t_all = [own_in[n * 256:(n + 1) * 256, :].astype(F32).T for n in range(2)]
    gather.close()
    odd = lax.rem(c, 2) == 1
    for n in range(2):
        at = pl.ds(n * 256, 256)
        own_t = own_t_all[n]
        out[:, at] = (gather.result(at) + jnp.where(odd, own_t[64:, :], own_t[:320, :])).astype(BF16)
    for one in waits + gather.sent:
        one.wait_send()


def finish(ctx, proj_t, mixed):
    dma = pltpu.SemaphoreType.DMA
    vm, anyw = pl.BlockSpec(memory_space=VMEM), pl.BlockSpec(memory_space=pl.ANY)
    return pl.pallas_call(
        finish_kernel,
        out_shape=jax.ShapeDtypeStruct((320, 512), BF16),
        in_specs=[anyw, anyw, anyw],
        out_specs=vm,
        scratch_shapes=[
            VMEM((2560, 640), BF16),
            VMEM((512, 384), BF16),
            VMEM((640, 512), BF16),
            VMEM((8, 320, 512), BF16),
            dma((15,)),
            dma((16,)),
            *ring_scratch(320, 512),
            dma((3,)),
        ],
        compiler_params=pltpu.CompilerParams(
            collective_id=2, has_side_effects=True, vmem_limit_bytes=67043328
        ),
        cost_estimate=pl.CostEstimate(flops=50_000_000_000, bytes_accessed=6_000_000, transcendentals=0),
        name="finish",
    )(ctx, proj_t, mixed)


def local(
    hidden,
    embedding,
    segments,
    input_norm_gain,
    gate_proj,
    input_proj,
    state_proj,
    step_proj,
    step_bias,
    decay_log,
    skip_gain,
    out_gain,
    out_proj,
    attn_gain,
    query_proj,
    key_proj,
    value_proj,
    attn_out,
):
    mixed, k_all, v_all, q_all, proj_t = front(
        segments, hidden.reshape(8, 64, 2560), input_norm_gain, input_proj, gate_proj, state_proj,
        step_proj.T, step_bias[None, :], decay_log[None, :], skip_gain[None, :], out_gain,
        out_proj, embedding.reshape(8, 64, 2560), attn_gain[None, :], key_proj, value_proj, query_proj,
        attn_out.T,
    )
    ctx = attend(segments, q_all, k_all, v_all)
    return finish(ctx, proj_t, mixed.reshape(512, 2560)).T


def solution(mesh):
    in_specs = (
        P("seq", None),
        P("seq", None),
        P(),
        P(),
        P(None, "chan"),
        P(None, "chan"),
        P(),
        P(None, "chan"),
        P("chan"),
        P("chan"),
        P("chan"),
        P("chan"),
        P("chan", None),
        P(),
        P("seq", "chan"),
        P("seq", "chan"),
        P("seq", "chan"),
        P("chan", "seq"),
    )
    out_specs = P("seq", "chan")
    return jax.shard_map(local, mesh=mesh, in_specs=in_specs, out_specs=out_specs, check_vma=False)
```

```python
import jax
import jax.numpy as jnp
from jax import lax
from jax.experimental import pallas as pl
from jax.experimental.pallas import tpu as pltpu
from jax.sharding import PartitionSpec as P

N = 64
HEAD_CHANNELS = 64
AP = 160
EPSILON = 1e-05
MESH = pl.DeviceIdType.MESH
VMEM = pltpu.VMEM
F32 = jnp.float32
BF16 = jnp.bfloat16


def greet(peers):
    barrier = pltpu.get_barrier_semaphore()
    for peer in peers:
        pl.semaphore_signal(barrier, inc=1, device_id=peer, device_id_type=MESH)
    pl.semaphore_wait(barrier, len(peers))


def copy_to(src, dst, send, recv, where):
    return pltpu.make_async_remote_copy(
        src_ref=src, dst_ref=dst, send_sem=send, recv_sem=recv,
        device_id=where, device_id_type=MESH,
    )


OFFSETS = ((1, 2), (1, 1), (1, 3), (0, 2), (1, 0), (0, 1), (0, 3))


def chan_peers(s, c):
    half, place = c // 4, lax.rem(c, 4)
    return [lax.rem(half + a, 2) * 4 + lax.rem(place + b, 4) for a, b in OFFSETS]


def chan_sources(s, c):
    half, place = c // 4, lax.rem(c, 4)
    return [lax.rem(half + a, 2) * 4 + lax.rem(place + 4 - b, 4) for a, b in OFFSETS]


def seq_parts(s):
    return s // 4, lax.rem(s // 2, 2), lax.rem(s, 2)


def seq_at(z, xl, core):
    return z * 4 + xl * 2 + core


class ChanSum:
    def __init__(self, s, c, part, ring, fin, comb, across, send_sem, recv_sem):
        self.s, self.part, self.ring, self.fin = s, part, ring, fin
        self.comb, self.across, self.send_sem, self.recv_sem = comb, across, send_sem, recv_sem
        self.rows, self.width = part.shape[1] // 2, part.shape[2]
        self.xh, self.yy = c // 4, lax.rem(c, 4)
        self.up = lax.rem(self.yy + 1, 4)
        self.down = lax.rem(self.yy + 3, 4)
        self.far = lax.rem(self.yy + 2, 4)
        self.sent = []

    def column(self, turn):
        return 1 - self.xh if turn == 0 else self.xh

    def side(self, ref, half):
        return ref.at[pl.ds(half * self.rows, self.rows), :]

    def piece(self, turn, y, half):
        return self.side(self.part.at[self.column(turn) * 4 + y], half)

    def copy(self, i, src, dst, y, turn=1):
        to = self.column(turn) * 4 + y
        return copy_to(src, dst, self.send_sem.at[i], self.recv_sem.at[i], (self.s, to))

    def send(self, i, src, dst, y, turn=1):
        one = self.copy(i, src, dst, y, turn)
        one.start()
        self.sent.append(one)

    def wait(self, i, dst):
        self.copy(i, dst, dst, self.up).wait_recv()

    def first(self, turn):
        i = 6 * turn
        self.send(i, self.piece(turn, self.far, 0), self.ring.at[turn, 0], self.up)
        self.send(i + 2, self.piece(turn, self.far, 1), self.ring.at[turn, 1], self.down)
        self.send(i + 1, self.piece(turn, self.up, 1), self.side(self.fin.at[turn, 0], 1), self.up)
        self.send(i + 3, self.piece(turn, self.down, 0), self.side(self.fin.at[turn, 1], 0), self.down)

    def second(self, turn):
        for way, y in ((0, self.up), (1, self.down)):
            self.wait(6 * turn + 2 * way, self.ring.at[turn, way])
            mine, its, both = self.piece(turn, y, way), self.ring.at[turn, way], self.comb.at[turn, way]

            def add(n, _):
                at = pl.ds(pl.multiple_of(n * 256, 256), 256)
                both[:, at] = (mine[:, at].astype(F32) + its[:, at].astype(F32)).astype(BF16)
                return 0

            lax.fori_loop(0, self.width // 256, add, 0)
            self.send(6 * turn + 4 + way, both, self.side(self.fin.at[turn, way], way), y)

    def arrived(self, turn):
        i = 6 * turn
        for way in (0, 1):
            self.wait(i + 1 + 2 * way, self.side(self.fin.at[turn, way], 1 - way))
            self.wait(i + 4 + way, self.side(self.fin.at[turn, way], way))

    def total(self, turn, at):
        value = self.part[self.column(turn) * 4 + self.yy, :, at].astype(F32)
        return value + self.fin[turn, 0, :, at].astype(F32) + self.fin[turn, 1, :, at].astype(F32)

    def cross(self):
        self.arrived(0)
        own = self.column(0) * 4 + self.yy

        def add(n, _):
            at = pl.ds(pl.multiple_of(n * 256, 256), 256)
            self.part[own, :, at] = self.total(0, at).astype(BF16)
            return 0

        lax.fori_loop(0, self.width // 256, add, 0)
        self.send(12, self.part.at[own], self.across, self.yy, 0)

    def close(self):
        self.arrived(1)
        self.wait(12, self.across)

    def result(self, at):
        return self.total(1, at) + self.across[:, at].astype(F32)


def ring_scratch(rows, width):
    return [
        VMEM((2, 2, rows // 2, width), BF16),
        VMEM((2, 2, rows, width), BF16),
        VMEM((2, 2, rows // 2, width), BF16),
        VMEM((rows, width), BF16),
        pltpu.SemaphoreType.DMA((13,)),
        pltpu.SemaphoreType.DMA((13,)),
    ]


def start_of(place, first, second):
    return jnp.where(place >= second, second, jnp.where(place >= first, first, 0))


def three_parts(value):
    high = value.astype(BF16)
    rest = value - high.astype(F32)
    middle = rest.astype(BF16)
    low = (rest - middle.astype(F32)).astype(BF16)
    return jnp.concatenate([high, middle, low], axis=1)


def silu(v):
    return v / (1.0 + jnp.exp(-v))


def front_kernel(segments, hidden, norm_gain, input_w, gate_w, state_w, step_w, bias, decay, skip, out_gain,
                 out_w, embedding, attn_gain, wk, wv, wq, p_in,
                 mixed_out, k_out, v_out, q_out, p_out,
                 mixed, hid, iw, gw, sw, dw, dwt, ow, vec, w, rows_in, part, flat_t, run_e, xs, ys, states, tx, rx, planes, tx_t, rx_t, planes_t,
                 run_rows, run_cols, step_e, bc_rows, bc_cols, pb, sq_all, sq_cols, weighted,
                 load_sem, w_send, w_recv, p_send, p_recv, st_send, st_recv,
                 sq_send, sq_recv, ring, fin, comb, across, rs_send, rs_recv, ag_send, ag_recv,
                 z_send, x_send, d_send, f_send, k_recv, v_recv, q_send, q_recv, local_sem, own_sem):
    s, c = lax.axis_index("seq"), lax.axis_index("chan")
    z, xl, core = seq_parts(s)
    peers, sources = chan_peers(s, c), chan_sources(s, c)
    up, down, far = lax.rem(z + 1, 4), lax.rem(z + 3, 4), lax.rem(z + 2, 4)
    waits = []

    def load(i, src, dst):
        one = pltpu.make_async_copy(src, dst, load_sem.at[i])
        one.start()
        return one

    own_rows = pl.ds(pl.multiple_of(s * 320, 64), 320)
    w_loads = [load(i, src, w.at[own_rows, pl.ds(i * 640, 640)]) for i, src in enumerate((wk, wv, wq))]
    l_hid = load(3, hidden, hid)
    l_sw = load(4, state_w, sw)
    l_dw = load(10, step_w, dw)
    l_iw = load(5, input_w, iw)
    l_pb = load(6, p_in, pb)
    l_gw = load(7, gate_w, gw)
    l_ow = load(8, out_w, ow)
    greet([(s, p) for p in peers] + [(lax.rem(s + d, 16), c) for d in range(1, 16)])

    used = [0, 0]
    sibling = seq_at(z, xl, 1 - core)

    def w_rows(block, half, group):
        rows = pl.ds(pl.multiple_of(block * 320 + half * 160, 32), 160)
        return w.at[rows, pl.ds(1280 * group, 1280 - 640 * group)]

    def w_to(block, half, group, to):
        rows = w_rows(block, half, group)
        one = copy_to(rows, rows, w_send.at[used[0]], w_recv.at[block, half, group], (to, c))
        used[0] += 1
        one.start()
        waits.append(one)

    def w_wait(block, half, group):
        rows = w_rows(block, half, group)
        copy_to(rows, rows, w_send.at[0], w_recv.at[block, half, group], (sibling, c)).wait_recv()

    def p_rows(block, half):
        return p_out.at[pl.ds(pl.multiple_of(block * 160 + half * 80, 16), 80), :]

    def p_to(block, half, to, src=None):
        rows = p_rows(block, half)
        one = copy_to(rows if src is None else src, rows, p_send.at[used[1]], p_recv.at[block, half], (to, c))
        used[1] += 1
        one.start()
        waits.append(one)

    def p_wait(block, half):
        rows = p_rows(block, half)
        copy_to(rows, rows, p_send.at[0], p_recv.at[block, half], (sibling, c)).wait_recv()

    def w_across(half, group):
        w_to(s, half, group, seq_at(z, 1 - xl, core))

    def w_first(half, group):
        w_to(s, half, group, seq_at(up, xl, core))
        w_to(s, half, group, seq_at(down, xl, core))
        w_to(s, half, group, sibling)

    def w_second(half, group):
        block = seq_at(z, 1 - xl, core)
        w_wait(block, half, group)
        w_to(block, half, group, seq_at(up, xl, core))
        w_to(block, half, group, seq_at(down, xl, core))
        w_to(block, half, group, sibling)

    def w_ring(side, group):
        for half in (0, 1):
            w_wait(seq_at(down, side, core), half, group)
            w_wait(seq_at(up, side, core), half, group)
            if half == 0:
                w_to(seq_at(down, side, core), 0, group, seq_at(up, xl, core))
        w_to(seq_at(up, side, core), 1, group, seq_at(down, xl, core))
        for half in (0, 1):
            w_to(seq_at(down, side, core), half, group, sibling)
            w_to(seq_at(up, side, core), half, group, sibling)

    def w_far(side, group):
        for half in (0, 1):
            w_wait(seq_at(far, side, core), half, group)
            w_to(seq_at(far, side, core), half, group, sibling)

    def w_last(group):
        for zz in range(4):
            for xx in range(2):
                for half in (0, 1):
                    w_wait(seq_at(zz, xx, 1 - core), half, group)

    def p_cross():
        for half in (0, 1):
            p_to(s, half, seq_at(z, 1 - xl, core), pb.at[pl.ds(half * 80, 80), :])

    def p_first():
        block = seq_at(z, 1 - xl, core)
        for half in (0, 1):
            for to in (seq_at(up, xl, core), seq_at(down, xl, core), sibling):
                p_to(s, half, to, pb.at[pl.ds(half * 80, 80), :])
        for half in (0, 1):
            p_wait(block, half)
            for to in (seq_at(up, xl, core), seq_at(down, xl, core), sibling):
                p_to(block, half, to)

    def p_second():
        p_ring(xl)

    def p_ring(side):
        for half in (0, 1):
            p_wait(seq_at(down, side, core), half)
            p_wait(seq_at(up, side, core), half)
        p_to(seq_at(down, side, core), 0, seq_at(up, xl, core))
        p_to(seq_at(up, side, core), 1, seq_at(down, xl, core))
        for half in (0, 1):
            p_to(seq_at(down, side, core), half, sibling)
            p_to(seq_at(up, side, core), half, sibling)

    def p_last():
        for half in (0, 1):
            for block in (seq_at(down, 1 - xl, core), seq_at(up, 1 - xl, core), seq_at(far, xl, core)):
                p_wait(block, half)
            for block in (sibling, seq_at(z, 1 - xl, 1 - core), seq_at(up, xl, 1 - core), seq_at(down, xl, 1 - core)):
                p_wait(block, half)

    for one in w_loads:
        one.wait()
    w_first(0, 0)
    w_first(0, 1)

    first, second = boundary(segments, 1), boundary(segments, 2)
    base = s * 512
    l_hid.wait()
    norm_row = norm_gain[...].reshape(1, 2560)
    out_row = out_gain[...].reshape(1, 640)

    def norm_first(p, _):
        at = pl.ds(pl.multiple_of(p * 64, 64), 64)
        value = hid[p].astype(F32)
        factor = lax.rsqrt(jnp.sum(value * value, axis=-1, keepdims=True) / 2560.0 + EPSILON)
        rows_in[at, pl.ds(0, 2560)] = (value * factor * norm_row).astype(BF16)
        return 0

    lax.fori_loop(0, 8, norm_first, 0)
    tokens = rows_in.at[:, pl.ds(0, 2560)]
    vec[...] = jnp.zeros((8, 128), F32)
    dwt[...] = jnp.zeros((128, 2560), BF16)
    vec[0:1, 0:10] = bias[...]
    vec[1:2, 0:10] = decay[...]
    vec[2:3, 0:10] = skip[...]
    l_sw.wait()
    l_dw.wait()
    dwt[0:10, :] = dw[...]
    bc = silu(jnp.dot(tokens[...], sw[...], preferred_element_type=F32))
    bc_rows[...] = bc.astype(BF16)
    bc_cols[...] = bc.T.astype(BF16)
    logits = lax.dot_general(tokens[...], dwt[...], (((1,), (1,)), ((), ())), preferred_element_type=F32) + vec[0:1, :]
    steps = jnp.maximum(logits, 0.0) + jnp.log1p(jnp.exp(-jnp.abs(logits)))
    rate = -jnp.exp(vec[1:2, :])
    lower = (lax.broadcasted_iota(jnp.int32, (512, 512), 0)
             >= lax.broadcasted_iota(jnp.int32, (512, 512), 1)).astype(F32).astype(BF16)
    sums = jnp.dot(lower, three_parts(steps * rate), preferred_element_type=F32)
    running = sums[:, :128] + sums[:, 128:256] + sums[:, 256:]
    spread = (lax.broadcasted_iota(jnp.int32, (384, 640), 1) // 64
              == lax.rem(lax.broadcasted_iota(jnp.int32, (384, 640), 0), 128)).astype(F32).astype(BF16)
    run_rows[...] = running
    run_cols[...] = running.T
    run_e[...] = jnp.dot(three_parts(running), spread, preferred_element_type=F32)
    step_e[...] = jnp.dot(three_parts(steps), spread, preferred_element_type=F32)
    skip_e = jnp.dot(three_parts(vec[...]), spread, preferred_element_type=F32)[2:3, :]
    l_iw.wait()

    def input_tile(n, width):
        at = pl.ds(n, width)
        xs[:, at] = silu(jnp.dot(tokens[...], iw[:, at], preferred_element_type=F32))
        step_e[:, at] = xs[:, at] * step_e[:, at]

    input_tile(0, 256)
    input_tile(256, 256)
    input_tile(512, 128)

    states[0] = jnp.zeros((64, 640), F32)
    total = None
    for k in range(4):
        rows = slice(k * 128, k * 128 + 128)
        end = run_e[k * 128 + 127:k * 128 + 128, :]
        begin_end = start_of(base + k * 128 + 127, first, second)
        place = base + k * 128 + lax.broadcasted_iota(jnp.int32, (128, 1), 0)
        keep = jnp.where(place >= begin_end, jnp.exp(end - run_e[rows, :]), 0.0)
        own = jnp.dot(bc_cols[:64, rows], (step_e[rows, :] * keep).astype(BF16), preferred_element_type=F32)
        gap = end if k == 0 else end - run_e[k * 128 - 1:k * 128, :]
        through = jnp.where(base + k * 128 - 1 >= begin_end, jnp.exp(gap), 0.0)
        if k == 0:
            total = through
            states[1] = own
        else:
            total = total * through
            if k < 3:
                states[k + 1] = through * states[k] + own
            else:
                tx[0] = (through * states[k] + own).astype(BF16)
    tx_t[0] = jnp.broadcast_to(total, (8, 640))

    def state_to(i, to):
        pair = [
            copy_to(tx_t.at[i], rx_t.at[i], st_send.at[2 * i], st_recv.at[2 * i], (to, c)),
            copy_to(tx.at[i], rx.at[i], st_send.at[2 * i + 1], st_recv.at[2 * i + 1], (to, c)),
        ]
        for one in pair:
            one.start()
            waits.append(one)
        return pair

    def joined(i, low):
        mine_s, mine_t = tx[i].astype(F32), tx_t[i, 0:1, :]
        its_s, its_t = rx[i].astype(F32), rx_t[i, 0:1, :]
        first_s, first_t = jnp.where(low, mine_s, its_s), jnp.where(low, mine_t, its_t)
        last_s, last_t = jnp.where(low, its_s, mine_s), jnp.where(low, its_t, mine_t)
        return (last_t * first_s + last_s).astype(BF16), jnp.broadcast_to(first_t * last_t, (8, 640))

    for one in state_to(0, sibling):
        one.wait_recv()
    tx[1], tx_t[1] = joined(0, core == 0)
    pair = state_to(1, seq_at(z, 1 - xl, core))
    for group in (0, 1):
        w_across(0, group)
        w_across(1, group)

    def chunk(k, _):
        at = pl.ds(pl.multiple_of(k * 128, 128), 128)
        place = base + k * 128 + lax.broadcasted_iota(jnp.int32, (128, 1), 0)
        key = base + k * 128 + lax.broadcasted_iota(jnp.int32, (1, 128), 1)
        begin = start_of(place, first, second)
        allowed = (key >= begin) & (key <= place)
        cross = jnp.dot(bc_rows[at, 64:128], bc_cols[0:64, at], preferred_element_type=F32)
        cross = jnp.where(allowed, cross, 0.0)
        lane = lax.broadcasted_iota(jnp.int32, (128, 128), 1)
        for pair in range(5):
            lanes = pl.ds(pair * 128, 128)
            scaled = step_e[at, lanes].astype(BF16)
            halves = []
            for h in (2 * pair, 2 * pair + 1):
                gap = run_rows[at, h:h + 1] - run_cols[h:h + 1, at]
                decay = jnp.exp(jnp.where(allowed, gap, -1e30))
                halves.append(jnp.dot((decay * cross).astype(BF16), scaled, preferred_element_type=F32))
            ys[at, lanes] = jnp.where(lane < 64, halves[0], halves[1])
        return 0

    lax.fori_loop(0, 2, chunk, 0)
    for one in pair:
        one.wait_recv()
    planes[z], planes_t[z] = joined(1, xl == 0)
    for d in (2, 1, 3):
        to = (seq_at(lax.rem(z + d, 4), xl, core), c)
        for one in (
            copy_to(planes_t.at[z], planes_t.at[z], st_send.at[2 + 2 * d], st_recv.at[4 + 2 * z], to),
            copy_to(planes.at[z], planes.at[z], st_send.at[3 + 2 * d], st_recv.at[5 + 2 * z], to),
        ):
            one.start()
            waits.append(one)
    w_first(1, 0)
    l_pb.wait()
    own_p = pltpu.make_async_copy(
        pb, p_out.at[pl.ds(pl.multiple_of(s * 160, 32), 160), :], own_sem.at[0])
    own_p.start()
    lax.fori_loop(2, 4, chunk, 0)

    for k in range(1, 4):
        rows = slice(k * 128, k * 128 + 128)
        place = base + k * 128 + lax.broadcasted_iota(jnp.int32, (128, 1), 0)
        begin = start_of(place, first, second)
        enter = jnp.where(base + k * 128 - 1 >= begin,
                          jnp.exp(run_e[rows, :] - run_e[k * 128 - 1:k * 128, :]), 0.0)
        ys[rows, :] += enter * jnp.dot(bc_rows[rows, 64:128], states[k].astype(BF16), preferred_element_type=F32)

    l_gw.wait()
    for n, width in ((0, 256), (256, 256), (512, 128)):
        at = pl.ds(n, width)
        step_e[:, at] = silu(jnp.dot(tokens[...], gw[:, at], preferred_element_type=F32))

    enter_s = jnp.zeros((64, 640), F32)
    for d in (1, 2, 3):
        zz = lax.rem(z + d, 4)
        of = (seq_at(zz, xl, core), c)
        copy_to(planes_t.at[zz], planes_t.at[zz], st_send.at[0], st_recv.at[4 + 2 * zz], of).wait_recv()
        copy_to(planes.at[zz], planes.at[zz], st_send.at[0], st_recv.at[5 + 2 * zz], of).wait_recv()
    for zz in range(3):
        enter_s = jnp.where(zz < z, planes_t[zz, 0:1, :] * enter_s + planes[zz].astype(F32), enter_s)
    for i, low in ((1, xl == 0), (0, core == 0)):
        first_s = jnp.where(low, tx[i].astype(F32), rx[i].astype(F32))
        first_t = jnp.where(low, tx_t[i, 0:1, :], rx_t[i, 0:1, :])
        enter_s = jnp.where(low, enter_s, first_t * enter_s + first_s)
    states[0] = enter_s

    def gating(k, _):
        at = pl.ds(pl.multiple_of(k * 128, 128), 128)
        place = base + k * 128 + lax.broadcasted_iota(jnp.int32, (128, 1), 0)
        begin = start_of(place, first, second)
        enter = jnp.where(base - 1 >= begin, jnp.exp(run_e[at, :]), 0.0)
        y = ys[at, :] + enter * jnp.dot(bc_rows[at, 64:128], states[0].astype(BF16), preferred_element_type=F32)
        y = y + xs[at, :] * skip_e
        gated = y * step_e[at, :]
        sq_cols[at, :] = jnp.broadcast_to(jnp.sum(gated * gated, axis=-1, keepdims=True), (128, 128))
        weighted[at, :] = (gated * out_row).astype(BF16)
        return 0

    w_second(0, 0)
    lax.fori_loop(0, 4, gating, 0)
    sq_all[c] = sq_cols[...].T[0:1, :]
    l_ow.wait()

    gather = ChanSum(s, c, part, ring, fin, comb, across, rs_send, rs_recv)

    def make(turn):
        rows = pl.ds(pl.multiple_of(gather.column(turn) * 256, 256), 256)
        first_piece = gather.column(turn) * 4

        def columns(n, _):
            at = pl.ds(pl.multiple_of(n * 256, 256), 256)
            tile = jnp.dot(weighted[rows, :], ow[:, at], preferred_element_type=F32)
            part[pl.ds(first_piece, 4), :, at] = tile.astype(BF16).reshape(4, 64, 256)
            return 0

        lax.fori_loop(0, 10, columns, 0)

    make(0)
    gather.first(0)
    for i, p in enumerate(peers):
        few = copy_to(sq_all.at[c], sq_all.at[c], sq_send.at[i], sq_recv.at[c], (s, p))
        few.start()
        waits.append(few)
    make(1)
    gather.second(0)
    gather.first(1)
    w_second(1, 0)
    w_ring(xl, 0)
    w_first(1, 1)
    gather.cross()
    gather.second(1)
    for i, p in enumerate(sources):
        copy_to(sq_all.at[p], sq_all.at[p], sq_send.at[0], sq_recv.at[p], (s, p)).wait_recv()
    gather.close()
    own64 = pl.ds(pl.multiple_of(c * 64, 64), 64)
    squares = sq_all[0]
    for i in range(1, 8):
        squares = squares + sq_all[i]
    sq_cols[...] = jnp.broadcast_to(squares, (128, 512)).T
    factor = lax.rsqrt(sq_cols[own64, 0:1] / 5120.0 + EPSILON)

    def gather_sum(n, _):
        at = pl.ds(pl.multiple_of(n * 256, 256), 256)
        mixed[c, :, at] = (hid[c, :, at].astype(F32) + gather.result(at) * factor).astype(BF16)
        return 0

    lax.fori_loop(0, 10, gather_sum, 0)
    xh, yy = c // 4, lax.rem(c, 4)
    y_up, y_down, y_far = lax.rem(yy + 1, 4), lax.rem(yy + 3, 4), lax.rem(yy + 2, 4)
    shared = [0]

    def m_rows(piece, side):
        return mixed.at[piece, pl.ds(side * 32, 32), :]

    def m_to(piece, side, to):
        rows = m_rows(piece, side)
        one = copy_to(rows, rows, ag_send.at[shared[0]], ag_recv.at[piece, side], (s, to))
        shared[0] += 1
        one.start()
        waits.append(one)

    def m_wait(piece, side):
        rows = m_rows(piece, side)
        copy_to(rows, rows, ag_send.at[0], ag_recv.at[piece, side], (s, (1 - xh) * 4 + yy)).wait_recv()

    def m_spread(piece):
        for side in (0, 1):
            m_to(piece, side, xh * 4 + y_up)
            m_to(piece, side, xh * 4 + y_down)

    def m_ring(col):
        for side in (0, 1):
            m_wait(col * 4 + y_down, side)
            m_wait(col * 4 + y_up, side)
            if side == 0:
                m_to(col * 4 + y_down, 0, xh * 4 + y_up)
        m_to(col * 4 + y_up, 1, xh * 4 + y_down)

    def m_end(col):
        for side in (0, 1):
            m_wait(col * 4 + y_far, side)

    for side in (0, 1):
        m_to(c, side, (1 - xh) * 4 + yy)
    m_spread(c)
    for one in gather.sent:
        one.wait_send()
    l_emb = load(9, embedding, part)
    w_ring(1 - xl, 0)
    p_cross()
    w_second(0, 1)
    m_ring(xh)
    for side in (0, 1):
        m_wait((1 - xh) * 4 + yy, side)
    m_spread((1 - xh) * 4 + yy)
    l_emb.wait()
    w_far(xl, 0)
    m_end(xh)

    def norm_second(p, _):
        at = pl.ds(pl.multiple_of(p * 64, 64), 64)
        top = mixed[p].astype(F32)
        low = part[p].astype(F32)
        mean = (jnp.sum(top * top, axis=-1, keepdims=True)
                + jnp.sum(low * low, axis=-1, keepdims=True)) / 5120.0
        scale = lax.rsqrt(mean + EPSILON)
        rows_in[at, pl.ds(0, 2560)] = (top * scale * attn_gain[:, pl.ds(0, 2560)]).astype(BF16)
        rows_in[at, pl.ds(2560, 2560)] = (low * scale * attn_gain[:, pl.ds(2560, 2560)]).astype(BF16)
        return 0

    def project_tiles(low, high, half):
        tokens_at = pl.ds(pl.multiple_of(half * 256, 256), 256)

        def project_tile(n, _):
            at = pl.ds(pl.multiple_of(n * 256, 256), 256)
            value = jnp.dot(rows_in[tokens_at, :], w[:, at], preferred_element_type=F32)
            flat_t[at, tokens_at] = value.T.astype(BF16)
            return 0

        lax.fori_loop(low, high, project_tile, 0)
        if high == 7:
            last = pl.ds(1792, 128)
            value = jnp.dot(rows_in[tokens_at, :], w[:, last], preferred_element_type=F32)
            flat_t[last, tokens_at] = value.T.astype(BF16)

    outs, recvs = (k_out, v_out), (k_recv, v_recv)

    def landing(lane, block, half):
        return outs[lane].at[block, :, pl.ds(pl.multiple_of(half * 256, 256), 256)]

    def head_rows(lane, head, half):
        return flat_t.at[pl.ds(pl.multiple_of(lane * 640 + head * 160, 32), 160),
                         pl.ds(pl.multiple_of(half * 256, 256), 256)]

    def first_stage(lane, half, turn):
        mine = pltpu.make_async_copy(head_rows(lane, z, half), landing(lane, s, half), local_sem.at[lane, turn])
        mine.start()
        for d in (2, 1, 3):
            to = lax.rem(z + d, 4)
            one = copy_to(head_rows(lane, to, half), landing(lane, s, half), z_send.at[lane, turn, d - 1],
                          recvs[lane].at[s, half], (seq_at(to, xl, core), c))
            one.start()
            waits.append(one)
        for there, sem in ((seq_at(z, 1 - xl, core), x_send), (sibling, d_send)):
            one = copy_to(head_rows(lane, z, half), landing(lane, s, half), sem.at[lane, turn, 0],
                          recvs[lane].at[s, half], (there, c))
            one.start()
            waits.append(one)
        return mine

    def block_wait(lane, block, half):
        rows = landing(lane, block, half)
        copy_to(rows, rows, z_send.at[0, 0, 0], recvs[lane].at[block, half], (sibling, c)).wait_recv()

    def block_to(lane, block, half, sem, there):
        rows = landing(lane, block, half)
        one = copy_to(rows, rows, sem, recvs[lane].at[block, half], (there, c))
        one.start()
        waits.append(one)

    def pass_on(lane, half, turn, d):
        block = seq_at(lax.rem(z + 4 - d, 4), xl, core)
        block_wait(lane, block, half)
        block_to(lane, block, half, x_send.at[lane, turn, d], seq_at(z, 1 - xl, core))
        block_to(lane, block, half, d_send.at[lane, turn, d], sibling)

    def relay(lane, half, turn, d):
        block = seq_at(lax.rem(z + 4 - d, 4), 1 - xl, core)
        block_wait(lane, block, half)
        block_to(lane, block, half, f_send.at[lane, turn, d], sibling)

    def send_queries(half, turn):
        for d in range(4):
            for j in range(2):
                to_z = lax.rem(z + d, 4)
                to = seq_at(to_z, half, j)
                piece = flat_t.at[pl.ds(pl.multiple_of(1280 + to_z * 160, 32), 160),
                                  pl.ds(pl.multiple_of(half * 256 + j * 128, 128), 128)]
                send_query(piece, to, d, j, turn, half)

    def send_query(piece, to, d, j, turn, half):
        remote = copy_to(piece, q_out.at[s], q_send.at[turn, d, j], q_recv.at[s], (to, c))
        if d:
            remote.start()
            waits.append(remote)
        else:
            here = pltpu.make_async_copy(piece, q_out.at[s], own_sem.at[2])
            mine = (half == xl) & (j == core)
            near.append((mine, here, remote))

            @pl.when(mine)
            def _():
                here.start()

            @pl.when(jnp.logical_not(mine))
            def _():
                remote.start()

    near = []
    early, late = xh, 1 - xh
    lax.fori_loop(early * 4, early * 4 + 4, norm_second, 0)
    w_far(1 - xl, 0)
    w_last(0)
    project_tiles(0, 3, early)
    own = [first_stage(0, early, 0)]
    project_tiles(3, 5, early)
    own.append(first_stage(1, early, 0))
    w_second(1, 1)
    m_ring(1 - xh)
    for d in (1, 3):
        pass_on(0, early, 0, d)
    m_end(1 - xh)
    kept = pltpu.make_async_copy(mixed, mixed_out, own_sem.at[1])
    kept.start()
    lax.fori_loop(late * 4, late * 4 + 4, norm_second, 0)
    project_tiles(0, 3, late)
    own.append(first_stage(0, late, 1))
    pass_on(0, early, 0, 2)
    for d in (1, 3):
        pass_on(1, early, 0, d)
    project_tiles(3, 5, late)
    own.append(first_stage(1, late, 1))
    w_ring(xl, 1)
    pass_on(1, early, 0, 2)
    relay(0, early, 0, 0)
    w_ring(1 - xl, 1)
    p_first()
    for lane in (0, 1):
        for d in (1, 3):
            pass_on(lane, late, 1, d)
    for d in (1, 3):
        relay(0, early, 0, d)
    for lane in (0, 1):
        pass_on(lane, late, 1, 2)
    p_second()
    w_far(xl, 1)
    w_far(1 - xl, 1)
    w_last(1)
    project_tiles(5, 7, early)
    send_queries(early, 0)
    project_tiles(5, 7, late)
    send_queries(late, 1)
    relay(0, early, 0, 2)
    for d in (0, 1, 3, 2):
        relay(1, early, 0, d)
    for lane in (0, 1):
        for d in (0, 1, 3, 2):
            relay(lane, late, 1, d)
    for half in (0, 1):
        for zz in range(4):
            for side in (0, 1):
                for lane in (0, 1):
                    block_wait(lane, seq_at(zz, side, 1 - core), half)
    for one in own:
        one.wait()
    for d in range(1, 16):
        block = lax.rem(s + d, 16)
        copy_to(q_out.at[block], q_out.at[block], q_send.at[0, 0, 0], q_recv.at[block], (block, c)).wait_recv()
    own_p.wait()
    kept.wait()
    p_last()
    for mine, here, remote in near:
        @pl.when(mine)
        def _():
            here.wait()

        @pl.when(jnp.logical_not(mine))
        def _():
            remote.wait_send()

    for one in waits:
        one.wait_send()


def front(*operands):
    dma = pltpu.SemaphoreType.DMA
    vm, anyw = pl.BlockSpec(memory_space=VMEM), pl.BlockSpec(memory_space=pl.ANY)
    return pl.pallas_call(
        front_kernel,
        out_shape=(
            jax.ShapeDtypeStruct((8, 64, 2560), BF16),
            jax.ShapeDtypeStruct((16, 160, 512), BF16),
            jax.ShapeDtypeStruct((16, 160, 512), BF16),
            jax.ShapeDtypeStruct((16, 160, 128), BF16),
            jax.ShapeDtypeStruct((2560, 640), BF16),
        ),
        in_specs=[pl.BlockSpec(memory_space=pltpu.SMEM), anyw, vm, anyw, anyw, anyw, anyw, vm, vm, vm, vm,
                  anyw, anyw, vm, anyw, anyw, anyw, anyw],
        out_specs=(anyw, anyw, anyw, anyw, anyw),
        scratch_shapes=[
            VMEM((8, 64, 2560), BF16),
            VMEM((8, 64, 2560), BF16),
            VMEM((2560, 640), BF16),
            VMEM((2560, 640), BF16),
            VMEM((2560, 128), BF16),
            VMEM((10, 2560), BF16),
            VMEM((128, 2560), BF16),
            VMEM((640, 2560), BF16),
            VMEM((8, 128), F32),
            VMEM((5120, 1920), BF16),
            VMEM((512, 5120), BF16),
            VMEM((8, 64, 2560), BF16),
            VMEM((1920, 512), BF16),
            VMEM((512, 640), F32),
            VMEM((512, 640), F32),
            VMEM((512, 640), F32),
            VMEM((4, 64, 640), F32),
            VMEM((2, 64, 640), BF16),
            VMEM((2, 64, 640), BF16),
            VMEM((4, 64, 640), BF16),
            VMEM((2, 8, 640), F32),
            VMEM((2, 8, 640), F32),
            VMEM((4, 8, 640), F32),
            VMEM((512, 128), F32),
            VMEM((128, 512), F32),
            VMEM((512, 640), F32),
            VMEM((512, 128), BF16),
            VMEM((128, 512), BF16),
            VMEM((160, 640), BF16),
            VMEM((8, 1, 512), F32),
            VMEM((512, 128), F32),
            VMEM((512, 640), BF16),
            dma((11,)),
            dma((60,)),
            dma((16, 2, 2)),
            dma((20,)),
            dma((16, 2)),
            dma((10,)),
            dma((12,)),
            dma((7,)),
            dma((8,)),
            *ring_scratch(64, 2560),
            dma((18,)),
            dma((8, 2)),
            dma((2, 2, 3)),
            dma((2, 2, 4)),
            dma((2, 2, 4)),
            dma((2, 2, 4)),
            dma((16, 2)),
            dma((16, 2)),
            dma((2, 4, 2)),
            dma((16,)),
            dma((2, 2)),
            dma((3,)),
        ],
        compiler_params=pltpu.CompilerParams(
            collective_id=0, has_side_effects=True, vmem_limit_bytes=67043328
        ),
        name="front",
    )(*operands)


def boundary(segments, value):
    count = jnp.int32(0)
    for bit in range(12, -1, -1):
        step = 1 << bit
        count = jnp.where(segments[count + step - 1] < value, count + step, count)
    return jnp.where(segments[jnp.minimum(count, 8191)] < value, count + 1, count)


def attend_kernel(segments, q_hbm, k_in, v_in, out, q_in, landed, keys, values, q_sem, k_sem, v_sem):
    quarter = lax.rem(lax.axis_index("seq"), 4)

    def loads(j):
        return [
            pltpu.make_async_copy(src.at[4 * j + side], dst.at[j, :, pl.ds(side * 512, 512)], sem.at[4 * j + side])
            for side in range(4) for src, dst, sem in ((k_in, landed, k_sem), (v_in, values, v_sem))
        ]

    q_load = pltpu.make_async_copy(q_hbm, q_in, q_sem)
    q_load.start()
    for j in range(4):
        for one in loads(j):
            one.start()
    first, second = boundary(segments, 1), boundary(segments, 2)
    scale = (AP ** -0.5) * 1.4426950408889634
    lane = lax.broadcasted_iota(jnp.int32, (1, 512), 1)
    q_load.wait()

    def tile(i, _):
        for n in range(1):
            for one in loads(i * 1 + n):
                one.wait()
            keys[i * 1 + n] = landed[i * 1 + n].astype(F32).T.astype(BF16)
        queries = jnp.concatenate([q_in[4 * i + n] for n in range(4)], axis=1)
        low_place = i * 2048 + quarter * 128
        place = low_place + lane + 384 * (lane // 128)
        begin = start_of(place, first, second)
        lowest = start_of(low_place, first, second) // 2048
        last_begin = start_of(low_place + 1663, first, second)
        plain_from = jnp.minimum((last_begin + 2047) // 2048, i * 1)

        def step(j, carry, causal, reset):
            top, total, acc = carry
            scores = jnp.dot(keys[j], queries, preferred_element_type=F32)
            if causal or reset:
                key = j * 2048 + lax.broadcasted_iota(jnp.int32, (2048, 512), 0)
                visible = key >= begin
                if causal:
                    visible = visible & (key <= place)
                scores = jnp.where(visible, scores, -1e30)
            new_top = jnp.maximum(top, jnp.max(scores, axis=0, keepdims=True))
            weights = jnp.exp2((scores - new_top) * scale)
            keep = jnp.exp2((top - new_top) * scale)
            total = total * keep + jnp.sum(weights, axis=0, keepdims=True)
            acc = acc * keep + jnp.dot(values[j], weights.astype(BF16), preferred_element_type=F32)
            return new_top, total, acc

        carry = (jnp.full((1, 512), -1e29, F32), jnp.zeros((1, 512), F32), jnp.zeros((AP, 512), F32))
        carry = lax.fori_loop(lowest, plain_from, lambda j, t: step(j, t, False, True), carry)
        carry = lax.fori_loop(
            jnp.maximum(lowest, plain_from), i * 1, lambda j, t: step(j, t, False, False), carry)
        top, total, acc = lax.fori_loop(
            jnp.maximum(lowest, i * 1), i * 1 + 1, lambda j, t: step(j, t, True, True), carry)
        context = (acc / total).astype(BF16)
        for n in range(4):
            out[4 * i + n] = context[:, n * 128:n * 128 + 128]
        return 0

    lax.fori_loop(0, 4, tile, 0)


def attend(segments, q_in, k_in, v_in):
    vm, anyw = pl.BlockSpec(memory_space=VMEM), pl.BlockSpec(memory_space=pl.ANY)
    return pl.pallas_call(
        attend_kernel,
        out_shape=jax.ShapeDtypeStruct((16, 160, 128), BF16),
        in_specs=[pl.BlockSpec(memory_space=pltpu.SMEM), anyw, anyw, anyw],
        out_specs=vm,
        scratch_shapes=[
            VMEM((16, 160, 128), BF16),
            VMEM((4, 160, 2048), BF16),
            VMEM((4, 2048, 160), BF16),
            VMEM((4, 160, 2048), BF16),
            pltpu.SemaphoreType.DMA,
            pltpu.SemaphoreType.DMA((16,)),
            pltpu.SemaphoreType.DMA((16,)),
        ],
        compiler_params=pltpu.CompilerParams(vmem_limit_bytes=67043328),
        name="attend",
    )(segments, q_in, k_in, v_in)


def finish_kernel(ctx, proj_in, mixed, out, proj_t, own_in, gathered, part, p_load, p_send, p_recv, in_send, in_recv, ring, fin, comb, across, rs_send, rs_recv, local_sem):
    s, c = lax.axis_index("seq"), lax.axis_index("chan")
    peers = chan_peers(s, c)
    z, xl, core = seq_parts(s)
    up, down, far = lax.rem(z + 1, 4), lax.rem(z + 3, 4), lax.rem(z + 2, 4)
    sibling = seq_at(z, xl, 1 - core)

    def p_rows(ref, block, half):
        if half is None:
            return ref.at[pl.ds(pl.multiple_of(block * 160, 32), 160), :]
        return ref.at[pl.ds(pl.multiple_of(block * 160 + half * 80, 16), 80), :]

    p_loads = []
    for i, block in enumerate((
        s, seq_at(z, 1 - xl, core), seq_at(up, xl, core), seq_at(down, xl, core), seq_at(far, xl, core),
        seq_at(up, 1 - xl, core), seq_at(down, 1 - xl, core),
        sibling, seq_at(z, 1 - xl, 1 - core), seq_at(up, xl, 1 - core), seq_at(down, xl, 1 - core),
    )):
        one = pltpu.make_async_copy(p_rows(proj_in, block, None), p_rows(proj_t, block, None), p_load.at[i])
        one.start()
        p_loads.append(one)
    window = pl.ds(pl.multiple_of(c * 5 // 2 * 128, 128), 384)
    own_load = pltpu.make_async_copy(mixed.at[:, window], own_in, local_sem.at[2])
    own_load.start()
    greet([(s, p) for p in peers] + [(lax.rem(s + d, 16), c) for d in range(1, 16)])
    lanes = pl.ds(pl.multiple_of(lax.rem(s, 4) * 128, 128), 128)
    waits = []
    for d in range(16):
        to = lax.rem(s + d, 16)
        where = gathered.at[pl.ds(pl.multiple_of(z * 160, 32), 160), lanes]
        if d == 0:
            own = pltpu.make_async_copy(ctx.at[s], where, local_sem.at[0])
            own.start()
        else:
            one = copy_to(ctx.at[to], where, in_send.at[d - 1], in_recv.at[s], (to, c))
            one.start()
            waits.append(one)
    def p_copy(i, src, block, half, to):
        return copy_to(p_rows(src, block, half), p_rows(proj_t, block, half), p_send.at[i], p_recv.at[i], (to, c))

    def p_to(i, src, block, half, to):
        one = p_copy(i, src, block, half, to)
        one.start()
        waits.append(one)

    p_to(0, proj_in, seq_at(down, 1 - xl, core), 0, seq_at(up, xl, core))
    p_to(1, proj_in, seq_at(up, 1 - xl, core), 1, seq_at(down, xl, core))
    p_to(2, proj_in, seq_at(down, 1 - xl, core), None, sibling)
    p_to(3, proj_in, seq_at(up, 1 - xl, core), None, sibling)
    p_to(4, proj_in, seq_at(far, xl, core), None, sibling)
    for half in (0, 1):
        p_copy(half, proj_t, seq_at(far, 1 - xl, core), half, sibling).wait_recv()
        p_to(5 + half, proj_t, seq_at(far, 1 - xl, core), half, sibling)
    own.wait()
    for d in range(1, 16):
        block = lax.rem(s + d, 16)
        where = gathered.at[pl.ds(pl.multiple_of((block // 4) * 160, 32), 160),
                            pl.ds(pl.multiple_of(lax.rem(block, 4) * 128, 128), 128)]
        copy_to(ctx.at[0], where, in_send.at[0], in_recv.at[block], (block, c)).wait_recv()
    gather = ChanSum(s, c, part, ring, fin, comb, across, rs_send, rs_recv)

    def make(turn):
        def rows_of(n, _):
            p = gather.column(turn) * 4 + n
            at = pl.ds(pl.multiple_of(p * 320, 32), 320)
            part[p] = jnp.dot(proj_t[at, :], gathered[...], preferred_element_type=F32).astype(BF16)
            return 0

        lax.fori_loop(0, 4, rows_of, 0)

    p_copy(2, proj_t, seq_at(down, 1 - xl, 1 - core), None, sibling).wait_recv()
    p_copy(3, proj_t, seq_at(up, 1 - xl, 1 - core), None, sibling).wait_recv()
    p_copy(4, proj_t, seq_at(far, xl, 1 - core), None, sibling).wait_recv()
    for half in (0, 1):
        p_copy(5 + half, proj_t, seq_at(far, 1 - xl, 1 - core), half, sibling).wait_recv()
    for one in p_loads:
        one.wait()
    make(0)
    gather.first(0)
    make(1)
    gather.second(0)
    gather.first(1)
    gather.cross()
    gather.second(1)
    own_load.wait()
    own_t_all = [own_in[n * 256:(n + 1) * 256, :].astype(F32).T for n in range(2)]
    gather.close()
    odd = lax.rem(c, 2) == 1
    for n in range(2):
        at = pl.ds(n * 256, 256)
        own_t = own_t_all[n]
        out[:, at] = (gather.result(at) + jnp.where(odd, own_t[64:, :], own_t[:320, :])).astype(BF16)
    for one in waits + gather.sent:
        one.wait_send()


def finish(ctx, proj_t, mixed):
    dma = pltpu.SemaphoreType.DMA
    vm, anyw = pl.BlockSpec(memory_space=VMEM), pl.BlockSpec(memory_space=pl.ANY)
    return pl.pallas_call(
        finish_kernel,
        out_shape=jax.ShapeDtypeStruct((320, 512), BF16),
        in_specs=[anyw, anyw, anyw],
        out_specs=vm,
        scratch_shapes=[
            VMEM((2560, 640), BF16),
            VMEM((512, 384), BF16),
            VMEM((640, 512), BF16),
            VMEM((8, 320, 512), BF16),
            dma((11,)),
            dma((7,)),
            dma((7,)),
            dma((15,)),
            dma((16,)),
            *ring_scratch(320, 512),
            dma((3,)),
        ],
        compiler_params=pltpu.CompilerParams(
            collective_id=2, has_side_effects=True, vmem_limit_bytes=67043328
        ),
        cost_estimate=pl.CostEstimate(flops=50_000_000_000, bytes_accessed=6_000_000, transcendentals=0),
        name="finish",
    )(ctx, proj_t, mixed)


def local(
    hidden,
    embedding,
    segments,
    input_norm_gain,
    gate_proj,
    input_proj,
    state_proj,
    step_proj,
    step_bias,
    decay_log,
    skip_gain,
    out_gain,
    out_proj,
    attn_gain,
    query_proj,
    key_proj,
    value_proj,
    attn_out,
):
    mixed, k_all, v_all, q_all, proj_t = front(
        segments, hidden.reshape(8, 64, 2560), input_norm_gain, input_proj, gate_proj, state_proj,
        step_proj.T, step_bias[None, :], decay_log[None, :], skip_gain[None, :], out_gain,
        out_proj, embedding.reshape(8, 64, 2560), attn_gain[None, :], key_proj, value_proj, query_proj,
        attn_out.T,
    )
    ctx = attend(segments, q_all, k_all, v_all)
    return finish(ctx, proj_t, mixed.reshape(512, 2560)).T


def solution(mesh):
    in_specs = (
        P("seq", None),
        P("seq", None),
        P(),
        P(),
        P(None, "chan"),
        P(None, "chan"),
        P(),
        P(None, "chan"),
        P("chan"),
        P("chan"),
        P("chan"),
        P("chan"),
        P("chan", None),
        P(),
        P("seq", "chan"),
        P("seq", "chan"),
        P("seq", "chan"),
        P("chan", "seq"),
    )
    out_specs = P("seq", "chan")
    return jax.shard_map(local, mesh=mesh, in_specs=in_specs, out_specs=out_specs, check_vma=False)
```
